8 devices in a mesh: dp: 2 (over z, y), ep: 4 (over x, core).
Axes of the slice: x: 2, y: 2, z: 1, core: 2. Of those that a mesh axis runs over, the one named last changes fastest.
Arguments:
- tokens: bfloat16 [8192, 768], P(('dp', 'ep')), parts along dimension 0
- choice_idx: int32 [64, 128], P(('dp', 'ep')), parts along dimension 0
- gate_weight: float32 [64, 128], P(('dp', 'ep')), parts along dimension 0
- w_in: bfloat16 [32, 768, 3072], P('ep')
- w_out: bfloat16 [32, 3072, 768], P('ep')
Outputs:
- output: bfloat16 [8192, 768], P(('dp', 'ep')), parts along dimension 0
There are 2 independent parts. The reference program is written for one: setup_inputs(seed, part) draws one part's arguments, and reference() takes and returns one part's arrays. A program takes and returns all parts, laid end to end along the dimension named above; an argument that names none is the same for every part.
All inputs are finite; a program needn't handle non-finite values.
Results may differ from the reference program's by a relative error of at most 0.001.
Values are sent between devices in bfloat16 or wider.
A program may use at most 1 GiB of HBM per device.

```python
import jax
import jax.numpy as jnp
from jax import lax

D_MODEL = 768
D_FF = 3072
EXPERTS = 32
TOKENS = 4096
CAPACITY = 128
GROUP_SIZE = 4


def draw_routing(route_key):
    tok_local = TOKENS // GROUP_SIZE
    slots_dev = (EXPERTS // GROUP_SIZE) * CAPACITY
    base_share = slots_dev // GROUP_SIZE
    hot_rows = tok_local // 8
    cold_rows = tok_local - hot_rows
    half_group = GROUP_SIZE // 2
    route_keys = jax.random.split(route_key, 6)
    dev_grid = jnp.tile(jnp.arange(GROUP_SIZE, dtype=jnp.int32)[None, :], (GROUP_SIZE, 1))
    src_perm = jax.random.permutation(route_keys[0], dev_grid, axis=1, independent=True)
    pair_delta = jax.random.randint(route_keys[1], (GROUP_SIZE, half_group), 0, base_share + 1)
    pair_delta = pair_delta.at[:, 0].set(base_share)
    perm_counts = jnp.stack([base_share + pair_delta, base_share - pair_delta], axis=2).reshape(GROUP_SIZE, GROUP_SIZE)
    dest_ids = jnp.arange(GROUP_SIZE)[:, None]
    counts = jnp.zeros((GROUP_SIZE, GROUP_SIZE), jnp.int32).at[dest_ids, src_perm].set(perm_counts)
    block_ends = jnp.cumsum(counts, axis=1)
    starts = block_ends - counts
    slot_pos = jnp.arange(slots_dev, dtype=jnp.int32)
    src_of = jax.vmap(lambda end_row: jnp.searchsorted(end_row, slot_pos, side="right"))(block_ends)
    within = slot_pos[None, :] - jnp.take_along_axis(starts, src_of, axis=1)
    block_len = jnp.take_along_axis(counts, src_of, axis=1)
    hot_count = jnp.minimum(block_len // 2, hot_rows)
    hot_off = jax.random.randint(route_keys[2], (GROUP_SIZE, GROUP_SIZE), 0, hot_rows)
    cold_off = jax.random.randint(route_keys[3], (GROUP_SIZE, GROUP_SIZE), 0, cold_rows)
    hot_pick = (jnp.take_along_axis(hot_off, src_of, axis=1) + within) % hot_rows
    cold_pick = hot_rows + (jnp.take_along_axis(cold_off, src_of, axis=1) + within - hot_count) % cold_rows
    local_rank = jnp.where(within < hot_count, hot_pick, cold_pick)
    row_grid = jnp.tile(jnp.arange(tok_local, dtype=jnp.int32)[None, :], (GROUP_SIZE, 1))
    row_order = jax.random.permutation(route_keys[4], row_grid, axis=1, independent=True).reshape(-1)
    chosen = src_of * tok_local + row_order[src_of * tok_local + local_rank]
    chosen = chosen.reshape(EXPERTS, CAPACITY)
    return jax.random.permutation(route_keys[5], chosen, axis=1, independent=True)


def setup_inputs(seed: int = 0, part: int = 0) -> dict:
    base_key = jax.random.key(seed)
    shared_keys = jax.random.split(base_key, 2)
    part_keys = jax.random.split(jax.random.fold_in(base_key, part), 3)
    tokens = jax.random.normal(part_keys[0], (TOKENS, D_MODEL), jnp.float32).astype(jnp.bfloat16)
    choice_idx = draw_routing(part_keys[1])
    gate_weight = jax.random.uniform(part_keys[2], (EXPERTS, CAPACITY), jnp.float32, 0.5, 1.5)
    w_in = (jax.random.normal(shared_keys[0], (EXPERTS, D_MODEL, D_FF), jnp.float32) * D_MODEL ** -0.5).astype(jnp.bfloat16)
    w_out = (jax.random.normal(shared_keys[1], (EXPERTS, D_FF, D_MODEL), jnp.float32) * D_FF ** -0.5).astype(jnp.bfloat16)
    return {"tokens": tokens, "choice_idx": choice_idx, "gate_weight": gate_weight, "w_in": w_in, "w_out": w_out}


def reference(tokens, choice_idx, gate_weight, w_in, w_out):
    def expert_step(acc_sum, per_expert):
        idx_row, gate_row, w_first, w_second = per_expert
        tok_rows = tokens[idx_row]
        pre_act = jnp.dot(tok_rows, w_first, preferred_element_type=jnp.float32)
        hidden = jax.nn.gelu(pre_act, approximate=True).astype(jnp.bfloat16)
        expert_out = jnp.dot(hidden, w_second, preferred_element_type=jnp.float32)
        weighted = (gate_row[:, None] * expert_out).astype(jnp.bfloat16)
        return acc_sum.at[idx_row].add(weighted.astype(jnp.float32)), None

    zero_acc = jnp.zeros((TOKENS, D_MODEL), jnp.float32)
    acc_sum = lax.scan(expert_step, zero_acc, (choice_idx, gate_weight, w_in, w_out))[0]
    return (tokens.astype(jnp.float32) + acc_sum).astype(jnp.bfloat16)
```

```python
import jax
import jax.numpy as jnp
from jax import lax
from jax.experimental import pallas as pl
from jax.experimental.pallas import tpu as pltpu
from jax.sharding import PartitionSpec as P

F32, BF16 = jnp.float32, jnp.bfloat16
W_SLOTS = 3
LANES = 128


def moe_kernel(tok, idx, gate, w_in, w_out, out,
               chip_tok, idx_all, gate_v, xsend, xrecv, xown, pbuf, acc, obuf, wi, wo,
               loc_sem, w_sem, idx_ss, idx_rs, tok_ss, tok_rs, x_ss, x_rs,
               po_ss, po_rs, pm_ss, pm_rs, pd_ss, pd_rs, out_sem):
    n_tok, d_model = tok.shape
    n_exp, cap = idx.shape
    d_ff = w_in.shape[2]
    ep = lax.axis_index("ep")
    chip, core = ep // 2, ep % 2
    mate = chip * 2 + (1 - core)
    opp = (1 - chip) * 2 + core
    diag = (1 - chip) * 2 + (1 - core)
    chip_base = chip * (2 * n_tok)

    def remote(src, dst, ss, rs, dev):
        return pltpu.make_async_remote_copy(src_ref=src, dst_ref=dst, send_sem=ss, recv_sem=rs,
                                            device_id={"ep": dev}, device_id_type=pl.DeviceIdType.MESH)

    def w_copies(e):
        slot = lax.rem(e, W_SLOTS)
        return (pltpu.make_async_copy(w_in.at[e], wi.at[slot], w_sem.at[0, slot]),
                pltpu.make_async_copy(w_out.at[e], wo.at[slot], w_sem.at[1, slot]))

    own_rows = pl.ds(pl.multiple_of(core * n_tok, n_tok), n_tok)
    own_tok = pltpu.make_async_copy(tok, chip_tok.at[own_rows], loc_sem.at[0])
    own_idx = pltpu.make_async_copy(idx, idx_all.at[ep], loc_sem.at[1])
    own_gate = pltpu.make_async_copy(gate, gate_v, loc_sem.at[2])
    own_tok.start()
    own_idx.start()
    own_gate.start()
    barrier = pltpu.get_barrier_semaphore()
    for dev in (mate, opp, diag):
        pl.semaphore_signal(barrier, inc=1, device_id={"ep": dev}, device_id_type=pl.DeviceIdType.MESH)
    pl.semaphore_wait(barrier, 3)

    idx_out = [remote(idx, idx_all.at[ep], idx_ss.at[k], idx_rs.at[k], dev) for k, dev in enumerate((opp, mate, diag))]
    tok_out = remote(tok, chip_tok.at[own_rows], tok_ss, tok_rs, mate)
    idx_out[0].start()
    tok_out.start()
    idx_out[1].start()
    idx_out[2].start()
    for e in range(W_SLOTS):
        for c in w_copies(e):
            c.start()

    lane = lax.broadcasted_iota(jnp.int32, (cap, LANES), 1)
    n_tiles = 2 * n_tok // LANES

    def gather(dev, e0, count):
        blocks = []
        for k in range(count):
            row = idx_all[dev, pl.ds(e0 + k, 1), :] - chip_base
            col = jnp.broadcast_to(row, (LANES, cap)).T
            tiles = [jnp.where(col == lane + LANES * j, 1.0, 0.0).astype(BF16) for j in range(n_tiles)]
            blocks.append(jnp.concatenate(tiles, axis=1))
        hot = jnp.concatenate(blocks, axis=0)
        return jnp.dot(hot, chip_tok[...], preferred_element_type=F32).astype(BF16)

    def rows_of(e, count=1):
        return pl.ds(pl.multiple_of(e * cap, cap), count * cap)

    def x_copy(e):
        return remote(xsend.at[rows_of(e)], xrecv.at[rows_of(e)], x_ss.at[e], x_rs.at[e], opp)

    own_tok.wait()
    own_idx.wait()
    idx_out[0].wait_recv()
    tok_out.wait_recv()

    @pl.loop(0, n_exp // 2)
    def _(g):
        xsend[rows_of(2 * g, 2), :] = gather(opp, 2 * g, 2)
        x_copy(2 * g).start()
        x_copy(2 * g + 1).start()

    @pl.loop(0, n_exp // 2)
    def _(g):
        xown[rows_of(2 * g, 2), :] = gather(ep, 2 * g, 2)

    own_gate.wait()

    @pl.loop(0, n_tok // 256)
    def _(b):
        r = pl.ds(pl.multiple_of(b * 256, 256), 256)
        acc[r, :] = chip_tok[pl.ds(pl.multiple_of(core * n_tok + b * 256, 256), 256), :].astype(F32)

    f_tile = 512

    def po_copy(e):
        return remote(pbuf.at[0, rows_of(e)], pbuf.at[2, rows_of(e)], po_ss.at[e], po_rs.at[e], opp)

    def pm_copy(e):
        return remote(pbuf.at[0, rows_of(e)], pbuf.at[1, rows_of(e)], pm_ss.at[e], pm_rs.at[e], mate)

    def pd_copy(e):
        return remote(pbuf.at[2, rows_of(e)], pbuf.at[3, rows_of(e)], pd_ss.at[e], pd_rs.at[e], mate)

    @pl.loop(0, n_exp)
    def _(e):
        slot = lax.rem(e, W_SLOTS)
        x_copy(e).wait_recv()
        x = xrecv[rows_of(e), :] + xown[rows_of(e), :]
        for c in w_copies(e):
            c.wait()
        o = None
        for f in range(d_ff // f_tile):
            fs = slice(f * f_tile, (f + 1) * f_tile)
            pre = jnp.dot(x, wi[slot, :, fs], preferred_element_type=F32)
            h = jax.nn.gelu(pre, approximate=True).astype(BF16)
            part = jnp.dot(h, wo[slot, fs, :], preferred_element_type=F32)
            o = part if o is None else o + part
        gcol = jnp.broadcast_to(gate_v[pl.ds(e, 1), :], (LANES, cap)).T
        pbuf[0, rows_of(e), :] = (jnp.concatenate([gcol] * (d_model // LANES), axis=1) * o).astype(BF16)
        po_copy(e).start()
        pm_copy(e).start()

        @pl.when(e + W_SLOTS < n_exp)
        def _():
            for c in w_copies(e + W_SLOTS):
                c.start()

    idx_out[1].wait_recv()
    idx_out[2].wait_recv()

    n_blk = n_tok // 256
    sub = lax.broadcasted_iota(jnp.int32, (256, cap), 0)

    def scatter(e, last):
        rows = [idx_all[dev, pl.ds(e, 1), :] - ep * n_tok for dev in (ep, mate, opp, diag)]
        pcat = jnp.concatenate([pbuf[k, rows_of(e), :] for k in range(4)], axis=0)

        def block(b):
            r = pl.ds(pl.multiple_of(b * 256, 256), 256)
            hot = jnp.concatenate(
                [jnp.where(row == sub + b * 256, 1.0, 0.0).astype(BF16) for row in rows], axis=1)
            total = acc[r, :] + jnp.dot(hot, pcat, preferred_element_type=F32)
            if last:
                obuf[r, :] = total.astype(BF16)
                pltpu.make_async_copy(obuf.at[r], out.at[r], out_sem.at[b]).start()
            else:
                acc[r, :] = total

        pl.loop(0, n_blk)(block)

    def combine(e, last):
        po_copy(e).wait_recv()
        pd_copy(e).start()
        pm_copy(e).wait_recv()
        pd_copy(e).wait_recv()
        scatter(e, last)

    @pl.loop(0, n_exp - 1)
    def _(e):
        combine(e, False)

    combine(n_exp - 1, True)

    for c in idx_out:
        c.wait_send()
    tok_out.wait_send()

    @pl.loop(0, n_exp)
    def _(e):
        x_copy(e).wait_send()
        po_copy(e).wait_send()
        pm_copy(e).wait_send()
        pd_copy(e).wait_send()

    @pl.loop(0, n_blk)
    def _(b):
        r = pl.ds(pl.multiple_of(b * 256, 256), 256)
        pltpu.make_async_copy(obuf.at[r], out.at[r], out_sem.at[b]).wait()


def solution(mesh):
    row_spec = P(("dp", "ep"), None)
    expert_spec = P("ep", None, None)

    def local_layer(tok, idx, gate, w_in, w_out):
        n_tok, d_model = tok.shape
        n_exp, cap = idx.shape
        d_ff = w_in.shape[2]
        slots = n_exp * cap
        dma = pltpu.SemaphoreType.DMA
        any_spec = pl.BlockSpec(memory_space=pl.ANY)
        return pl.pallas_call(
            moe_kernel,
            out_shape=jax.ShapeDtypeStruct((n_tok, d_model), BF16),
            in_specs=[any_spec] * 5,
            out_specs=any_spec,
            scratch_shapes=[
                pltpu.VMEM((2 * n_tok, d_model), BF16),
                pltpu.VMEM((4, n_exp, cap), jnp.int32),
                pltpu.VMEM((n_exp, cap), F32),
                pltpu.VMEM((slots, d_model), BF16),
                pltpu.VMEM((slots, d_model), BF16),
                pltpu.VMEM((slots, d_model), BF16),
                pltpu.VMEM((4, slots, d_model), BF16),
                pltpu.VMEM((n_tok, d_model), F32),
                pltpu.VMEM((n_tok, d_model), BF16),
                pltpu.VMEM((W_SLOTS, d_model, d_ff), BF16),
                pltpu.VMEM((W_SLOTS, d_ff, d_model), BF16),
                dma((3,)), dma((2, W_SLOTS)), dma((3,)), dma((3,)), dma, dma,
                dma((n_exp,)), dma((n_exp,)), dma((n_exp,)), dma((n_exp,)),
                dma((n_exp,)), dma((n_exp,)), dma((n_exp,)), dma((n_exp,)),
                dma((n_tok // 256,)),
            ],
            compiler_params=pltpu.CompilerParams(
                collective_id=0, has_side_effects=True, vmem_limit_bytes=63 * 1024 * 1024),
        )(tok, idx, gate, w_in, w_out)

    return jax.shard_map(local_layer, mesh=mesh, in_specs=(row_spec, row_spec, row_spec, expert_spec, expert_spec),
                         out_specs=row_spec, check_vma=False)
```

```python
import functools

import jax
import jax.numpy as jnp
from jax import lax
from jax.experimental import pallas as pl
from jax.experimental.pallas import tpu as pltpu
from jax.sharding import PartitionSpec as P

F32, BF16, I32 = jnp.float32, jnp.bfloat16, jnp.int32
W_SLOTS = 3
LANES = 128
FAR = 1 << 20


def remote(src, dst, ss, rs, **dev):
    return pltpu.make_async_remote_copy(src_ref=src, dst_ref=dst, send_sem=ss, recv_sem=rs,
                                        device_id=dev, device_id_type=pl.DeviceIdType.MESH)


def signal(sem, **dev):
    pl.semaphore_signal(sem, inc=1, device_id=dev, device_id_type=pl.DeviceIdType.MESH)


def plan_kernel(n_dp, n_ep, sizes, tok, idx, mate_tok, meta, bucket, idx_g, loc_sem, idx_ss, idx_rs, tok_ss, tok_rs):
    n_tok = tok.shape[0]
    n_exp, cap = idx.shape
    dp, ep = lax.axis_index("dp"), lax.axis_index("ep")
    me = dp * n_ep + ep
    n_dev = n_dp * n_ep
    own_idx = pltpu.make_async_copy(idx, idx_g.at[me], loc_sem)
    own_idx.start()
    barrier = pltpu.get_barrier_semaphore()
    others = []
    for k in range(1, n_dev):
        dev = lax.rem(me + k, n_dev)
        others.append((dev // n_ep, lax.rem(dev, n_ep)))
    for d, e in others:
        signal(barrier, dp=d, ep=e)
    pl.semaphore_wait(barrier, n_dev - 1)
    mate = ep + 1 - 2 * lax.rem(ep, 2)
    tok_out = remote(tok, mate_tok, tok_ss, tok_rs, dp=dp, ep=mate)
    tok_out.start()
    own_idx.wait()
    sends = []
    for k, (d, e) in enumerate(others):
        c = remote(idx_g.at[me], idx_g.at[me], idx_ss.at[k], idx_rs.at[k], dp=d, ep=e)
        c.start()
        sends.append(c)
    rows = 2 * n_exp
    half = 2 * n_tok

    key_r = lax.broadcasted_iota(I32, (rows, rows), 0)
    key_c = lax.broadcasted_iota(I32, (rows, rows), 1)
    order_r = lax.rem(key_r, n_exp) * 2 + key_r // n_exp
    order_c = lax.rem(key_c, n_exp) * 2 + key_c // n_exp
    before = jnp.where(order_c < order_r, 1.0, 0.0).astype(BF16)
    every = jnp.ones((rows, rows), BF16)
    up_r = lax.broadcasted_iota(I32, (cap, cap), 0)
    up_c = lax.broadcasted_iota(I32, (cap, cap), 1)
    upper = jnp.where(up_r < up_c, 1.0, 0.0).astype(BF16)
    ones = jnp.ones((cap, cap), BF16)

    for c in sends:
        c.wait_recv()

    def crosses(d, h):
        ids = jnp.concatenate([idx_g[d * n_ep + 2 * h], idx_g[d * n_ep + 2 * h + 1]], axis=0)
        return ids, (ids >= half) if h == 0 else (ids < half)

    most = None
    for d in range(n_dp):
        for h in range(2):
            _, need = crosses(d, h)
            n = jnp.sum(jnp.where(need, 1.0, 0.0))
            most = n if most is None else jnp.maximum(most, n)
    pick = jnp.int32(0)
    for s in sizes[:-1]:
        pick = pick + jnp.where(most > s, 1, 0).astype(I32)
    bucket[0] = pick

    for h in range(2):
        ids, need = crosses(dp, h)
        flag = jnp.where(need, 1.0, 0.0).astype(BF16)
        in_row = jnp.dot(flag, upper, preferred_element_type=F32)
        row_sum = jnp.dot(flag, ones, preferred_element_type=F32).astype(BF16)
        prior = jnp.dot(before, row_sum, preferred_element_type=F32)
        total = jnp.dot(every, row_sum, preferred_element_type=F32)
        pos = (in_row + prior).astype(I32)
        meta[0, h * rows:(h + 1) * rows, :] = ids
        meta[1, h * rows:(h + 1) * rows, :] = jnp.where(need, pos, FAR)
        meta[2, h * rows:(h + 1) * rows, :] = jnp.where(need, pos - total.astype(I32), FAR)

    for c in sends:
        c.wait_send()
    tok_out.wait()


def layer_kernel(k_rows, tok, mate_tok, meta, gate, w_in, w_out, out,
                 chip_tok, meta_v, gate_v, xsend, land, local, xbuf, chip_p, pland, rsend, rland, tokrow,
                 acc, obuf, wi, wo,
                 loc_sem, w_sem, d_ss, d_rs, f_ss, f_rs, p_ss, p_rs, r_ss, r_rs, g_ss, g_rs, out_sem):
    n_tok, d_model = tok.shape
    n_exp, d_ff = w_in.shape[0], w_in.shape[2]
    cap = gate.shape[1]
    slots = n_exp * cap
    rows = 2 * n_exp
    nc = k_rows // (2 * cap)
    ep = lax.axis_index("ep")
    chip, core = ep // 2, ep % 2
    mate = chip * 2 + (1 - core)
    opp = (1 - chip) * 2 + core
    chip_base = chip * (2 * n_tok)

    def at(start, size):
        return pl.ds(pl.multiple_of(start, cap), size)

    def w_copies(e):
        slot = lax.rem(e, W_SLOTS)
        return (pltpu.make_async_copy(w_in.at[e], wi.at[slot], w_sem.at[0, slot]),
                pltpu.make_async_copy(w_out.at[e], wo.at[slot], w_sem.at[1, slot]))

    first = [pltpu.make_async_copy(meta, meta_v, loc_sem.at[0]),
             pltpu.make_async_copy(tok, chip_tok.at[at(core * n_tok, n_tok)], loc_sem.at[1]),
             pltpu.make_async_copy(mate_tok, chip_tok.at[at((1 - core) * n_tok, n_tok)], loc_sem.at[2]),
             pltpu.make_async_copy(gate, gate_v, loc_sem.at[3])]
    for c in first:
        c.start()
    barrier = pltpu.get_barrier_semaphore()
    signal(barrier, ep=mate)
    signal(barrier, ep=opp)
    for e in range(W_SLOTS):
        for c in w_copies(e):
            c.start()

    def d_copy(m):
        return remote(xsend.at[at(m * cap, cap)], land.at[at((2 * m + core) * cap, cap)], d_ss.at[m], d_rs.at[m], ep=opp)

    def f_copy(m):
        r = at((2 * m + core) * cap, cap)
        return remote(land.at[r], land.at[r], f_ss.at[m], f_rs.at[m], ep=mate)

    def p_copy(e):
        return remote(chip_p.at[at(core * slots + e * cap, cap)], pland.at[at(e * cap, cap)], p_ss.at[e], p_rs.at[e], ep=mate)

    def r_copy(m):
        return remote(rsend.at[at(m * cap, cap)], rland.at[at((2 * m + core) * cap, cap)], r_ss.at[m], r_rs.at[m], ep=opp)

    def g_copy(m):
        r = at((2 * m + core) * cap, cap)
        return remote(rland.at[r], rland.at[r], g_ss.at[m], g_rs.at[m], ep=mate)

    lane = lax.broadcasted_iota(I32, (cap, LANES), 1)
    sub = lax.broadcasted_iota(I32, (cap, LANES), 0)

    def spread(col, width, base):
        return jnp.concatenate(
            [jnp.where(col == lane + (base + LANES * j), 1.0, 0.0).astype(BF16) for j in range(width // LANES)], axis=1)

    def column(row):
        return jnp.broadcast_to(row, (LANES, cap)).T

    their = (1 - chip) * rows
    mine = chip * rows

    def owner_ids(kind, block, shift):
        t = jnp.zeros((cap, LANES), I32)
        for i in range(rows):
            pos = meta_v[kind, pl.ds(their + i, 1), :] + shift
            ids = meta_v[0, pl.ds(their + i, 1), :]
            t = t + jnp.where(jnp.broadcast_to(pos, (cap, LANES)) == sub + block * cap, jnp.broadcast_to(ids, (cap, LANES)), 0)
        return t

    first[0].wait()

    def gather_block(m):
        t = owner_ids(1, 2 * m + core, 0).astype(F32)
        ids = jnp.sum(t, axis=1, keepdims=True).astype(I32) - chip_base
        return spread(jnp.broadcast_to(ids, (cap, LANES)), 2 * n_tok, 0)

    first[1].wait()
    first[2].wait()
    pl.semaphore_wait(barrier, 2)

    def send_group(m0, count):
        hot = jnp.concatenate([gather_block(m0 + k) for k in range(count)], axis=0)
        xsend[at(m0 * cap, count * cap), :] = jnp.dot(hot, chip_tok[...], preferred_element_type=F32).astype(BF16)
        for k in range(count):
            d_copy(m0 + k).start()

    @pl.loop(0, nc // 2)
    def _(g):
        send_group(2 * g, 2)

    if nc % 2:
        send_group(nc - 1, 1)

    @pl.loop(0, n_exp // 2)
    def _(g):
        hot = jnp.concatenate(
            [spread(column(meta_v[0, pl.ds(mine + core * n_exp + 2 * g + k, 1), :] - chip_base), 2 * n_tok, 0)
             for k in range(2)], axis=0)
        xbuf[at(2 * g * cap, 2 * cap), :] = jnp.dot(hot, chip_tok[...], preferred_element_type=F32).astype(BF16)

    @pl.loop(0, 2 * nc)
    def _(j):
        t = owner_ids(2, j, k_rows).astype(F32).T
        tokrow[pl.ds(j, 1), :] = jnp.sum(t, axis=0, keepdims=True).astype(I32)

    @pl.loop(0, k_rows // (2 * cap))
    def _(b):
        local[at(b * 2 * cap, 2 * cap), :] = jnp.zeros((2 * cap, d_model), BF16)

    @pl.loop(0, rows // 2)
    def _(b):
        chip_p[at(b * 2 * cap, 2 * cap), :] = jnp.zeros((2 * cap, d_model), BF16)

    first[3].wait()

    def forward(m):
        d_copy(m).wait_recv()
        f_copy(m).start()

    forward(0)
    if nc > 1:
        forward(1)
    f_tile = 512

    def pack_return(e):
        p_copy(e).wait_recv()
        chip_p[at((1 - core) * slots + e * cap, cap), :] = pland[at(e * cap, cap), :]
        m = e - (n_exp - nc)

        @pl.when(m >= 0)
        def _():
            parts = []
            for i in range(rows):
                pos = meta_v[2, pl.ds(mine + i, 1), :] + k_rows
                parts.append(jnp.where(jnp.broadcast_to(pos, (cap, LANES)) == sub + (2 * m + core) * cap, 1.0, 0.0).astype(BF16))
            hot = jnp.concatenate(parts, axis=1)
            rsend[at(m * cap, cap), :] = jnp.dot(hot, chip_p[...], preferred_element_type=F32).astype(BF16)
            r_copy(m).start()

    @pl.loop(0, n_exp)
    def _(e):
        slot = lax.rem(e, W_SLOTS)

        @pl.when(lax.rem(e, 2) == 0)
        def _():
            for k in range(2):
                m = e + k

                @pl.when(m < nc)
                def _():
                    f_copy(m).wait_recv()
                    local[at(2 * m * cap, 2 * cap), :] = land[at(2 * m * cap, 2 * cap), :]

            hot = jnp.concatenate(
                [spread(column(meta_v[1, pl.ds(mine + core * n_exp + e + k, 1), :]), k_rows, 0) for k in range(2)], axis=0)
            r = at(e * cap, 2 * cap)
            xbuf[r, :] = xbuf[r, :] + jnp.dot(hot, local[...], preferred_element_type=F32).astype(BF16)

        x = xbuf[at(e * cap, cap), :]
        for c in w_copies(e):
            c.wait()
        o = None
        for f in range(d_ff // f_tile):
            fs = slice(f * f_tile, (f + 1) * f_tile)
            pre = jnp.dot(x, wi[slot, :, fs], preferred_element_type=F32)
            h = jax.nn.gelu(pre, approximate=True).astype(BF16)
            part = jnp.dot(h, wo[slot, fs, :], preferred_element_type=F32)
            o = part if o is None else o + part
        gcol = column(gate_v[pl.ds(e, 1), :])
        chip_p[at(core * slots + e * cap, cap), :] = (jnp.concatenate([gcol] * (d_model // LANES), axis=1) * o).astype(BF16)
        p_copy(e).start()

        @pl.when(e + W_SLOTS < n_exp)
        def _():
            for c in w_copies(e + W_SLOTS):
                c.start()

        @pl.when(e + 2 < nc)
        def _():
            forward(e + 2)

        @pl.when(e > 0)
        def _():
            pack_return(e - 1)

    pack_return(n_exp - 1)

    n_blk = n_tok // (2 * cap)
    blk = 2 * cap
    sub_b = lax.broadcasted_iota(I32, (blk, LANES), 0) + ep * n_tok

    @pl.loop(0, n_blk)
    def _(b):
        r = at(b * blk, blk)
        hot = jnp.concatenate(
            [jnp.where(jnp.broadcast_to(meta_v[0, pl.ds(mine + i, 1), :], (blk, LANES)) == sub_b + b * blk, 1.0, 0.0).astype(BF16)
             for i in range(rows)], axis=1)
        own = chip_tok[at(core * n_tok + b * blk, blk), :].astype(F32)
        acc[r, :] = own + jnp.dot(hot, chip_p[...], preferred_element_type=F32)

    def combine(m, last):
        r_copy(m).wait_recv()
        g_copy(m).start()
        ids = [tokrow[pl.ds(2 * m + k, 1), :] for k in range(2)]
        g_copy(m).wait_recv()
        back = rland[at(2 * m * cap, 2 * cap), :]

        @pl.loop(0, n_blk)
        def _(b):
            r = at(b * blk, blk)
            hot = jnp.concatenate(
                [jnp.where(jnp.broadcast_to(i, (blk, LANES)) == sub_b + b * blk, 1.0, 0.0).astype(BF16) for i in ids], axis=1)
            total = acc[r, :] + jnp.dot(hot, back, preferred_element_type=F32)
            if last:
                obuf[r, :] = total.astype(BF16)
                pltpu.make_async_copy(obuf.at[r], out.at[r], out_sem.at[b]).start()
            else:
                acc[r, :] = total

    @pl.loop(0, nc - 1)
    def _(m):
        combine(m, False)

    combine(nc - 1, True)

    @pl.loop(0, nc)
    def _(m):
        d_copy(m).wait_send()
        f_copy(m).wait_send()
        r_copy(m).wait_send()
        g_copy(m).wait_send()

    @pl.loop(0, n_exp)
    def _(e):
        p_copy(e).wait_send()

    @pl.loop(0, n_blk)
    def _(b):
        r = at(b * blk, blk)
        pltpu.make_async_copy(obuf.at[r], out.at[r], out_sem.at[b]).wait()


def solution(mesh):
    n_dp, n_ep = mesh.shape["dp"], mesh.shape["ep"]
    row_spec = P(("dp", "ep"), None)
    expert_spec = P("ep", None, None)
    dma = pltpu.SemaphoreType.DMA
    any_spec = pl.BlockSpec(memory_space=pl.ANY)

    def local_layer(tok, idx, gate, w_in, w_out):
        n_tok, d_model = tok.shape
        n_exp, cap = idx.shape
        d_ff = w_in.shape[2]
        slots = n_exp * cap
        sizes = tuple(slots + i * 2 * cap for i in range(slots // (2 * cap) + 1))
        n_dev = n_dp * n_ep

        mate_tok, meta, bucket = pl.pallas_call(
            functools.partial(plan_kernel, n_dp, n_ep, sizes),
            out_shape=(jax.ShapeDtypeStruct((n_tok, d_model), BF16),
                       jax.ShapeDtypeStruct((3, 4 * n_exp, cap), I32),
                       jax.ShapeDtypeStruct((1,), I32)),
            in_specs=[any_spec] * 2,
            out_specs=(any_spec, pl.BlockSpec(memory_space=pltpu.VMEM), pl.BlockSpec(memory_space=pltpu.SMEM)),
            scratch_shapes=[
                pltpu.VMEM((n_dev, n_exp, cap), I32),
                dma, dma((n_dev - 1,)), dma((n_dev - 1,)), dma, dma,
            ],
            compiler_params=pltpu.CompilerParams(collective_id=0, has_side_effects=True),
        )(tok, idx)

        def branch(i):
            k_rows = sizes[i]
            nc = k_rows // (2 * cap)

            def run(tok, mate_tok, meta, gate, w_in, w_out):
                return pl.pallas_call(
                    functools.partial(layer_kernel, k_rows),
                    out_shape=jax.ShapeDtypeStruct((n_tok, d_model), BF16),
                    in_specs=[any_spec] * 6,
                    out_specs=any_spec,
                    scratch_shapes=[
                        pltpu.VMEM((2 * n_tok, d_model), BF16),
                        pltpu.VMEM((3, 4 * n_exp, cap), I32),
                        pltpu.VMEM((n_exp, cap), F32),
                        pltpu.VMEM((nc * cap, d_model), BF16),
                        pltpu.VMEM((k_rows, d_model), BF16),
                        pltpu.VMEM((k_rows, d_model), BF16),
                        pltpu.VMEM((slots, d_model), BF16),
                        pltpu.VMEM((2 * slots, d_model), BF16),
                        pltpu.VMEM((slots, d_model), BF16),
                        pltpu.VMEM((nc * cap, d_model), BF16),
                        pltpu.VMEM((k_rows, d_model), BF16),
                        pltpu.VMEM((2 * nc, cap), I32),
                        pltpu.VMEM((n_tok, d_model), F32),
                        pltpu.VMEM((n_tok, d_model), BF16),
                        pltpu.VMEM((W_SLOTS, d_model, d_ff), BF16),
                        pltpu.VMEM((W_SLOTS, d_ff, d_model), BF16),
                        dma((4,)), dma((2, W_SLOTS)),
                        dma((nc,)), dma((nc,)), dma((nc,)), dma((nc,)),
                        dma((n_exp,)), dma((n_exp,)),
                        dma((nc,)), dma((nc,)), dma((nc,)), dma((nc,)),
                        dma((n_tok // (2 * cap),)),
                    ],
                    compiler_params=pltpu.CompilerParams(
                        collective_id=1 + i, has_side_effects=True, vmem_limit_bytes=63 * 1024 * 1024),
                )(tok, mate_tok, meta, gate, w_in, w_out)

            return run

        return lax.switch(bucket[0], [branch(i) for i in range(len(sizes))], tok, mate_tok, meta, gate, w_in, w_out)

    return jax.shard_map(local_layer, mesh=mesh, in_specs=(row_spec, row_spec, row_spec, expert_spec, expert_spec),
                         out_specs=row_spec, check_vma=False)
```

```python
import functools

import jax
import jax.numpy as jnp
from jax import lax
from jax.experimental import pallas as pl
from jax.experimental.pallas import tpu as pltpu
from jax.sharding import PartitionSpec as P

F32, BF16, I32 = jnp.float32, jnp.bfloat16, jnp.int32
W_SLOTS = 3
LANES = 128
FAR = 1 << 20


def remote(src, dst, ss, rs, **dev):
    return pltpu.make_async_remote_copy(src_ref=src, dst_ref=dst, send_sem=ss, recv_sem=rs,
                                        device_id=dev, device_id_type=pl.DeviceIdType.MESH)


def signal(sem, **dev):
    pl.semaphore_signal(sem, inc=1, device_id=dev, device_id_type=pl.DeviceIdType.MESH)


def plan_kernel(n_dp, n_ep, sizes, tok, idx, mate_tok, meta, bucket, idx_g, loc_sem, idx_ss, idx_rs, tok_ss, tok_rs):
    n_tok = tok.shape[0]
    n_exp, cap = idx.shape
    dp, ep = lax.axis_index("dp"), lax.axis_index("ep")
    me = dp * n_ep + ep
    n_dev = n_dp * n_ep
    own_idx = pltpu.make_async_copy(idx, idx_g.at[me], loc_sem)
    own_idx.start()
    barrier = pltpu.get_barrier_semaphore()
    others = []
    for k in range(1, n_dev):
        dev = lax.rem(me + k, n_dev)
        others.append((dev // n_ep, lax.rem(dev, n_ep)))
    for d, e in others:
        signal(barrier, dp=d, ep=e)
    pl.semaphore_wait(barrier, n_dev - 1)
    mate = ep + 1 - 2 * lax.rem(ep, 2)
    tok_out = remote(tok, mate_tok, tok_ss, tok_rs, dp=dp, ep=mate)
    tok_out.start()
    own_idx.wait()
    sends = []
    for k, (d, e) in enumerate(others):
        c = remote(idx_g.at[me], idx_g.at[me], idx_ss.at[k], idx_rs.at[k], dp=d, ep=e)
        c.start()
        sends.append(c)
    rows = 2 * n_exp
    half = 2 * n_tok

    key_r = lax.broadcasted_iota(I32, (rows, rows), 0)
    key_c = lax.broadcasted_iota(I32, (rows, rows), 1)
    order_r = lax.rem(key_r, n_exp) * 2 + key_r // n_exp
    order_c = lax.rem(key_c, n_exp) * 2 + key_c // n_exp
    before = jnp.where(order_c < order_r, 1.0, 0.0).astype(BF16)
    every = jnp.ones((rows, rows), BF16)
    up_r = lax.broadcasted_iota(I32, (cap, cap), 0)
    up_c = lax.broadcasted_iota(I32, (cap, cap), 1)
    upper = jnp.where(up_r < up_c, 1.0, 0.0).astype(BF16)
    ones = jnp.ones((cap, cap), BF16)

    for c in sends:
        c.wait_recv()

    def crosses(d, h):
        ids = jnp.concatenate([idx_g[d * n_ep + 2 * h], idx_g[d * n_ep + 2 * h + 1]], axis=0)
        return ids, (ids >= half) if h == 0 else (ids < half)

    most = None
    for d in range(n_dp):
        for h in range(2):
            _, need = crosses(d, h)
            n = jnp.sum(jnp.where(need, 1.0, 0.0))
            most = n if most is None else jnp.maximum(most, n)
    pick = jnp.int32(0)
    for s in sizes[:-1]:
        pick = pick + jnp.where(most > s, 1, 0).astype(I32)
    bucket[0] = pick

    for h in range(2):
        ids, need = crosses(dp, h)
        flag = jnp.where(need, 1.0, 0.0).astype(BF16)
        in_row = jnp.dot(flag, upper, preferred_element_type=F32)
        row_sum = jnp.dot(flag, ones, preferred_element_type=F32).astype(BF16)
        prior = jnp.dot(before, row_sum, preferred_element_type=F32)
        total = jnp.dot(every, row_sum, preferred_element_type=F32)
        pos = (in_row + prior).astype(I32)
        meta[0, h * rows:(h + 1) * rows, :] = ids
        meta[1, h * rows:(h + 1) * rows, :] = jnp.where(need, pos, FAR)
        meta[2, h * rows:(h + 1) * rows, :] = jnp.where(need, pos - total.astype(I32), FAR)

    for c in sends:
        c.wait_send()
    tok_out.wait()


def layer_kernel(k_rows, tok, mate_tok, meta, gate, w_in, w_out, out,
                 chip_tok, meta_v, gate_v, xsend, land, local, xbuf, chip_p, pland, rsend, rland, tokrow,
                 acc, obuf, half_o, wi, wo,
                 loc_sem, w_sem, d_ss, d_rs, f_ss, f_rs, p_ss, p_rs, r_ss, r_rs, g_ss, g_rs, out_sem):
    n_tok, d_model = tok.shape
    n_exp, d_ff = w_in.shape[0], w_in.shape[2]
    cap = gate.shape[1]
    slots = n_exp * cap
    rows = 2 * n_exp
    nc = k_rows // (2 * cap)
    ep = lax.axis_index("ep")
    chip, core = ep // 2, ep % 2
    mate = chip * 2 + (1 - core)
    opp = (1 - chip) * 2 + core
    chip_base = chip * (2 * n_tok)

    def at(start, size):
        return pl.ds(pl.multiple_of(start, cap), size)

    def w_copies(e):
        slot = lax.rem(e, W_SLOTS)
        return (pltpu.make_async_copy(w_in.at[e], wi.at[slot], w_sem.at[0, slot]),
                pltpu.make_async_copy(w_out.at[e], wo.at[slot], w_sem.at[1, slot]))

    first = [pltpu.make_async_copy(meta, meta_v, loc_sem.at[0]),
             pltpu.make_async_copy(tok, chip_tok.at[at(core * n_tok, n_tok)], loc_sem.at[1]),
             pltpu.make_async_copy(mate_tok, chip_tok.at[at((1 - core) * n_tok, n_tok)], loc_sem.at[2]),
             pltpu.make_async_copy(gate, gate_v, loc_sem.at[3])]
    for c in first:
        c.start()
    barrier = pltpu.get_barrier_semaphore()
    signal(barrier, ep=mate)
    signal(barrier, ep=opp)
    for e in range(W_SLOTS):
        for c in w_copies(e):
            c.start()

    def d_copy(m):
        return remote(xsend.at[at(m * cap, cap)], land.at[at((2 * m + core) * cap, cap)], d_ss.at[m], d_rs.at[m], ep=opp)

    def f_copy(m):
        r = at((2 * m + core) * cap, cap)
        return remote(land.at[r], land.at[r], f_ss.at[m], f_rs.at[m], ep=mate)

    def p_copy(e):
        return remote(chip_p.at[at(core * slots + e * cap, cap)], pland.at[at(e * cap, cap)], p_ss.at[e], p_rs.at[e], ep=mate)

    def r_copy(m):
        return remote(rsend.at[at(m * cap, cap)], rland.at[at((2 * m + core) * cap, cap)], r_ss.at[m], r_rs.at[m], ep=opp)

    def g_copy(m):
        r = at((2 * m + core) * cap, cap)
        return remote(rland.at[r], rland.at[r], g_ss.at[m], g_rs.at[m], ep=mate)

    lane = lax.broadcasted_iota(I32, (cap, LANES), 1)
    sub = lax.broadcasted_iota(I32, (cap, LANES), 0)

    def spread(col, width, base):
        return jnp.concatenate(
            [jnp.where(col == lane + (base + LANES * j), 1.0, 0.0).astype(BF16) for j in range(width // LANES)], axis=1)

    def column(row):
        return jnp.broadcast_to(row, (LANES, cap)).T

    their = (1 - chip) * rows
    mine = chip * rows

    def owner_ids(kind, block, shift):
        t = jnp.zeros((cap, LANES), I32)
        for i in range(rows):
            pos = meta_v[kind, pl.ds(their + i, 1), :] + shift
            ids = meta_v[0, pl.ds(their + i, 1), :]
            t = t + jnp.where(jnp.broadcast_to(pos, (cap, LANES)) == sub + block * cap, jnp.broadcast_to(ids, (cap, LANES)), 0)
        return t

    first[0].wait()

    def gather_block(m):
        t = owner_ids(1, 2 * m + core, 0).astype(F32)
        ids = jnp.sum(t, axis=1, keepdims=True).astype(I32) - chip_base
        return spread(jnp.broadcast_to(ids, (cap, LANES)), 2 * n_tok, 0)

    with jax.named_scope('tokwait'):
        first[1].wait()
        first[2].wait()
    pl.semaphore_wait(barrier, 2)

    def send_group(m0, count):
        hot = jnp.concatenate([gather_block(m0 + k) for k in range(count)], axis=0)
        xsend[at(m0 * cap, count * cap), :] = jnp.dot(hot, chip_tok[...], preferred_element_type=F32).astype(BF16)
        for k in range(count):
            d_copy(m0 + k).start()

    @pl.loop(0, nc // 2)
    def _(g):
        send_group(2 * g, 2)

    if nc % 2:
        send_group(nc - 1, 1)

    def own_rows(g):
        with jax.named_scope("own_gather"):
            hot = jnp.concatenate(
                [spread(column(meta_v[0, pl.ds(mine + core * n_exp + 2 * g + k, 1), :] - chip_base), 2 * n_tok, 0)
                 for k in range(2)], axis=0)
            xbuf[at(2 * g * cap, 2 * cap), :] = jnp.dot(hot, chip_tok[...], preferred_element_type=F32).astype(BF16)

    def forward(m):
        with jax.named_scope("forward"):
            d_copy(m).wait_recv()
            f_copy(m).start()

    pl.loop(0, n_exp // 2)(own_rows)
    forward(0)

    @pl.loop(0, k_rows // (2 * cap))
    def _(b):
        local[at(b * 2 * cap, 2 * cap), :] = jnp.zeros((2 * cap, d_model), BF16)

    @pl.loop(0, rows // 2)
    def _(b):
        chip_p[at(b * 2 * cap, 2 * cap), :] = jnp.zeros((2 * cap, d_model), BF16)

    first[3].wait()
    f_tile = 512
    n_f = d_ff // f_tile

    def pack_return(e):
        with jax.named_scope("pwait"):
            p_copy(e).wait_recv()
        chip_p[at((1 - core) * slots + e * cap, cap), :] = pland[at(e * cap, cap), :]
        m = e - (n_exp - nc)

        @pl.when(m >= 0)
        def _():
            parts = []
            for i in range(rows):
                pos = meta_v[2, pl.ds(mine + i, 1), :] + k_rows
                parts.append(jnp.where(jnp.broadcast_to(pos, (cap, LANES)) == sub + (2 * m + core) * cap, 1.0, 0.0).astype(BF16))
            hot = jnp.concatenate(parts, axis=1)
            rsend[at(m * cap, cap), :] = jnp.dot(hot, chip_p[...], preferred_element_type=F32).astype(BF16)
            r_copy(m).start()

    @pl.loop(0, n_exp)
    def _(e):
        slot = lax.rem(e, W_SLOTS)

        @pl.when(e < nc)
        def _():
            with jax.named_scope("fwait"):
                f_copy(e).wait_recv()
            r = at(2 * e * cap, 2 * cap)
            local[r, :] = land[r, :]

        mine_e = at(e * cap, cap)
        hot = spread(column(meta_v[1, pl.ds(mine + core * n_exp + e, 1), :]), k_rows, 0)
        xbuf[mine_e, :] = xbuf[mine_e, :] + jnp.dot(hot, local[...], preferred_element_type=F32).astype(BF16)

        @pl.when(e > 0)
        def _():
            pack_return(e - 1)

        with jax.named_scope("wwait"):
            for c in w_copies(e):
                c.wait()

        def ffn(x, tiles):
            o = None
            for f in tiles:
                fs = slice(f * f_tile, (f + 1) * f_tile)
                pre = jnp.dot(x, wi[slot, :, fs], preferred_element_type=F32)
                h = jax.nn.gelu(pre, approximate=True).astype(BF16)
                part = jnp.dot(h, wo[slot, fs, :], preferred_element_type=F32)
                o = part if o is None else o + part
            return o

        half_o[...] = ffn(xbuf[mine_e, :], range(n_f // 2))

        @pl.when(e + 1 < nc)
        def _():
            forward(e + 1)

        o = half_o[...] + ffn(xbuf[mine_e, :], range(n_f // 2, n_f))
        gcol = column(gate_v[pl.ds(e, 1), :])
        chip_p[at(core * slots + e * cap, cap), :] = (jnp.concatenate([gcol] * (d_model // LANES), axis=1) * o).astype(BF16)
        with jax.named_scope("p_start"):
            p_copy(e).start()

        @pl.when(e + W_SLOTS < n_exp)
        def _():
            for c in w_copies(e + W_SLOTS):
                c.start()

        @pl.when(e < nc)
        def _():
            for k in range(2):
                t = owner_ids(2, 2 * e + k, k_rows).astype(F32).T
                tokrow[pl.ds(2 * e + k, 1), :] = jnp.sum(t, axis=0, keepdims=True).astype(I32)

    n_blk = n_tok // (2 * cap)
    blk = 2 * cap
    sub_b = lax.broadcasted_iota(I32, (blk, LANES), 0) + ep * n_tok
    early = nc - 3

    def forward_back(m):
        with jax.named_scope("rwait"):
            r_copy(m).wait_recv()
            g_copy(m).start()

    def back_wait(m):
        with jax.named_scope("gwait"):
            g_copy(m).wait_recv()

    pl.loop(0, early)(forward_back)
    with jax.named_scope("pack_last"):
        pack_return(n_exp - 1)
    pl.loop(0, early)(back_wait)

    def owners(row, b):
        return jnp.where(jnp.broadcast_to(row, (blk, LANES)) == sub_b + b * blk, 1.0, 0.0).astype(BF16)

    @pl.loop(0, n_blk)
    def _(b):
        @pl.when(b == n_blk // 2)
        def _():
            forward_back(early)

        with jax.named_scope("own_scatter"):
            hot = jnp.concatenate([owners(meta_v[0, pl.ds(mine + i, 1), :], b) for i in range(rows)], axis=1)
            hot_back = jnp.concatenate([owners(tokrow[pl.ds(i, 1), :], b) for i in range(2 * early)], axis=1)
            own = chip_tok[at(core * n_tok + b * blk, blk), :].astype(F32)
            acc[at(b * blk, blk), :] = (own + jnp.dot(hot, chip_p[...], preferred_element_type=F32)
                                        + jnp.dot(hot_back, rland[0:early * 2 * cap, :], preferred_element_type=F32))

    def combine(m, last):
        ids = [tokrow[pl.ds(2 * m + k, 1), :] for k in range(2)]
        back_wait(m)
        back = rland[at(2 * m * cap, 2 * cap), :]

        @pl.loop(0, n_blk)
        def _(b):
            r = at(b * blk, blk)
            hot = jnp.concatenate([owners(i, b) for i in ids], axis=1)
            total = acc[r, :] + jnp.dot(hot, back, preferred_element_type=F32)
            if last:
                obuf[r, :] = total.astype(BF16)
                pltpu.make_async_copy(obuf.at[r], out.at[r], out_sem.at[b]).start()
            else:
                acc[r, :] = total

    @pl.loop(early, nc - 1)
    def _(m):
        forward_back(m + 1)
        combine(m, False)

    combine(nc - 1, True)

    @pl.loop(0, nc)
    def _(m):
        d_copy(m).wait_send()
        f_copy(m).wait_send()
        r_copy(m).wait_send()
        g_copy(m).wait_send()

    @pl.loop(0, n_exp)
    def _(e):
        p_copy(e).wait_send()

    @pl.loop(0, n_blk)
    def _(b):
        r = at(b * blk, blk)
        pltpu.make_async_copy(obuf.at[r], out.at[r], out_sem.at[b]).wait()


def solution(mesh):
    n_dp, n_ep = mesh.shape["dp"], mesh.shape["ep"]
    row_spec = P(("dp", "ep"), None)
    expert_spec = P("ep", None, None)
    dma = pltpu.SemaphoreType.DMA
    any_spec = pl.BlockSpec(memory_space=pl.ANY)

    def local_layer(tok, idx, gate, w_in, w_out):
        n_tok, d_model = tok.shape
        n_exp, cap = idx.shape
        d_ff = w_in.shape[2]
        slots = n_exp * cap
        sizes = tuple(slots + i * 2 * cap for i in range(1, slots // (2 * cap) + 1))
        n_dev = n_dp * n_ep

        mate_tok, meta, bucket = pl.pallas_call(
            functools.partial(plan_kernel, n_dp, n_ep, sizes),
            out_shape=(jax.ShapeDtypeStruct((n_tok, d_model), BF16),
                       jax.ShapeDtypeStruct((3, 4 * n_exp, cap), I32),
                       jax.ShapeDtypeStruct((1,), I32)),
            in_specs=[any_spec] * 2,
            out_specs=(any_spec, pl.BlockSpec(memory_space=pltpu.VMEM), pl.BlockSpec(memory_space=pltpu.SMEM)),
            scratch_shapes=[
                pltpu.VMEM((n_dev, n_exp, cap), I32),
                dma, dma((n_dev - 1,)), dma((n_dev - 1,)), dma, dma,
            ],
            compiler_params=pltpu.CompilerParams(collective_id=0, has_side_effects=True),
        )(tok, idx)

        def branch(i):
            k_rows = sizes[i]
            nc = k_rows // (2 * cap)

            def run(tok, mate_tok, meta, gate, w_in, w_out):
                return pl.pallas_call(
                    functools.partial(layer_kernel, k_rows),
                    out_shape=jax.ShapeDtypeStruct((n_tok, d_model), BF16),
                    in_specs=[any_spec] * 6,
                    out_specs=any_spec,
                    scratch_shapes=[
                        pltpu.VMEM((2 * n_tok, d_model), BF16),
                        pltpu.VMEM((3, 4 * n_exp, cap), I32),
                        pltpu.VMEM((n_exp, cap), F32),
                        pltpu.VMEM((nc * cap, d_model), BF16),
                        pltpu.VMEM((k_rows, d_model), BF16),
                        pltpu.VMEM((k_rows, d_model), BF16),
                        pltpu.VMEM((slots, d_model), BF16),
                        pltpu.VMEM((2 * slots, d_model), BF16),
                        pltpu.VMEM((slots, d_model), BF16),
                        pltpu.VMEM((nc * cap, d_model), BF16),
                        pltpu.VMEM((k_rows, d_model), BF16),
                        pltpu.VMEM((2 * nc, cap), I32),
                        pltpu.VMEM((n_tok, d_model), F32),
                        pltpu.VMEM((n_tok, d_model), BF16),
                        pltpu.VMEM((cap, d_model), F32),
                        pltpu.VMEM((W_SLOTS, d_model, d_ff), BF16),
                        pltpu.VMEM((W_SLOTS, d_ff, d_model), BF16),
                        dma((4,)), dma((2, W_SLOTS)),
                        dma((nc,)), dma((nc,)), dma((nc,)), dma((nc,)),
                        dma((n_exp,)), dma((n_exp,)),
                        dma((nc,)), dma((nc,)), dma((nc,)), dma((nc,)),
                        dma((n_tok // (2 * cap),)),
                    ],
                    compiler_params=pltpu.CompilerParams(
                        collective_id=1 + i, has_side_effects=True, vmem_limit_bytes=63 * 1024 * 1024),
                )(tok, mate_tok, meta, gate, w_in, w_out)

            return run

        return lax.switch(bucket[0], [branch(i) for i in range(len(sizes))], tok, mate_tok, meta, gate, w_in, w_out)

    return jax.shard_map(local_layer, mesh=mesh, in_specs=(row_spec, row_spec, row_spec, expert_spec, expert_spec),
                         out_specs=row_spec, check_vma=False)
```

```python
import functools

import jax
import jax.numpy as jnp
from jax import lax
from jax.experimental import pallas as pl
from jax.experimental.pallas import tpu as pltpu
from jax.sharding import PartitionSpec as P

F32, BF16, I32 = jnp.float32, jnp.bfloat16, jnp.int32
W_SLOTS = 3
LANES = 128
FAR = 1 << 20


def remote(src, dst, ss, rs, **dev):
    return pltpu.make_async_remote_copy(src_ref=src, dst_ref=dst, send_sem=ss, recv_sem=rs,
                                        device_id=dev, device_id_type=pl.DeviceIdType.MESH)


def signal(sem, **dev):
    pl.semaphore_signal(sem, inc=1, device_id=dev, device_id_type=pl.DeviceIdType.MESH)


def plan_kernel(n_dp, n_ep, sizes, tok, idx, chip_tok, meta, bucket, idx_g, loc_sem, idx_ss, idx_rs, tok_ss, tok_rs):
    n_tok = tok.shape[0]
    n_exp, cap = idx.shape
    dp, ep = lax.axis_index("dp"), lax.axis_index("ep")
    me = dp * n_ep + ep
    n_dev = n_dp * n_ep
    core = lax.rem(ep, 2)
    own_rows = chip_tok.at[pl.ds(pl.multiple_of(core * n_tok, n_tok), n_tok)]
    own_idx = pltpu.make_async_copy(idx, idx_g.at[me], loc_sem.at[0])
    own_tok = pltpu.make_async_copy(tok, own_rows, loc_sem.at[1])
    own_idx.start()
    own_tok.start()
    barrier = pltpu.get_barrier_semaphore()
    others = []
    for k in range(1, n_dev):
        dev = lax.rem(me + k, n_dev)
        others.append((dev // n_ep, lax.rem(dev, n_ep)))
    for d, e in others:
        signal(barrier, dp=d, ep=e)
    pl.semaphore_wait(barrier, n_dev - 1)
    own_idx.wait()
    sends = []
    for k, (d, e) in enumerate(others):
        c = remote(idx_g.at[me], idx_g.at[me], idx_ss.at[k], idx_rs.at[k], dp=d, ep=e)
        c.start()
        sends.append(c)
    own_tok.wait()
    tok_out = remote(own_rows, own_rows, tok_ss, tok_rs, dp=dp, ep=ep + 1 - 2 * core)
    tok_out.start()
    rows = 2 * n_exp
    half = 2 * n_tok

    key_r = lax.broadcasted_iota(I32, (rows, rows), 0)
    key_c = lax.broadcasted_iota(I32, (rows, rows), 1)
    order_r = lax.rem(key_r, n_exp) * 2 + key_r // n_exp
    order_c = lax.rem(key_c, n_exp) * 2 + key_c // n_exp
    before = jnp.where(order_c < order_r, 1.0, 0.0).astype(BF16)
    every = jnp.ones((rows, rows), BF16)
    up_r = lax.broadcasted_iota(I32, (cap, cap), 0)
    up_c = lax.broadcasted_iota(I32, (cap, cap), 1)
    upper = jnp.where(up_r < up_c, 1.0, 0.0).astype(BF16)
    ones = jnp.ones((cap, cap), BF16)

    for c in sends:
        c.wait_recv()

    def crosses(d, h):
        ids = jnp.concatenate([idx_g[d * n_ep + 2 * h], idx_g[d * n_ep + 2 * h + 1]], axis=0)
        return ids, (ids >= half) if h == 0 else (ids < half)

    most = None
    for d in range(n_dp):
        for h in range(2):
            _, need = crosses(d, h)
            n = jnp.sum(jnp.where(need, 1.0, 0.0))
            most = n if most is None else jnp.maximum(most, n)
    pick = jnp.int32(0)
    for s in sizes[:-1]:
        pick = pick + jnp.where(most > s, 1, 0).astype(I32)
    bucket[0] = pick

    for h in range(2):
        ids, need = crosses(dp, h)
        flag = jnp.where(need, 1.0, 0.0).astype(BF16)
        in_row = jnp.dot(flag, upper, preferred_element_type=F32)
        row_sum = jnp.dot(flag, ones, preferred_element_type=F32).astype(BF16)
        prior = jnp.dot(before, row_sum, preferred_element_type=F32)
        total = jnp.dot(every, row_sum, preferred_element_type=F32)
        pos = (in_row + prior).astype(I32)
        meta[0, h * rows:(h + 1) * rows, :] = ids
        meta[1, h * rows:(h + 1) * rows, :] = jnp.where(need, pos, FAR)
        meta[2, h * rows:(h + 1) * rows, :] = jnp.where(need, pos - total.astype(I32), FAR)

    for c in sends:
        c.wait_send()
    tok_out.wait()


def layer_kernel(k_rows, chip_tok, meta_v, gate_v, w_in, w_out, out,
                 xsend, land, local, xbuf, chip_p, pland, rsend, rland, tokrow,
                 acc, half_o, wi, wo,
                 w_sem, d_ss, d_rs, f_ss, f_rs, p_ss, p_rs, r_ss, r_rs, g_ss, g_rs):
    n_tok, d_model = out.shape
    n_exp, d_ff = w_in.shape[0], w_in.shape[2]
    cap = gate_v.shape[1]
    slots = n_exp * cap
    rows = 2 * n_exp
    nc = k_rows // (2 * cap)
    ep = lax.axis_index("ep")
    chip, core = ep // 2, ep % 2
    mate = chip * 2 + (1 - core)
    opp = (1 - chip) * 2 + core
    chip_base = chip * (2 * n_tok)

    def at(start, size):
        return pl.ds(pl.multiple_of(start, cap), size)

    def w_copies(e):
        slot = lax.rem(e, W_SLOTS)
        return (pltpu.make_async_copy(w_in.at[e], wi.at[slot], w_sem.at[0, slot]),
                pltpu.make_async_copy(w_out.at[e], wo.at[slot], w_sem.at[1, slot]))

    barrier = pltpu.get_barrier_semaphore()
    signal(barrier, ep=mate)
    signal(barrier, ep=opp)
    for e in range(W_SLOTS):
        for c in w_copies(e):
            c.start()

    def d_copy(m):
        return remote(xsend.at[at(m * cap, cap)], land.at[at((2 * m + core) * cap, cap)], d_ss.at[m], d_rs.at[m], ep=opp)

    def f_copy(m):
        r = at((2 * m + core) * cap, cap)
        return remote(land.at[r], land.at[r], f_ss.at[m], f_rs.at[m], ep=mate)

    def p_copy(e):
        return remote(chip_p.at[at(core * slots + e * cap, cap)], pland.at[at(e * cap, cap)], p_ss.at[e], p_rs.at[e], ep=mate)

    def r_copy(m):
        return remote(rsend.at[at(m * cap, cap)], rland.at[at((2 * m + core) * cap, cap)], r_ss.at[m], r_rs.at[m], ep=opp)

    def g_copy(m):
        r = at((2 * m + core) * cap, cap)
        return remote(rland.at[r], rland.at[r], g_ss.at[m], g_rs.at[m], ep=mate)

    lane = lax.broadcasted_iota(I32, (cap, LANES), 1)
    sub = lax.broadcasted_iota(I32, (cap, LANES), 0)

    def spread(col, width, base):
        return jnp.concatenate(
            [jnp.where(col == lane + (base + LANES * j), 1.0, 0.0).astype(BF16) for j in range(width // LANES)], axis=1)

    def column(row):
        return jnp.broadcast_to(row, (LANES, cap)).T

    their = (1 - chip) * rows
    mine = chip * rows

    def owner_ids(kind, block, shift):
        t = jnp.zeros((cap, LANES), I32)
        for i in range(rows):
            pos = meta_v[kind, pl.ds(their + i, 1), :] + shift
            ids = meta_v[0, pl.ds(their + i, 1), :]
            t = t + jnp.where(jnp.broadcast_to(pos, (cap, LANES)) == sub + block * cap, jnp.broadcast_to(ids, (cap, LANES)), 0)
        return t

    def gather_block(m):
        t = owner_ids(1, 2 * m + core, 0).astype(F32)
        ids = jnp.sum(t, axis=1, keepdims=True).astype(I32) - chip_base
        return spread(jnp.broadcast_to(ids, (cap, LANES)), 2 * n_tok, 0)

    pl.semaphore_wait(barrier, 2)

    def send_group(m0, count):
        hot = jnp.concatenate([gather_block(m0 + k) for k in range(count)], axis=0)
        xsend[at(m0 * cap, count * cap), :] = jnp.dot(hot, chip_tok[...], preferred_element_type=F32).astype(BF16)
        for k in range(count):
            d_copy(m0 + k).start()

    @pl.loop(0, nc // 2)
    def _(g):
        send_group(2 * g, 2)

    if nc % 2:
        send_group(nc - 1, 1)

    def own_rows(g):
        with jax.named_scope("own_gather"):
            hot = jnp.concatenate(
                [spread(column(meta_v[0, pl.ds(mine + core * n_exp + 2 * g + k, 1), :] - chip_base), 2 * n_tok, 0)
                 for k in range(2)], axis=0)
            xbuf[at(2 * g * cap, 2 * cap), :] = jnp.dot(hot, chip_tok[...], preferred_element_type=F32).astype(BF16)

    def forward(m):
        with jax.named_scope("forward"):
            d_copy(m).wait_recv()
            f_copy(m).start()

    pl.loop(0, n_exp // 2)(own_rows)
    forward(0)

    @pl.loop(0, k_rows // (2 * cap))
    def _(b):
        local[at(b * 2 * cap, 2 * cap), :] = jnp.zeros((2 * cap, d_model), BF16)

    @pl.loop(0, rows // 2)
    def _(b):
        chip_p[at(b * 2 * cap, 2 * cap), :] = jnp.zeros((2 * cap, d_model), BF16)

    f_tile = 512
    n_f = d_ff // f_tile

    def pack_return(e):
        with jax.named_scope("pwait"):
            p_copy(e).wait_recv()
        chip_p[at((1 - core) * slots + e * cap, cap), :] = pland[at(e * cap, cap), :]
        m = e - (n_exp - nc)

        @pl.when(m >= 0)
        def _():
            parts = []
            for i in range(rows):
                pos = meta_v[2, pl.ds(mine + i, 1), :] + k_rows
                parts.append(jnp.where(jnp.broadcast_to(pos, (cap, LANES)) == sub + (2 * m + core) * cap, 1.0, 0.0).astype(BF16))
            hot = jnp.concatenate(parts, axis=1)
            rsend[at(m * cap, cap), :] = jnp.dot(hot, chip_p[...], preferred_element_type=F32).astype(BF16)
            r_copy(m).start()

    @pl.loop(0, n_exp)
    def _(e):
        slot = lax.rem(e, W_SLOTS)

        @pl.when(e < nc)
        def _():
            with jax.named_scope("fwait"):
                f_copy(e).wait_recv()
            r = at(2 * e * cap, 2 * cap)
            local[r, :] = land[r, :]

        mine_e = at(e * cap, cap)
        hot = spread(column(meta_v[1, pl.ds(mine + core * n_exp + e, 1), :]), k_rows, 0)
        xbuf[mine_e, :] = xbuf[mine_e, :] + jnp.dot(hot, local[...], preferred_element_type=F32).astype(BF16)

        @pl.when(e > 0)
        def _():
            pack_return(e - 1)

        with jax.named_scope("wwait"):
            for c in w_copies(e):
                c.wait()

        def ffn(x, tiles):
            o = None
            for f in tiles:
                fs = slice(f * f_tile, (f + 1) * f_tile)
                pre = jnp.dot(x, wi[slot, :, fs], preferred_element_type=F32)
                h = jax.nn.gelu(pre, approximate=True).astype(BF16)
                part = jnp.dot(h, wo[slot, fs, :], preferred_element_type=F32)
                o = part if o is None else o + part
            return o

        half_o[...] = ffn(xbuf[mine_e, :], range(n_f // 2))

        @pl.when(e + 1 < nc)
        def _():
            forward(e + 1)

        o = half_o[...] + ffn(xbuf[mine_e, :], range(n_f // 2, n_f))
        gcol = column(gate_v[pl.ds(e, 1), :])
        chip_p[at(core * slots + e * cap, cap), :] = (jnp.concatenate([gcol] * (d_model // LANES), axis=1) * o).astype(BF16)
        with jax.named_scope("p_start"):
            p_copy(e).start()

        @pl.when(e + W_SLOTS < n_exp)
        def _():
            for c in w_copies(e + W_SLOTS):
                c.start()

        @pl.when(e < nc)
        def _():
            for k in range(2):
                t = owner_ids(2, 2 * e + k, k_rows).astype(F32).T
                tokrow[pl.ds(2 * e + k, 1), :] = jnp.sum(t, axis=0, keepdims=True).astype(I32)

    n_blk = n_tok // (2 * cap)
    blk = 2 * cap
    sub_b = lax.broadcasted_iota(I32, (blk, LANES), 0) + ep * n_tok
    early = nc - 3

    def forward_back(m):
        with jax.named_scope("rwait"):
            r_copy(m).wait_recv()
            g_copy(m).start()

    def back_wait(m):
        with jax.named_scope("gwait"):
            g_copy(m).wait_recv()

    pl.loop(0, early)(forward_back)
    with jax.named_scope("pack_last"):
        pack_return(n_exp - 1)
    pl.loop(0, early)(back_wait)

    def owners(row, b):
        return jnp.where(jnp.broadcast_to(row, (blk, LANES)) == sub_b + b * blk, 1.0, 0.0).astype(BF16)

    @pl.loop(0, n_blk)
    def _(b):
        @pl.when(b == n_blk // 2)
        def _():
            forward_back(early)

        with jax.named_scope("own_scatter"):
            hot = jnp.concatenate([owners(meta_v[0, pl.ds(mine + i, 1), :], b) for i in range(rows)], axis=1)
            hot_back = jnp.concatenate([owners(tokrow[pl.ds(i, 1), :], b) for i in range(2 * early)], axis=1)
            own = chip_tok[at(core * n_tok + b * blk, blk), :].astype(F32)
            acc[at(b * blk, blk), :] = (own + jnp.dot(hot, chip_p[...], preferred_element_type=F32)
                                        + jnp.dot(hot_back, rland[0:early * 2 * cap, :], preferred_element_type=F32))

    def combine(m, last):
        ids = [tokrow[pl.ds(2 * m + k, 1), :] for k in range(2)]
        back_wait(m)
        back = rland[at(2 * m * cap, 2 * cap), :]

        @pl.loop(0, n_blk)
        def _(b):
            r = at(b * blk, blk)
            hot = jnp.concatenate([owners(i, b) for i in ids], axis=1)
            total = acc[r, :] + jnp.dot(hot, back, preferred_element_type=F32)
            if last:
                out[r, :] = total.astype(BF16)
            else:
                acc[r, :] = total

    @pl.loop(early, nc - 1)
    def _(m):
        forward_back(m + 1)
        combine(m, False)

    combine(nc - 1, True)

    @pl.loop(0, nc)
    def _(m):
        d_copy(m).wait_send()
        f_copy(m).wait_send()
        r_copy(m).wait_send()
        g_copy(m).wait_send()

    @pl.loop(0, n_exp)
    def _(e):
        p_copy(e).wait_send()


def solution(mesh):
    n_dp, n_ep = mesh.shape["dp"], mesh.shape["ep"]
    row_spec = P(("dp", "ep"), None)
    expert_spec = P("ep", None, None)
    dma = pltpu.SemaphoreType.DMA
    any_spec = pl.BlockSpec(memory_space=pl.ANY)
    vmem_spec = pl.BlockSpec(memory_space=pltpu.VMEM)

    def local_layer(tok, idx, gate, w_in, w_out):
        n_tok, d_model = tok.shape
        n_exp, cap = idx.shape
        d_ff = w_in.shape[2]
        slots = n_exp * cap
        sizes = tuple(slots + i * 2 * cap for i in range(1, slots // (2 * cap) + 1))
        n_dev = n_dp * n_ep

        chip_tok, meta, bucket = pl.pallas_call(
            functools.partial(plan_kernel, n_dp, n_ep, sizes),
            out_shape=(jax.ShapeDtypeStruct((2 * n_tok, d_model), BF16),
                       jax.ShapeDtypeStruct((3, 4 * n_exp, cap), I32),
                       jax.ShapeDtypeStruct((1,), I32)),
            in_specs=[any_spec] * 2,
            out_specs=(vmem_spec, vmem_spec, pl.BlockSpec(memory_space=pltpu.SMEM)),
            scratch_shapes=[
                pltpu.VMEM((n_dev, n_exp, cap), I32),
                dma((2,)), dma((n_dev - 1,)), dma((n_dev - 1,)), dma, dma,
            ],
            compiler_params=pltpu.CompilerParams(
                collective_id=0, has_side_effects=True, vmem_limit_bytes=60 * 1024 * 1024),
        )(tok, idx)

        def branch(i):
            k_rows = sizes[i]
            nc = k_rows // (2 * cap)

            def run(chip_tok, meta, gate, w_in, w_out):
                return pl.pallas_call(
                    functools.partial(layer_kernel, k_rows),
                    out_shape=jax.ShapeDtypeStruct((n_tok, d_model), BF16),
                    in_specs=[vmem_spec] * 3 + [any_spec] * 2,
                    out_specs=vmem_spec,
                    scratch_shapes=[
                        pltpu.VMEM((nc * cap, d_model), BF16),
                        pltpu.VMEM((k_rows, d_model), BF16),
                        pltpu.VMEM((k_rows, d_model), BF16),
                        pltpu.VMEM((slots, d_model), BF16),
                        pltpu.VMEM((2 * slots, d_model), BF16),
                        pltpu.VMEM((slots, d_model), BF16),
                        pltpu.VMEM((nc * cap, d_model), BF16),
                        pltpu.VMEM((k_rows, d_model), BF16),
                        pltpu.VMEM((2 * nc, cap), I32),
                        pltpu.VMEM((n_tok, d_model), F32),
                        pltpu.VMEM((cap, d_model), F32),
                        pltpu.VMEM((W_SLOTS, d_model, d_ff), BF16),
                        pltpu.VMEM((W_SLOTS, d_ff, d_model), BF16),
                        dma((2, W_SLOTS)),
                        dma((nc,)), dma((nc,)), dma((nc,)), dma((nc,)),
                        dma((n_exp,)), dma((n_exp,)),
                        dma((nc,)), dma((nc,)), dma((nc,)), dma((nc,)),
                    ],
                    compiler_params=pltpu.CompilerParams(
                        collective_id=1 + i, has_side_effects=True, vmem_limit_bytes=58 * 1024 * 1024),
                )(chip_tok, meta, gate, w_in, w_out)

            return run

        return lax.switch(bucket[0], [branch(i) for i in range(len(sizes))], chip_tok, meta, gate, w_in, w_out)

    return jax.shard_map(local_layer, mesh=mesh, in_specs=(row_spec, row_spec, row_spec, expert_spec, expert_spec),
                         out_specs=row_spec, check_vma=False)
```

```python
import functools

import jax
import jax.numpy as jnp
from jax import lax
from jax.experimental import pallas as pl
from jax.experimental.pallas import tpu as pltpu
from jax.sharding import PartitionSpec as P

F32, BF16, I32 = jnp.float32, jnp.bfloat16, jnp.int32
W_SLOTS = 3
LANES = 128
FAR = 1 << 20
LENGTHS = (2, 3, 4, 6, 8)


def remote(src, dst, ss, rs, **dev):
    return pltpu.make_async_remote_copy(src_ref=src, dst_ref=dst, send_sem=ss, recv_sem=rs,
                                        device_id=dev, device_id_type=pl.DeviceIdType.MESH)


def signal(sem, **dev):
    pl.semaphore_signal(sem, inc=1, device_id=dev, device_id_type=pl.DeviceIdType.MESH)


def spread(col, width, lane):
    return jnp.concatenate(
        [jnp.where(col == lane + LANES * j, 1.0, 0.0).astype(BF16) for j in range(width // LANES)], axis=1)


def column(row, cap):
    return jnp.broadcast_to(row, (LANES, cap)).T


def plan_kernel(n_dp, n_ep, sizes, tok, idx, chip_tok, xown, meta, bucket, idx_g, loc_sem, idx_ss, idx_rs, tok_ss, tok_rs):
    n_tok = tok.shape[0]
    n_exp, cap = idx.shape
    dp, ep = lax.axis_index("dp"), lax.axis_index("ep")
    me = dp * n_ep + ep
    n_dev = n_dp * n_ep
    core = lax.rem(ep, 2)
    own_rows = chip_tok.at[pl.ds(pl.multiple_of(core * n_tok, n_tok), n_tok)]
    own_idx = pltpu.make_async_copy(idx, idx_g.at[me], loc_sem.at[0])
    own_tok = pltpu.make_async_copy(tok, own_rows, loc_sem.at[1])
    own_idx.start()
    own_tok.start()
    barrier = pltpu.get_barrier_semaphore()
    others = []
    for k in range(1, n_dev):
        dev = lax.rem(me + k, n_dev)
        others.append((dev // n_ep, lax.rem(dev, n_ep)))
    for d, e in others:
        signal(barrier, dp=d, ep=e)
    pl.semaphore_wait(barrier, n_dev - 1)
    own_idx.wait()
    sends = []
    for k, (d, e) in enumerate(others):
        c = remote(idx_g.at[me], idx_g.at[me], idx_ss.at[k], idx_rs.at[k], dp=d, ep=e)
        c.start()
        sends.append(c)
    own_tok.wait()
    tok_out = remote(own_rows, own_rows, tok_ss, tok_rs, dp=dp, ep=ep + 1 - 2 * core)
    tok_out.start()
    lane = lax.broadcasted_iota(I32, (cap, LANES), 1)

    @pl.loop(0, n_exp // 2)
    def _(g):
        hot = jnp.concatenate(
            [spread(column(idx_g[me, pl.ds(2 * g + k, 1), :] - ep * n_tok, cap), n_tok, lane) for k in range(2)], axis=0)
        xown[pl.ds(pl.multiple_of(2 * g * cap, 2 * cap), 2 * cap), :] = jnp.dot(
            hot, own_rows[...], preferred_element_type=F32).astype(BF16)

    rows = 2 * n_exp
    half = 2 * n_tok

    key_r = lax.broadcasted_iota(I32, (rows, rows), 0)
    key_c = lax.broadcasted_iota(I32, (rows, rows), 1)
    order_r = lax.rem(key_r, n_exp) * 2 + key_r // n_exp
    order_c = lax.rem(key_c, n_exp) * 2 + key_c // n_exp
    before = jnp.where(order_c < order_r, 1.0, 0.0).astype(BF16)
    every = jnp.ones((rows, rows), BF16)
    up_r = lax.broadcasted_iota(I32, (cap, cap), 0)
    up_c = lax.broadcasted_iota(I32, (cap, cap), 1)
    upper = jnp.where(up_r < up_c, 1.0, 0.0).astype(BF16)
    ones = jnp.ones((cap, cap), BF16)

    for c in sends:
        c.wait_recv()

    def crosses(d, h):
        ids = jnp.concatenate([idx_g[d * n_ep + 2 * h], idx_g[d * n_ep + 2 * h + 1]], axis=0)
        return ids, (ids >= half) if h == 0 else (ids < half)

    most = None
    for d in range(n_dp):
        for h in range(2):
            _, need = crosses(d, h)
            n = jnp.sum(jnp.where(need, 1.0, 0.0))
            most = n if most is None else jnp.maximum(most, n)
    pick = jnp.int32(0)
    for s in sizes[:-1]:
        pick = pick + jnp.where(most > s, 1, 0).astype(I32)
    bucket[0] = pick

    for h in range(2):
        ids, need = crosses(dp, h)
        flag = jnp.where(need, 1.0, 0.0).astype(BF16)
        in_row = jnp.dot(flag, upper, preferred_element_type=F32)
        row_sum = jnp.dot(flag, ones, preferred_element_type=F32).astype(BF16)
        prior = jnp.dot(before, row_sum, preferred_element_type=F32)
        total = jnp.dot(every, row_sum, preferred_element_type=F32)
        pos = (in_row + prior).astype(I32)
        meta[0, h * rows:(h + 1) * rows, :] = ids
        meta[1, h * rows:(h + 1) * rows, :] = jnp.where(need, pos, FAR)
        meta[2, h * rows:(h + 1) * rows, :] = jnp.where(need, pos - total.astype(I32), FAR)

    for c in sends:
        c.wait_send()
    tok_out.wait()


def layer_kernel(k_rows, chip_tok, xown, meta_v, gate_v, w_in, w_out, out,
                 xsend, land, local, xbuf, chip_p, pland, rsend, rland, tokrow, acc, sum_o, wi, wo,
                 w_sem, d_ss, d_rs, f_ss, f_rs, p_ss, p_rs, r_ss, r_rs, g_ss, g_rs):
    n_tok, d_model = out.shape
    n_exp, d_ff = w_in.shape[0], w_in.shape[2]
    cap = gate_v.shape[1]
    slots = n_exp * cap
    rows = 2 * n_exp
    n_list = k_rows // cap
    odd = n_list % 2
    nc = (n_list + 1) // 2
    ep = lax.axis_index("ep")
    chip, core = ep // 2, ep % 2
    mate = chip * 2 + (1 - core)
    opp = (1 - chip) * 2 + core
    chip_base = chip * (2 * n_tok)

    def at(start, size):
        return pl.ds(pl.multiple_of(start, cap), size)

    def w_copies(e):
        slot = lax.rem(e, W_SLOTS)
        return (pltpu.make_async_copy(w_in.at[e], wi.at[slot], w_sem.at[0, slot]),
                pltpu.make_async_copy(w_out.at[e], wo.at[slot], w_sem.at[1, slot]))

    barrier = pltpu.get_barrier_semaphore()
    signal(barrier, ep=mate)
    signal(barrier, ep=opp)
    for e in range(W_SLOTS):
        for c in w_copies(e):
            c.start()

    def d_copy(m):
        return remote(xsend.at[at(m * cap, cap)], land.at[at((2 * m + core) * cap, cap)], d_ss.at[m], d_rs.at[m], ep=opp)

    def f_copy(m):
        r = at((2 * m + core) * cap, cap)
        return remote(land.at[r], land.at[r], f_ss.at[m], f_rs.at[m], ep=mate)

    def p_copy(e):
        return remote(chip_p.at[at(core * slots + e * cap, cap)], pland.at[at(e * cap, cap)], p_ss.at[e], p_rs.at[e], ep=mate)

    def r_copy(m):
        return remote(rsend.at[at(m * cap, cap)], rland.at[at((2 * m + core) * cap, cap)], r_ss.at[m], r_rs.at[m], ep=opp)

    def g_copy(m):
        r = at((2 * m + core) * cap, cap)
        return remote(rland.at[r], rland.at[r], g_ss.at[m], g_rs.at[m], ep=mate)

    def if_mine(m, f):
        if odd:
            pl.when(2 * m + core < n_list)(f)
        else:
            f()

    def if_mates(m, f):
        if odd:
            pl.when(2 * m + 1 - core < n_list)(f)
        else:
            f()

    lane = lax.broadcasted_iota(I32, (cap, LANES), 1)
    sub = lax.broadcasted_iota(I32, (cap, LANES), 0)
    their = (1 - chip) * rows
    mine = chip * rows

    def owner_ids(kind, block, shift):
        t = jnp.zeros((cap, LANES), I32)
        for i in range(rows):
            pos = meta_v[kind, pl.ds(their + i, 1), :] + shift
            ids = meta_v[0, pl.ds(their + i, 1), :]
            t = t + jnp.where(jnp.broadcast_to(pos, (cap, LANES)) == sub + block * cap, jnp.broadcast_to(ids, (cap, LANES)), 0)
        return t

    def gather_block(m):
        t = owner_ids(1, 2 * m + core, 0).astype(F32)
        ids = jnp.sum(t, axis=1, keepdims=True).astype(I32) - chip_base
        return spread(jnp.broadcast_to(ids, (cap, LANES)), 2 * n_tok, lane)

    @pl.loop(0, (nc + 1) // 2)
    def _(g):
        with jax.named_scope("send_group"):
            hot = jnp.concatenate([gather_block(2 * g + k) for k in range(2)], axis=0)
            xsend[at(2 * g * cap, 2 * cap), :] = jnp.dot(hot, chip_tok[...], preferred_element_type=F32).astype(BF16)

        @pl.when(g == 0)
        def _():
            pl.semaphore_wait(barrier, 2)

        for k in range(2):
            pl.when(2 * (2 * g + k) + core < n_list)(lambda k=k: d_copy(2 * g + k).start())

    mate_rows = at((1 - core) * n_tok, n_tok)

    @pl.loop(0, n_exp // 2)
    def _(g):
        with jax.named_scope("own_gather"):
            hot = jnp.concatenate(
                [spread(column(meta_v[0, pl.ds(mine + core * n_exp + 2 * g + k, 1), :] - mate * n_tok, cap), n_tok, lane)
                 for k in range(2)], axis=0)
            r = at(2 * g * cap, 2 * cap)
            xbuf[r, :] = xown[r, :] + jnp.dot(hot, chip_tok[mate_rows, :], preferred_element_type=F32).astype(BF16)

    @pl.loop(0, nc)
    def _(b):
        local[at(b * 2 * cap, 2 * cap), :] = jnp.zeros((2 * cap, d_model), BF16)

    @pl.loop(0, n_exp)
    def _(b):
        chip_p[at(b * 2 * cap, 2 * cap), :] = jnp.zeros((2 * cap, d_model), BF16)

    def forward(m):
        def go():
            with jax.named_scope("forward"):
                d_copy(m).wait_recv()
                f_copy(m).start()

        if_mine(m, go)

    forward(0)
    f_tile = 512
    n_f = d_ff // f_tile

    def pack_return(e):
        with jax.named_scope("pwait"):
            p_copy(e).wait_recv()
        chip_p[at((1 - core) * slots + e * cap, cap), :] = pland[at(e * cap, cap), :]
        m = e - (n_exp - nc) - (core if odd else 0)

        @pl.when(m >= 0)
        def _():
            parts = []
            for i in range(rows):
                pos = meta_v[2, pl.ds(mine + i, 1), :] + k_rows
                parts.append(jnp.where(jnp.broadcast_to(pos, (cap, LANES)) == sub + (2 * m + core) * cap, 1.0, 0.0).astype(BF16))
            hot = jnp.concatenate(parts, axis=1)
            rsend[at(m * cap, cap), :] = jnp.dot(hot, chip_p[...], preferred_element_type=F32).astype(BF16)
            r_copy(m).start()

    @pl.loop(0, n_exp)
    def _(e):
        slot = lax.rem(e, W_SLOTS)

        @pl.when(e < nc)
        def _():
            def go():
                with jax.named_scope("fwait"):
                    f_copy(e).wait_recv()

            if_mates(e, go)
            for k in range(2):
                @pl.when(2 * e + k < n_list)
                def _():
                    r = at((2 * e + k) * cap, cap)
                    local[r, :] = land[r, :]

        mine_e = at(e * cap, cap)
        hot = spread(column(meta_v[1, pl.ds(mine + core * n_exp + e, 1), :], cap), k_rows, lane)
        xbuf[mine_e, :] = xbuf[mine_e, :] + jnp.dot(hot, local[0:k_rows, :], preferred_element_type=F32).astype(BF16)

        with jax.named_scope("wwait"):
            for c in w_copies(e):
                c.wait()

        sum_o[...] = jnp.zeros((cap, d_model), F32)

        @pl.loop(0, 2)
        def _(half):
            x = xbuf[mine_e, :]
            o = None
            for f in range(n_f // 2):
                fs = at(half * (d_ff // 2) + f * f_tile, f_tile)
                pre = jnp.dot(x, wi[slot, :, fs], preferred_element_type=F32)
                h = jax.nn.gelu(pre, approximate=True).astype(BF16)
                part = jnp.dot(h, wo[slot, fs, :], preferred_element_type=F32)
                o = part if o is None else o + part
            sum_o[...] = sum_o[...] + o

            @pl.when((half == 0) & (e > 0))
            def _():
                pack_return(e - 1)

            @pl.when((half == 0) & (e + 1 < nc))
            def _():
                forward(e + 1)

        gcol = column(gate_v[pl.ds(e, 1), :], cap)
        chip_p[at(core * slots + e * cap, cap), :] = (
            jnp.concatenate([gcol] * (d_model // LANES), axis=1) * sum_o[...]).astype(BF16)
        p_copy(e).start()

        @pl.when(e + W_SLOTS < n_exp)
        def _():
            for c in w_copies(e + W_SLOTS):
                c.start()

        @pl.when(e < nc)
        def _():
            with jax.named_scope("tokrow"):
                for k in range(2):
                    t = owner_ids(2, 2 * e + k, k_rows).astype(F32).T
                    tokrow[pl.ds(2 * e + k, 1), :] = jnp.sum(t, axis=0, keepdims=True).astype(I32)

    n_blk = n_tok // (2 * cap)
    blk = 2 * cap
    sub_b = lax.broadcasted_iota(I32, (blk, LANES), 0) + ep * n_tok
    early = nc - 3

    def forward_back(m):
        def go():
            with jax.named_scope("rwait"):
                r_copy(m).wait_recv()
                g_copy(m).start()

        if_mine(m, go)

    def back_wait(m):
        def go():
            with jax.named_scope("gwait"):
                g_copy(m).wait_recv()

        if_mates(m, go)

    pl.loop(0, early)(forward_back)
    pl.loop(0, early)(back_wait)

    def owners(row, b):
        return jnp.where(jnp.broadcast_to(row, (blk, LANES)) == sub_b + b * blk, 1.0, 0.0).astype(BF16)

    @pl.loop(0, n_blk)
    def _(b):
        with jax.named_scope("early_back"):
            hot = jnp.concatenate([owners(tokrow[pl.ds(i, 1), :], b) for i in range(2 * early)], axis=1)
            own = chip_tok[at(core * n_tok + b * blk, blk), :].astype(F32)
            acc[at(b * blk, blk), :] = own + jnp.dot(hot, rland[0:early * 2 * cap, :], preferred_element_type=F32)

    with jax.named_scope("pack_last"):
        pack_return(n_exp - 1)

    @pl.loop(0, n_blk)
    def _(b):
        @pl.when(b == n_blk // 2)
        def _():
            forward_back(early)

        with jax.named_scope("own_scatter"):
            r = at(b * blk, blk)
            hot = jnp.concatenate([owners(meta_v[0, pl.ds(mine + i, 1), :], b) for i in range(rows)], axis=1)
            acc[r, :] = acc[r, :] + jnp.dot(hot, chip_p[...], preferred_element_type=F32)

    def combine(m, last):
        n_in = 1 if last and odd else 2
        ids = [tokrow[pl.ds(2 * m + k, 1), :] for k in range(n_in)]
        back_wait(m)
        back = rland[at(2 * m * cap, n_in * cap), :]

        @pl.loop(0, n_blk)
        def _(b):
            r = at(b * blk, blk)
            hot = jnp.concatenate([owners(i, b) for i in ids], axis=1)
            total = acc[r, :] + jnp.dot(hot, back, preferred_element_type=F32)
            if last:
                out[r, :] = total.astype(BF16)
            else:
                acc[r, :] = total

    @pl.loop(early, nc - 1)
    def _(m):
        forward_back(m + 1)
        combine(m, False)

    combine(nc - 1, True)

    @pl.loop(0, nc)
    def _(m):
        def go():
            d_copy(m).wait_send()
            f_copy(m).wait_send()
            r_copy(m).wait_send()
            g_copy(m).wait_send()

        if_mine(m, go)

    @pl.loop(0, n_exp)
    def _(e):
        p_copy(e).wait_send()


def solution(mesh):
    n_dp, n_ep = mesh.shape["dp"], mesh.shape["ep"]
    row_spec = P(("dp", "ep"), None)
    expert_spec = P("ep", None, None)
    dma = pltpu.SemaphoreType.DMA
    any_spec = pl.BlockSpec(memory_space=pl.ANY)
    vmem_spec = pl.BlockSpec(memory_space=pltpu.VMEM)

    def local_layer(tok, idx, gate, w_in, w_out):
        n_tok, d_model = tok.shape
        n_exp, cap = idx.shape
        d_ff = w_in.shape[2]
        slots = n_exp * cap
        sizes = tuple(slots + i * cap for i in LENGTHS)
        n_dev = n_dp * n_ep

        chip_tok, xown, meta, bucket = pl.pallas_call(
            functools.partial(plan_kernel, n_dp, n_ep, sizes),
            out_shape=(jax.ShapeDtypeStruct((2 * n_tok, d_model), BF16),
                       jax.ShapeDtypeStruct((slots, d_model), BF16),
                       jax.ShapeDtypeStruct((3, 4 * n_exp, cap), I32),
                       jax.ShapeDtypeStruct((1,), I32)),
            in_specs=[any_spec] * 2,
            out_specs=(vmem_spec, vmem_spec, vmem_spec, pl.BlockSpec(memory_space=pltpu.SMEM)),
            scratch_shapes=[
                pltpu.VMEM((n_dev, n_exp, cap), I32),
                dma((2,)), dma((n_dev - 1,)), dma((n_dev - 1,)), dma, dma,
            ],
            compiler_params=pltpu.CompilerParams(
                collective_id=0, has_side_effects=True, vmem_limit_bytes=58 * 1024 * 1024),
        )(tok, idx)

        def branch(i):
            k_rows = sizes[i]
            nc = (k_rows // cap + 1) // 2

            def run(chip_tok, xown, meta, gate, w_in, w_out):
                return pl.pallas_call(
                    functools.partial(layer_kernel, k_rows),
                    out_shape=jax.ShapeDtypeStruct((n_tok, d_model), BF16),
                    in_specs=[vmem_spec] * 4 + [any_spec] * 2,
                    out_specs=vmem_spec,
                    scratch_shapes=[
                        pltpu.VMEM(((nc + 1) // 2 * 2 * cap, d_model), BF16),
                        pltpu.VMEM((2 * nc * cap, d_model), BF16),
                        pltpu.VMEM((2 * nc * cap, d_model), BF16),
                        pltpu.VMEM((slots, d_model), BF16),
                        pltpu.VMEM((2 * slots, d_model), BF16),
                        pltpu.VMEM((slots, d_model), BF16),
                        pltpu.VMEM((nc * cap, d_model), BF16),
                        pltpu.VMEM((2 * nc * cap, d_model), BF16),
                        pltpu.VMEM((2 * nc, cap), I32),
                        pltpu.VMEM((n_tok, d_model), F32),
                        pltpu.VMEM((cap, d_model), F32),
                        pltpu.VMEM((W_SLOTS, d_model, d_ff), BF16),
                        pltpu.VMEM((W_SLOTS, d_ff, d_model), BF16),
                        dma((2, W_SLOTS)),
                        dma((nc,)), dma((nc,)), dma((nc,)), dma((nc,)),
                        dma((n_exp,)), dma((n_exp,)),
                        dma((nc,)), dma((nc,)), dma((nc,)), dma((nc,)),
                    ],
                    compiler_params=pltpu.CompilerParams(
                        collective_id=1 + i, has_side_effects=True, vmem_limit_bytes=54 * 1024 * 1024),
                )(chip_tok, xown, meta, gate, w_in, w_out)

            return run

        return lax.switch(bucket[0], [branch(i) for i in range(len(sizes))], chip_tok, xown, meta, gate, w_in, w_out)

    return jax.shard_map(local_layer, mesh=mesh, in_specs=(row_spec, row_spec, row_spec, expert_spec, expert_spec),
                         out_specs=row_spec, check_vma=False)
```

```python
import functools

import jax
import jax.numpy as jnp
from jax import lax
from jax.experimental import pallas as pl
from jax.experimental.pallas import tpu as pltpu
from jax.sharding import PartitionSpec as P

F32, BF16, I32 = jnp.float32, jnp.bfloat16, jnp.int32
W_SLOTS = 3
LANES = 128
FAR = 1 << 20
LENGTHS = ((2, 4), (3, 6), (5, 8), (8, 8))


def remote(src, dst, ss, rs, **dev):
    return pltpu.make_async_remote_copy(src_ref=src, dst_ref=dst, send_sem=ss, recv_sem=rs,
                                        device_id=dev, device_id_type=pl.DeviceIdType.MESH)


def signal(sem, **dev):
    pl.semaphore_signal(sem, inc=1, device_id=dev, device_id_type=pl.DeviceIdType.MESH)


def spread(col, width, lane):
    return jnp.concatenate(
        [jnp.where(col == lane + LANES * j, 1.0, 0.0).astype(BF16) for j in range(width // LANES)], axis=1)


def column(row, cap):
    return jnp.broadcast_to(row, (LANES, cap)).T


def table(pos, his, los):
    n = len(pos)
    sub_b = lax.broadcasted_iota(I32, (n, LANES), 0)
    sub_l = lax.broadcasted_iota(I32, (LANES, LANES), 0)
    blocks, his_b, los_b, lanes = [], [], [], []
    for p, hi, lo in zip(pos, his, los):
        b = jnp.where(jnp.broadcast_to(p >> 7, sub_b.shape) == sub_b, 1.0, 0.0)
        blocks.append(b.astype(BF16))
        his_b.append((b * hi.astype(F32)).astype(BF16))
        los_b.append((b * lo.astype(F32)).astype(BF16))
        lanes.append(jnp.where(jnp.broadcast_to(p & (LANES - 1), sub_l.shape) == sub_l, 1.0, 0.0).astype(BF16))
    left = jnp.concatenate([jnp.concatenate(x, axis=1) for x in (blocks, his_b, los_b)], axis=0)
    out = lax.dot_general(left, jnp.concatenate(lanes, axis=1), (((1,), (1,)), ((), ())), preferred_element_type=F32)
    ids = (out[n:2 * n] * LANES + out[2 * n:3 * n]).astype(I32)
    return jnp.where(out[0:n] > 0.5, ids, -FAR)


def plan_kernel(n_dp, n_ep, sizes, tok, idx, chip_tok, xown, meta, bucket, idx_g, loc_sem, idx_ss, idx_rs, tok_ss, tok_rs):
    n_tok = tok.shape[0]
    n_exp, cap = idx.shape
    dp, ep = lax.axis_index("dp"), lax.axis_index("ep")
    me = dp * n_ep + ep
    n_dev = n_dp * n_ep
    core = lax.rem(ep, 2)
    own_rows = chip_tok.at[pl.ds(pl.multiple_of(core * n_tok, n_tok), n_tok)]
    own_idx = pltpu.make_async_copy(idx, idx_g.at[me], loc_sem.at[0])
    own_tok = pltpu.make_async_copy(tok, own_rows, loc_sem.at[1])
    own_idx.start()
    own_tok.start()
    barrier = pltpu.get_barrier_semaphore()
    offsets = [(a, b) for a in range(n_dp - 1, -1, -1) for b in range(n_ep - 1, -1, -1) if a or b]
    others = [(lax.rem(dp + a, n_dp), lax.rem(ep + b, n_ep)) for a, b in offsets]
    n_far = (n_dp - 1) * n_ep
    for d, e in others:
        signal(barrier, dp=d, ep=e)
    own_idx.wait()
    pl.semaphore_wait(barrier, n_dev - 1)
    sends = []
    for k, (d, e) in enumerate(others):
        c = remote(idx_g.at[me], idx_g.at[me], idx_ss.at[k], idx_rs.at[k], dp=d, ep=e)
        c.start()
        sends.append(c)
    own_tok.wait()
    tok_out = remote(own_rows, own_rows, tok_ss, tok_rs, dp=dp, ep=ep + 1 - 2 * core)
    tok_out.start()
    lane = lax.broadcasted_iota(I32, (cap, LANES), 1)

    @pl.loop(0, n_exp // 2)
    def _(g):
        hot = jnp.concatenate(
            [spread(column(idx_g[me, pl.ds(2 * g + k, 1), :] - ep * n_tok, cap), n_tok, lane) for k in range(2)], axis=0)
        xown[pl.ds(pl.multiple_of(2 * g * cap, 2 * cap), 2 * cap), :] = jnp.dot(
            hot, own_rows[...], preferred_element_type=F32).astype(BF16)

    rows = 2 * n_exp
    half = 2 * n_tok
    t_lanes = LANES // 2
    t_rows = half // t_lanes

    def below(shape, key):
        r, c = (key(lax.broadcasted_iota(I32, shape, a)) for a in (0, 1))
        return jnp.where(c < r, 1.0, 0.0).astype(BF16)

    before = below((rows, rows), lambda x: lax.rem(x, n_exp) * 2 + x // n_exp)
    every = jnp.ones((rows, rows), BF16)
    upper = jnp.where(lax.broadcasted_iota(I32, (cap, cap), 0) < lax.broadcasted_iota(I32, (cap, cap), 1), 1.0, 0.0).astype(BF16)
    ones = jnp.ones((cap, cap), BF16)
    upper_t, ones_t = upper[0:t_lanes, 0:t_lanes], ones[0:t_lanes, 0:t_lanes]
    lower = below((n_exp * t_rows, n_exp * t_rows), lambda x: x)
    sub_hi = lax.broadcasted_iota(I32, (t_rows, cap), 0)
    sub_lo = lax.broadcasted_iota(I32, (t_lanes, cap), 0)

    def presence(d, h, e):
        his, los = [], []
        for c in range(2):
            at_chip = idx_g[d * n_ep + 2 * h + c, e:e + 1, :] - (1 - h) * half
            his.append(jnp.where(jnp.broadcast_to(at_chip >> 6, sub_hi.shape) == sub_hi, 1.0, 0.0).astype(BF16))
            los.append(jnp.where(jnp.broadcast_to(at_chip & (t_lanes - 1), sub_lo.shape) == sub_lo, 1.0, 0.0).astype(BF16))
        count = lax.dot_general(jnp.concatenate(his, axis=1), jnp.concatenate(los, axis=1),
                                (((1,), (1,)), ((), ())), preferred_element_type=F32)
        return jnp.minimum(count, 1.0)

    def crosses(d, h):
        ids = jnp.concatenate([idx_g[d * n_ep + 2 * h], idx_g[d * n_ep + 2 * h + 1]], axis=0)
        return ids, (ids >= half) if h == 0 else (ids < half)

    with jax.named_scope("A_near"):
        for c in sends[n_far:]:
            c.wait_recv()

    distinct = most = None
    for h in range(2):
        seen = jnp.zeros((t_rows, t_lanes), F32)
        fresh = []
        for e in range(n_exp):
            here = presence(dp, h, e)
            fresh.append(here * (1.0 - seen))
            seen = jnp.maximum(seen, here)
        n = jnp.sum(seen)
        distinct = n if distinct is None else jnp.maximum(distinct, n)
        new = jnp.concatenate(fresh, axis=0)
        new_b = new.astype(BF16)
        row_sum = jnp.dot(new_b, ones_t, preferred_element_type=F32).astype(BF16)
        pos = (jnp.dot(new_b, upper_t, preferred_element_type=F32) + jnp.dot(lower, row_sum, preferred_element_type=F32)) * new
        place = jnp.zeros((t_rows, t_lanes), F32)
        for e in range(n_exp):
            place = place + pos[e * t_rows:(e + 1) * t_rows, :]
        place = jnp.where(seen > 0.5, place.astype(I32), FAR)
        meta[1, h * rows:(h + 1) * rows, :] = jnp.concatenate([place[0:t_rows // 2], place[t_rows // 2:]], axis=1)

        ids, need = crosses(dp, h)
        flag = jnp.where(need, 1.0, 0.0)
        n = jnp.sum(flag)
        most = n if most is None else jnp.maximum(most, n)
        flag = flag.astype(BF16)
        in_row = jnp.dot(flag, upper, preferred_element_type=F32)
        slot_sum = jnp.dot(flag, ones, preferred_element_type=F32).astype(BF16)
        after = jnp.dot(before - every, slot_sum, preferred_element_type=F32)
        meta[0, h * rows:(h + 1) * rows, :] = ids
        meta[2, h * rows:(h + 1) * rows, :] = jnp.where(need, (in_row + after).astype(I32), FAR)

    with jax.named_scope("A_far"):
        for c in sends[:n_far]:
            c.wait_recv()

    for a in range(1, n_dp):
        d = lax.rem(dp + a, n_dp)
        for h in range(2):
            most = jnp.maximum(most, jnp.sum(jnp.where(crosses(d, h)[1], 1.0, 0.0)))
            seen = presence(d, h, 0)
            for e in range(1, n_exp):
                seen = jnp.maximum(seen, presence(d, h, e))
            distinct = jnp.maximum(distinct, jnp.sum(seen))
    pick = jnp.int32(0)
    for k_out, k_back in sizes[:-1]:
        pick = pick + jnp.where((distinct > k_out) | (most > k_back), 1, 0).astype(I32)
    bucket[0] = pick

    for c in sends:
        c.wait_send()
    with jax.named_scope("A_tok"):
        tok_out.wait()


def layer_kernel(k_out, k_rows, chip_tok, xown, meta_v, gate_v, w_in, w_out, out,
                 xsend, land, local, xbuf, chip_p, pland, rsend, rland, listtok, tokrow, acc, sum_o, wi, wo,
                 w_sem, d_ss, d_rs, f_ss, f_rs, p_ss, p_rs, r_ss, r_rs, g_ss, g_rs):
    n_tok, d_model = out.shape
    n_exp, d_ff = w_in.shape[0], w_in.shape[2]
    cap = gate_v.shape[1]
    slots = n_exp * cap
    rows = 2 * n_exp
    n_list = k_rows // cap
    odd = n_list % 2
    nc = (n_list + 1) // 2
    n_out = k_out // cap
    no = (n_out + 1) // 2
    ep = lax.axis_index("ep")
    chip, core = ep // 2, ep % 2
    mate = chip * 2 + (1 - core)
    opp = (1 - chip) * 2 + core

    def at(start, size):
        return pl.ds(start if isinstance(start, int) else pl.multiple_of(start, cap), size)

    def w_copies(e):
        slot = lax.rem(e, W_SLOTS)
        return (pltpu.make_async_copy(w_in.at[e], wi.at[slot], w_sem.at[0, slot]),
                pltpu.make_async_copy(w_out.at[e], wo.at[slot], w_sem.at[1, slot]))

    barrier = pltpu.get_barrier_semaphore()
    signal(barrier, ep=mate)
    signal(barrier, ep=opp)
    for e in range(W_SLOTS):
        for c in w_copies(e):
            c.start()

    def d_copy(m):
        return remote(xsend.at[at(m * cap, cap)], land.at[at((2 * m + core) * cap, cap)], d_ss.at[m], d_rs.at[m], ep=opp)

    def f_copy(m):
        r = at((2 * m + core) * cap, cap)
        return remote(land.at[r], land.at[r], f_ss.at[m], f_rs.at[m], ep=mate)

    def p_copy(e):
        return remote(chip_p.at[at(core * slots + e * cap, cap)], pland.at[at(e * cap, cap)], p_ss.at[e], p_rs.at[e], ep=mate)

    def r_copy(m):
        return remote(rsend.at[at(m * cap, cap)], rland.at[at((2 * m + core) * cap, cap)], r_ss.at[m], r_rs.at[m], ep=opp)

    def g_copy(m):
        r = at((2 * m + core) * cap, cap)
        return remote(rland.at[r], rland.at[r], g_ss.at[m], g_rs.at[m], ep=mate)

    def if_in(block, total, f):
        if total % 2:
            pl.when(block < total)(f)
        else:
            f()

    lane = lax.broadcasted_iota(I32, (cap, LANES), 1)
    sub = lax.broadcasted_iota(I32, (cap, LANES), 0)
    t_half = LANES // 2

    def tokens_of(lanes, i):
        return jnp.where(lanes < t_half, lanes, lanes + (n_tok - t_half)) + t_half * i

    their = (1 - chip) * rows
    mine = chip * rows

    def gather_block(m):
        t = jnp.zeros((cap, LANES), I32)
        for i in range(rows):
            pos = meta_v[1, pl.ds(their + i, 1), :]
            t = t + jnp.where(jnp.broadcast_to(pos, (cap, LANES)) == sub + (2 * m + core) * cap, tokens_of(lane, i), 0)
        at_chip = jnp.sum(t.astype(F32), axis=1, keepdims=True).astype(I32)
        return spread(jnp.broadcast_to(at_chip, (cap, LANES)), 2 * n_tok, lane)

    @pl.loop(0, (no + 1) // 2)
    def _(g):
        with jax.named_scope("send_group"):
            hot = jnp.concatenate([gather_block(2 * g + k) for k in range(2)], axis=0)
            xsend[at(2 * g * cap, 2 * cap), :] = jnp.dot(hot, chip_tok[...], preferred_element_type=F32).astype(BF16)

        @pl.when(g == 0)
        def _():
            pl.semaphore_wait(barrier, 2)

        for k in range(2):
            pl.when(2 * (2 * g + k) + core < n_out)(lambda k=k: d_copy(2 * g + k).start())

    mate_rows = at((1 - core) * n_tok, n_tok)

    @pl.loop(0, n_exp // 2)
    def _(g):
        with jax.named_scope("own_gather"):
            hot = jnp.concatenate(
                [spread(column(meta_v[0, pl.ds(mine + core * n_exp + 2 * g + k, 1), :] - mate * n_tok, cap), n_tok, lane)
                 for k in range(2)], axis=0)
            r = at(2 * g * cap, 2 * cap)
            xbuf[r, :] = xown[r, :] + jnp.dot(hot, chip_tok[mate_rows, :], preferred_element_type=F32).astype(BF16)

    @pl.loop(0, no)
    def _(b):
        local[at(b * 2 * cap, 2 * cap), :] = jnp.zeros((2 * cap, d_model), BF16)

    @pl.loop(0, n_exp)
    def _(b):
        chip_p[at(b * 2 * cap, 2 * cap), :] = jnp.zeros((2 * cap, d_model), BF16)

    def forward(m):
        def go():
            with jax.named_scope("forward"):
                d_copy(m).wait_recv()
                f_copy(m).start()

        if_in(2 * m + core, n_out, go)

    lane_row = lax.broadcasted_iota(I32, (1, LANES), 1)
    listtok[...] = table([meta_v[1, pl.ds(mine + i, 1), :] for i in range(rows)],
                         [tokens_of(lane_row, i) >> 7 for i in range(rows)],
                         [tokens_of(lane_row, i) & (LANES - 1) for i in range(rows)])
    forward(0)

    back_pos = [meta_v[2, pl.ds(their + i, 1), :] + k_rows for i in range(rows)]
    back_ids = [meta_v[0, pl.ds(their + i, 1), :] for i in range(rows)]
    tokrow[...] = table(back_pos, [i >> 7 for i in back_ids], [i & (LANES - 1) for i in back_ids])
    f_tile = 512
    n_f = d_ff // f_tile

    def m_of(e):
        return e - (n_exp - nc) - (core if odd else 0)

    def pack_return(e):
        with jax.named_scope("pwait"):
            p_copy(e).wait_recv()
        chip_p[at((1 - core) * slots + e * cap, cap), :] = pland[at(e * cap, cap), :]
        m = m_of(e)

        @pl.when(m >= 0)
        def _():
            parts = []
            for i in range(rows):
                pos = meta_v[2, pl.ds(mine + i, 1), :] + k_rows
                parts.append(jnp.where(jnp.broadcast_to(pos, (cap, LANES)) == sub + (2 * m + core) * cap, 1.0, 0.0).astype(BF16))
            hot = jnp.concatenate(parts, axis=1)
            rsend[at(m * cap, cap), :] = jnp.dot(hot, chip_p[...], preferred_element_type=F32).astype(BF16)
            r_copy(m).start()

    @pl.loop(0, n_exp)
    def _(e):
        slot = lax.rem(e, W_SLOTS)

        mine_e = at(e * cap, cap)

        def take_block():
            def go():
                with jax.named_scope("fwait"):
                    f_copy(e).wait_recv()

            if_in(2 * e + 1 - core, n_out, go)
            for k in range(2):
                @pl.when(2 * e + k < n_out)
                def _():
                    r = at((2 * e + k) * cap, cap)
                    local[r, :] = land[r, :]

        def fill():
            pl.when(e < no)(take_block)
            wanted = column(meta_v[0, pl.ds(mine + core * n_exp + e, 1), :], cap) - (1 - chip) * (2 * n_tok)
            hot = jnp.concatenate(
                [jnp.where(wanted == jnp.broadcast_to(listtok[j:j + 1, :], (cap, LANES)), 1.0, 0.0).astype(BF16)
                 for j in range(n_out)], axis=1)
            xbuf[mine_e, :] = xbuf[mine_e, :] + jnp.dot(hot, local[0:k_out, :], preferred_element_type=F32).astype(BF16)
            with jax.named_scope("wwait"):
                for c in w_copies(e):
                    c.wait()
            sum_o[...] = jnp.zeros((cap, d_model), F32)

        @pl.loop(0, 2)
        def _(half):
            @pl.when((e > 0) & ((half == 0) == (m_of(e - 1) == 0)))
            def _():
                pack_return(e - 1)

            pl.when(half == 0)(fill)

            @pl.when((half == 1) & (e + 1 < no))
            def _():
                forward(e + 1)

            x = xbuf[mine_e, :]
            o = None
            for f in range(n_f // 2):
                fs = at(half * (d_ff // 2) + f * f_tile, f_tile)
                pre = jnp.dot(x, wi[slot, :, fs], preferred_element_type=F32)
                h = jax.nn.gelu(pre, approximate=True).astype(BF16)
                part = jnp.dot(h, wo[slot, fs, :], preferred_element_type=F32)
                o = part if o is None else o + part
            sum_o[...] = sum_o[...] + o

        gcol = column(gate_v[pl.ds(e, 1), :], cap)
        chip_p[at(core * slots + e * cap, cap), :] = (
            jnp.concatenate([gcol] * (d_model // LANES), axis=1) * sum_o[...]).astype(BF16)
        p_copy(e).start()

        @pl.when(e + W_SLOTS < n_exp)
        def _():
            for c in w_copies(e + W_SLOTS):
                c.start()

    n_blk = n_tok // (2 * cap)
    blk = 2 * cap
    sub_b = lax.broadcasted_iota(I32, (blk, LANES), 0) + ep * n_tok
    early = nc - 3

    def forward_back(m):
        def go():
            with jax.named_scope("rwait"):
                r_copy(m).wait_recv()
                g_copy(m).start()

        if_in(2 * m + core, n_list, go)

    def back_wait(m):
        def go():
            with jax.named_scope("gwait"):
                g_copy(m).wait_recv()

        if_in(2 * m + 1 - core, n_list, go)

    pl.loop(0, early)(forward_back)
    with jax.named_scope("pack_last"):
        pack_return(n_exp - 1)
    pl.loop(0, early)(back_wait)

    def owners(row, b):
        return jnp.where(jnp.broadcast_to(row, (blk, LANES)) == sub_b + b * blk, 1.0, 0.0).astype(BF16)

    @pl.loop(0, n_blk)
    def _(b):
        with jax.named_scope("early_back"):
            hot = jnp.concatenate([owners(tokrow[pl.ds(i, 1), :], b) for i in range(2 * early)], axis=1)
            own = chip_tok[at(core * n_tok + b * blk, blk), :].astype(F32)
            acc[at(b * blk, blk), :] = own + jnp.dot(hot, rland[0:early * 2 * cap, :], preferred_element_type=F32)

    @pl.loop(0, n_blk)
    def _(b):
        @pl.when(b == n_blk // 2)
        def _():
            forward_back(early)

        with jax.named_scope("own_scatter"):
            r = at(b * blk, blk)
            hot = jnp.concatenate([owners(meta_v[0, pl.ds(mine + i, 1), :], b) for i in range(rows)], axis=1)
            acc[r, :] = acc[r, :] + jnp.dot(hot, chip_p[...], preferred_element_type=F32)

    def combine(m, last):
        n_in = 1 if last and odd else 2
        ids = [tokrow[pl.ds(2 * m + k, 1), :] for k in range(n_in)]
        back_wait(m)
        back = rland[at(2 * m * cap, n_in * cap), :]

        def block(b):
            r = at(b * blk, blk)
            hot = jnp.concatenate([owners(i, b) for i in ids], axis=1)
            return r, acc[r, :] + jnp.dot(hot, back, preferred_element_type=F32)

        if last:
            for b in range(n_blk):
                r, total = block(b)
                out[r, :] = total.astype(BF16)
        else:
            @pl.loop(0, n_blk)
            def _(b):
                r, total = block(b)
                acc[r, :] = total

    @pl.loop(early, nc - 1)
    def _(m):
        forward_back(m + 1)
        combine(m, False)

    combine(nc - 1, True)

    @pl.loop(0, no)
    def _(m):
        def go():
            d_copy(m).wait_send()
            f_copy(m).wait_send()

        if_in(2 * m + core, n_out, go)

    @pl.loop(0, nc)
    def _(m):
        def go():
            r_copy(m).wait_send()
            g_copy(m).wait_send()

        if_in(2 * m + core, n_list, go)

    @pl.loop(0, n_exp)
    def _(e):
        p_copy(e).wait_send()


def solution(mesh):
    n_dp, n_ep = mesh.shape["dp"], mesh.shape["ep"]
    row_spec = P(("dp", "ep"), None)
    expert_spec = P("ep", None, None)
    dma = pltpu.SemaphoreType.DMA
    any_spec = pl.BlockSpec(memory_space=pl.ANY)
    vmem_spec = pl.BlockSpec(memory_space=pltpu.VMEM)

    def local_layer(tok, idx, gate, w_in, w_out):
        n_tok, d_model = tok.shape
        n_exp, cap = idx.shape
        d_ff = w_in.shape[2]
        slots = n_exp * cap
        sizes = tuple((slots + i * cap, slots + j * cap) for i, j in LENGTHS)
        n_dev = n_dp * n_ep

        chip_tok, xown, meta, bucket = pl.pallas_call(
            functools.partial(plan_kernel, n_dp, n_ep, sizes),
            out_shape=(jax.ShapeDtypeStruct((2 * n_tok, d_model), BF16),
                       jax.ShapeDtypeStruct((slots, d_model), BF16),
                       jax.ShapeDtypeStruct((3, 4 * n_exp, cap), I32),
                       jax.ShapeDtypeStruct((1,), I32)),
            in_specs=[any_spec] * 2,
            out_specs=(vmem_spec, vmem_spec, vmem_spec, pl.BlockSpec(memory_space=pltpu.SMEM)),
            scratch_shapes=[
                pltpu.VMEM((n_dev, n_exp, cap), I32),
                dma((2,)), dma((n_dev - 1,)), dma((n_dev - 1,)), dma, dma,
            ],
            compiler_params=pltpu.CompilerParams(
                collective_id=0, has_side_effects=True, vmem_limit_bytes=58 * 1024 * 1024),
        )(tok, idx)

        def branch(i):
            k_out, k_rows = sizes[i]
            no = (k_out // cap + 1) // 2
            nc = (k_rows // cap + 1) // 2

            def run(chip_tok, xown, meta, gate, w_in, w_out):
                return pl.pallas_call(
                    functools.partial(layer_kernel, k_out, k_rows),
                    out_shape=jax.ShapeDtypeStruct((n_tok, d_model), BF16),
                    in_specs=[vmem_spec] * 4 + [any_spec] * 2,
                    out_specs=vmem_spec,
                    scratch_shapes=[
                        pltpu.VMEM(((no + 1) // 2 * 2 * cap, d_model), BF16),
                        pltpu.VMEM((2 * no * cap, d_model), BF16),
                        pltpu.VMEM((2 * no * cap, d_model), BF16),
                        pltpu.VMEM((slots, d_model), BF16),
                        pltpu.VMEM((2 * slots, d_model), BF16),
                        pltpu.VMEM((slots, d_model), BF16),
                        pltpu.VMEM((nc * cap, d_model), BF16),
                        pltpu.VMEM((2 * nc * cap, d_model), BF16),
                        pltpu.VMEM((2 * n_exp, cap), I32),
                        pltpu.VMEM((2 * n_exp, cap), I32),
                        pltpu.VMEM((n_tok, d_model), F32),
                        pltpu.VMEM((cap, d_model), F32),
                        pltpu.VMEM((W_SLOTS, d_model, d_ff), BF16),
                        pltpu.VMEM((W_SLOTS, d_ff, d_model), BF16),
                        dma((2, W_SLOTS)),
                        dma((no,)), dma((no,)), dma((no,)), dma((no,)),
                        dma((n_exp,)), dma((n_exp,)),
                        dma((nc,)), dma((nc,)), dma((nc,)), dma((nc,)),
                    ],
                    compiler_params=pltpu.CompilerParams(
                        collective_id=1 + i, has_side_effects=True, vmem_limit_bytes=54 * 1024 * 1024),
                )(chip_tok, xown, meta, gate, w_in, w_out)

            return run

        return lax.switch(bucket[0], [branch(i) for i in range(len(sizes))], chip_tok, xown, meta, gate, w_in, w_out)

    return jax.shard_map(local_layer, mesh=mesh, in_specs=(row_spec, row_spec, row_spec, expert_spec, expert_spec),
                         out_specs=row_spec, check_vma=False)
```

```python
import functools

import jax
import jax.numpy as jnp
from jax import lax
from jax.experimental import pallas as pl
from jax.experimental.pallas import tpu as pltpu
from jax.sharding import PartitionSpec as P

F32, BF16, I32 = jnp.float32, jnp.bfloat16, jnp.int32
W_SLOTS = 3
LANES = 128
FAR = 1 << 20
LENGTHS = ((2, 4), (3, 6), (5, 8), (8, 8))


def remote(src, dst, ss, rs, **dev):
    return pltpu.make_async_remote_copy(src_ref=src, dst_ref=dst, send_sem=ss, recv_sem=rs,
                                        device_id=dev, device_id_type=pl.DeviceIdType.MESH)


def signal(sem, **dev):
    pl.semaphore_signal(sem, inc=1, device_id=dev, device_id_type=pl.DeviceIdType.MESH)


def spread(col, width, lane):
    return jnp.concatenate(
        [jnp.where(col == lane + LANES * j, 1.0, 0.0).astype(BF16) for j in range(width // LANES)], axis=1)


def column(row, cap):
    return jnp.broadcast_to(row, (LANES, cap)).T


def table(pos, his, los):
    n = len(pos)
    sub_b = lax.broadcasted_iota(I32, (n, LANES), 0)
    sub_l = lax.broadcasted_iota(I32, (LANES, LANES), 0)
    blocks, his_b, los_b, lanes = [], [], [], []
    for p, hi, lo in zip(pos, his, los):
        b = jnp.where(jnp.broadcast_to(p >> 7, sub_b.shape) == sub_b, 1.0, 0.0)
        blocks.append(b.astype(BF16))
        his_b.append((b * hi.astype(F32)).astype(BF16))
        los_b.append((b * lo.astype(F32)).astype(BF16))
        lanes.append(jnp.where(jnp.broadcast_to(p & (LANES - 1), sub_l.shape) == sub_l, 1.0, 0.0).astype(BF16))
    left = jnp.concatenate([jnp.concatenate(x, axis=1) for x in (blocks, his_b, los_b)], axis=0)
    out = lax.dot_general(left, jnp.concatenate(lanes, axis=1), (((1,), (1,)), ((), ())), preferred_element_type=F32)
    ids = (out[n:2 * n] * LANES + out[2 * n:3 * n]).astype(I32)
    return jnp.where(out[0:n] > 0.5, ids, -FAR)


def below(shape, key):
    r, c = (key(lax.broadcasted_iota(I32, shape, a)) for a in (0, 1))
    return jnp.where(c < r, 1.0, 0.0).astype(BF16)


def plan_kernel(n_dp, n_ep, sizes, tok, idx, chip_tok, xown, meta, bucket, idx_g, pick_s, loc_sem, idx_ss, idx_rs, tok_ss, tok_rs):
    n_tok = tok.shape[0]
    n_exp, cap = idx.shape
    dp, ep = lax.axis_index("dp"), lax.axis_index("ep")
    me = dp * n_ep + ep
    n_dev = n_dp * n_ep
    core = lax.rem(ep, 2)
    own_rows = chip_tok.at[pl.ds(pl.multiple_of(core * n_tok, n_tok), n_tok)]
    own_idx = pltpu.make_async_copy(idx, idx_g.at[me], loc_sem.at[0])
    own_tok = pltpu.make_async_copy(tok, own_rows, loc_sem.at[1])
    own_idx.start()
    own_tok.start()
    barrier = pltpu.get_barrier_semaphore()
    offsets = [(a, b) for a in range(n_dp - 1, -1, -1) for b in range(n_ep - 1, -1, -1) if a or b]
    others = [(lax.rem(dp + a, n_dp), lax.rem(ep + b, n_ep)) for a, b in offsets]
    n_far = (n_dp - 1) * n_ep
    for d, e in others:
        signal(barrier, dp=d, ep=e)
    own_idx.wait()
    pl.semaphore_wait(barrier, n_dev - 1)
    sends = []
    for k, (d, e) in enumerate(others):
        c = remote(idx_g.at[me], idx_g.at[me], idx_ss.at[k], idx_rs.at[k], dp=d, ep=e)
        c.start()
        sends.append(c)
    own_tok.wait()
    tok_out = remote(own_rows, own_rows, tok_ss, tok_rs, dp=dp, ep=ep + 1 - 2 * core)
    tok_out.start()
    lane = lax.broadcasted_iota(I32, (cap, LANES), 1)

    @pl.loop(0, n_exp // 2)
    def _(g):
        hot = jnp.concatenate(
            [spread(column(idx_g[me, pl.ds(2 * g + k, 1), :] - ep * n_tok, cap), n_tok, lane) for k in range(2)], axis=0)
        xown[pl.ds(pl.multiple_of(2 * g * cap, 2 * cap), 2 * cap), :] = jnp.dot(
            hot, own_rows[...], preferred_element_type=F32).astype(BF16)

    rows = 2 * n_exp
    half = 2 * n_tok
    t_lanes = LANES // 2
    t_rows = half // t_lanes

    upper_t = jnp.where(lax.broadcasted_iota(I32, (t_lanes, t_lanes), 0) < lax.broadcasted_iota(I32, (t_lanes, t_lanes), 1),
                        1.0, 0.0).astype(BF16)
    ones_t = jnp.ones((t_lanes, t_lanes), BF16)
    lower = below((n_exp * t_rows, n_exp * t_rows), lambda x: x)
    sub_hi = lax.broadcasted_iota(I32, (t_rows, cap), 0)
    sub_lo = lax.broadcasted_iota(I32, (t_lanes, cap), 0)

    def presence(d, h, e):
        his, los = [], []
        for c in range(2):
            at_chip = idx_g[d * n_ep + 2 * h + c, e:e + 1, :] - (1 - h) * half
            his.append(jnp.where(jnp.broadcast_to(at_chip >> 6, sub_hi.shape) == sub_hi, 1.0, 0.0).astype(BF16))
            los.append(jnp.where(jnp.broadcast_to(at_chip & (t_lanes - 1), sub_lo.shape) == sub_lo, 1.0, 0.0).astype(BF16))
        count = lax.dot_general(jnp.concatenate(his, axis=1), jnp.concatenate(los, axis=1),
                                (((1,), (1,)), ((), ())), preferred_element_type=F32)
        return jnp.minimum(count, 1.0)

    def crosses(d, h):
        ids = jnp.concatenate([idx_g[d * n_ep + 2 * h], idx_g[d * n_ep + 2 * h + 1]], axis=0)
        return ids, (ids >= half) if h == 0 else (ids < half)

    with jax.named_scope("A_near"):
        for c in sends[n_far:]:
            c.wait_recv()

    distinct = most = None
    lists = []
    for h in range(2):
        seen = jnp.zeros((t_rows, t_lanes), F32)
        fresh = []
        for e in range(n_exp):
            here = presence(dp, h, e)
            fresh.append(here * (1.0 - seen))
            seen = jnp.maximum(seen, here)
        lists.append((seen, fresh))
        n = jnp.sum(seen)
        distinct = n if distinct is None else jnp.maximum(distinct, n)
        ids, need = crosses(dp, h)
        meta[0, h * rows:(h + 1) * rows, :] = ids
        n = jnp.sum(jnp.where(need, 1.0, 0.0))
        most = n if most is None else jnp.maximum(most, n)

    with jax.named_scope("A_far"):
        for c in sends[:n_far]:
            c.wait_recv()

    for a in range(1, n_dp):
        d = lax.rem(dp + a, n_dp)
        for h in range(2):
            most = jnp.maximum(most, jnp.sum(jnp.where(crosses(d, h)[1], 1.0, 0.0)))
            seen = presence(d, h, 0)
            for e in range(1, n_exp):
                seen = jnp.maximum(seen, presence(d, h, e))
            distinct = jnp.maximum(distinct, jnp.sum(seen))
    pick = jnp.int32(0)
    for k_out, k_back in sizes[:-1]:
        pick = pick + jnp.where((distinct > k_out) | (most > k_back), 1, 0).astype(I32)
    pick_s[0] = pick
    pick_out = pltpu.make_async_copy(pick_s, bucket, loc_sem.at[2])
    pick_out.start()

    for h, (seen, fresh) in enumerate(lists):
        new = jnp.concatenate(fresh, axis=0)
        new_b = new.astype(BF16)
        row_sum = jnp.dot(new_b, ones_t, preferred_element_type=F32).astype(BF16)
        pos = (jnp.dot(new_b, upper_t, preferred_element_type=F32) + jnp.dot(lower, row_sum, preferred_element_type=F32)) * new
        place = jnp.zeros((t_rows, t_lanes), F32)
        for e in range(n_exp):
            place = place + pos[e * t_rows:(e + 1) * t_rows, :]
        place = jnp.where(seen > 0.5, place.astype(I32), FAR)
        meta[1, h * rows:(h + 1) * rows, :] = jnp.concatenate([place[0:t_rows // 2], place[t_rows // 2:]], axis=1)

    for c in sends:
        c.wait_send()
    with jax.named_scope("A_tok"):
        tok_out.wait()
    pick_out.wait()


def layer_kernel(k_out, k_rows, chip_tok, xown, meta_v, gate_v, w_in, w_out, out,
                 xsend, land, local, xbuf, chip_p, pland, rsend, rland, listtok, tokrow, back_at, acc, sum_o, wi, wo,
                 w_sem, d_ss, d_rs, f_ss, f_rs, p_ss, p_rs, r_ss, r_rs, g_ss, g_rs):
    n_tok, d_model = out.shape
    n_exp, d_ff = w_in.shape[0], w_in.shape[2]
    cap = gate_v.shape[1]
    slots = n_exp * cap
    rows = 2 * n_exp
    n_list = k_rows // cap
    odd = n_list % 2
    nc = (n_list + 1) // 2
    n_out = k_out // cap
    no = (n_out + 1) // 2
    ep = lax.axis_index("ep")
    chip, core = ep // 2, ep % 2
    mate = chip * 2 + (1 - core)
    opp = (1 - chip) * 2 + core

    def at(start, size):
        return pl.ds(start if isinstance(start, int) else pl.multiple_of(start, cap), size)

    def w_copies(e):
        slot = lax.rem(e, W_SLOTS)
        return (pltpu.make_async_copy(w_in.at[e], wi.at[slot], w_sem.at[0, slot]),
                pltpu.make_async_copy(w_out.at[e], wo.at[slot], w_sem.at[1, slot]))

    barrier = pltpu.get_barrier_semaphore()
    signal(barrier, ep=mate)
    signal(barrier, ep=opp)
    for e in range(W_SLOTS):
        for c in w_copies(e):
            c.start()

    def d_copy(m):
        return remote(xsend.at[at(m * cap, cap)], land.at[at((2 * m + core) * cap, cap)], d_ss.at[m], d_rs.at[m], ep=opp)

    def f_copy(m):
        r = at((2 * m + core) * cap, cap)
        return remote(land.at[r], land.at[r], f_ss.at[m], f_rs.at[m], ep=mate)

    def p_copy(e):
        return remote(chip_p.at[at(core * slots + e * cap, cap)], pland.at[at(e * cap, cap)], p_ss.at[e], p_rs.at[e], ep=mate)

    def r_copy(m):
        return remote(rsend.at[at(m * cap, cap)], rland.at[at((2 * m + core) * cap, cap)], r_ss.at[m], r_rs.at[m], ep=opp)

    def g_copy(m):
        r = at((2 * m + core) * cap, cap)
        return remote(rland.at[r], rland.at[r], g_ss.at[m], g_rs.at[m], ep=mate)

    def if_in(block, total, f):
        if total % 2:
            pl.when(block < total)(f)
        else:
            f()

    lane = lax.broadcasted_iota(I32, (cap, LANES), 1)
    sub = lax.broadcasted_iota(I32, (cap, LANES), 0)
    t_half = LANES // 2

    def tokens_of(lanes, i):
        return jnp.where(lanes < t_half, lanes, lanes + (n_tok - t_half)) + t_half * i

    their = (1 - chip) * rows
    mine = chip * rows

    def gather_block(m):
        t = jnp.zeros((cap, LANES), I32)
        for i in range(rows):
            pos = meta_v[1, pl.ds(their + i, 1), :]
            t = t + jnp.where(jnp.broadcast_to(pos, (cap, LANES)) == sub + (2 * m + core) * cap, tokens_of(lane, i), 0)
        at_chip = jnp.sum(t.astype(F32), axis=1, keepdims=True).astype(I32)
        return spread(jnp.broadcast_to(at_chip, (cap, LANES)), 2 * n_tok, lane)

    @pl.loop(0, (no + 1) // 2)
    def _(g):
        with jax.named_scope("send_group"):
            hot = jnp.concatenate([gather_block(2 * g + k) for k in range(2)], axis=0)
            xsend[at(2 * g * cap, 2 * cap), :] = jnp.dot(hot, chip_tok[...], preferred_element_type=F32).astype(BF16)

        @pl.when(g == 0)
        def _():
            pl.semaphore_wait(barrier, 2)

        for k in range(2):
            pl.when(2 * (2 * g + k) + core < n_out)(lambda k=k: d_copy(2 * g + k).start())

    mate_rows = at((1 - core) * n_tok, n_tok)

    @pl.loop(0, n_exp // 2)
    def _(g):
        with jax.named_scope("own_gather"):
            hot = jnp.concatenate(
                [spread(column(meta_v[0, pl.ds(mine + core * n_exp + 2 * g + k, 1), :] - mate * n_tok, cap), n_tok, lane)
                 for k in range(2)], axis=0)
            r = at(2 * g * cap, 2 * cap)
            xbuf[r, :] = xown[r, :] + jnp.dot(hot, chip_tok[mate_rows, :], preferred_element_type=F32).astype(BF16)

    @pl.loop(0, no)
    def _(b):
        local[at(b * 2 * cap, 2 * cap), :] = jnp.zeros((2 * cap, d_model), BF16)

    @pl.loop(0, n_exp)
    def _(b):
        chip_p[at(b * 2 * cap, 2 * cap), :] = jnp.zeros((2 * cap, d_model), BF16)

    def forward(m):
        def go():
            with jax.named_scope("forward"):
                d_copy(m).wait_recv()
                f_copy(m).start()

        if_in(2 * m + core, n_out, go)

    lane_row = lax.broadcasted_iota(I32, (1, LANES), 1)
    listtok[...] = table([meta_v[1, pl.ds(mine + i, 1), :] for i in range(rows)],
                         [tokens_of(lane_row, i) >> 7 for i in range(rows)],
                         [tokens_of(lane_row, i) & (LANES - 1) for i in range(rows)])
    before = below((rows, rows), lambda x: lax.rem(x, n_exp) * 2 + x // n_exp) - jnp.ones((rows, rows), BF16)
    upper = below((cap, cap), lambda x: -x)
    ones = jnp.ones((cap, cap), BF16)
    for h in range(2):
        ids = meta_v[0, h * rows:(h + 1) * rows, :]
        need = (ids >= 2 * n_tok) if h == 0 else (ids < 2 * n_tok)
        flag = jnp.where(need, 1.0, 0.0).astype(BF16)
        slot_sum = jnp.dot(flag, ones, preferred_element_type=F32).astype(BF16)
        place = jnp.dot(flag, upper, preferred_element_type=F32) + jnp.dot(before, slot_sum, preferred_element_type=F32)
        back_at[h * rows:(h + 1) * rows, :] = jnp.where(need, place.astype(I32) + k_rows, FAR)

    forward(0)

    back_pos = [back_at[pl.ds(their + i, 1), :] for i in range(rows)]
    back_ids = [meta_v[0, pl.ds(their + i, 1), :] for i in range(rows)]
    tokrow[...] = table(back_pos, [i >> 7 for i in back_ids], [i & (LANES - 1) for i in back_ids])
    f_tile = 512
    n_f = d_ff // f_tile

    def m_of(e):
        return e - (n_exp - nc) - (core if odd else 0)

    def pack_return(e):
        with jax.named_scope("pwait"):
            p_copy(e).wait_recv()
        chip_p[at((1 - core) * slots + e * cap, cap), :] = pland[at(e * cap, cap), :]
        m = m_of(e)

        @pl.when(m >= 0)
        def _():
            parts = []
            for i in range(rows):
                pos = back_at[pl.ds(mine + i, 1), :]
                parts.append(jnp.where(jnp.broadcast_to(pos, (cap, LANES)) == sub + (2 * m + core) * cap, 1.0, 0.0).astype(BF16))
            hot = jnp.concatenate(parts, axis=1)
            rsend[at(m * cap, cap), :] = jnp.dot(hot, chip_p[...], preferred_element_type=F32).astype(BF16)
            r_copy(m).start()

    @pl.loop(0, n_exp)
    def _(e):
        slot = lax.rem(e, W_SLOTS)

        mine_e = at(e * cap, cap)

        def take_block():
            def go():
                with jax.named_scope("fwait"):
                    f_copy(e).wait_recv()

            if_in(2 * e + 1 - core, n_out, go)
            for k in range(2):
                @pl.when(2 * e + k < n_out)
                def _():
                    r = at((2 * e + k) * cap, cap)
                    local[r, :] = land[r, :]

        def fill():
            pl.when(e < no)(take_block)
            wanted = column(meta_v[0, pl.ds(mine + core * n_exp + e, 1), :], cap) - (1 - chip) * (2 * n_tok)
            hot = jnp.concatenate(
                [jnp.where(wanted == jnp.broadcast_to(listtok[j:j + 1, :], (cap, LANES)), 1.0, 0.0).astype(BF16)
                 for j in range(n_out)], axis=1)
            xbuf[mine_e, :] = xbuf[mine_e, :] + jnp.dot(hot, local[0:k_out, :], preferred_element_type=F32).astype(BF16)
            with jax.named_scope("wwait"):
                for c in w_copies(e):
                    c.wait()
            sum_o[...] = jnp.zeros((cap, d_model), F32)

        soon = (m_of(e - 1) == 0) | (m_of(e - 1) == 1)

        @pl.loop(0, 2)
        def _(half):
            @pl.when((e > 0) & ((half == 0) == soon))
            def _():
                pack_return(e - 1)

            pl.when(half == 0)(fill)

            @pl.when((half == 1) & (e + 1 < no) & (m_of(e) != 0))
            def _():
                forward(e + 1)

            x = xbuf[mine_e, :]
            o = None
            for f in range(n_f // 2):
                fs = at(half * (d_ff // 2) + f * f_tile, f_tile)
                pre = jnp.dot(x, wi[slot, :, fs], preferred_element_type=F32)
                h = jax.nn.gelu(pre, approximate=True).astype(BF16)
                part = jnp.dot(h, wo[slot, fs, :], preferred_element_type=F32)
                o = part if o is None else o + part
            sum_o[...] = sum_o[...] + o

        gcol = column(gate_v[pl.ds(e, 1), :], cap)
        chip_p[at(core * slots + e * cap, cap), :] = (
            jnp.concatenate([gcol] * (d_model // LANES), axis=1) * sum_o[...]).astype(BF16)
        p_copy(e).start()

        @pl.when((e + 1 < no) & (m_of(e) == 0))
        def _():
            forward(e + 1)

        @pl.when(e + W_SLOTS < n_exp)
        def _():
            for c in w_copies(e + W_SLOTS):
                c.start()

    n_blk = n_tok // (2 * cap)
    blk = 2 * cap
    sub_b = lax.broadcasted_iota(I32, (blk, LANES), 0) + ep * n_tok
    early = nc - 3

    def forward_back(m):
        def go():
            with jax.named_scope("rwait"):
                r_copy(m).wait_recv()
                g_copy(m).start()

        if_in(2 * m + core, n_list, go)

    def back_wait(m):
        def go():
            with jax.named_scope("gwait"):
                g_copy(m).wait_recv()

        if_in(2 * m + 1 - core, n_list, go)

    pl.loop(0, early)(forward_back)
    with jax.named_scope("pack_last"):
        pack_return(n_exp - 1)
    pl.loop(0, early)(back_wait)

    def owners(row, b):
        return jnp.where(jnp.broadcast_to(row, (blk, LANES)) == sub_b + b * blk, 1.0, 0.0).astype(BF16)

    @pl.loop(0, n_blk)
    def _(b):
        with jax.named_scope("early_back"):
            hot = jnp.concatenate([owners(tokrow[pl.ds(i, 1), :], b) for i in range(2 * early)], axis=1)
            own = chip_tok[at(core * n_tok + b * blk, blk), :].astype(F32)
            acc[at(b * blk, blk), :] = own + jnp.dot(hot, rland[0:early * 2 * cap, :], preferred_element_type=F32)

    @pl.loop(0, n_blk)
    def _(b):
        @pl.when(b == n_blk // 2)
        def _():
            forward_back(early)

        with jax.named_scope("own_scatter"):
            r = at(b * blk, blk)
            hot = jnp.concatenate([owners(meta_v[0, pl.ds(mine + i, 1), :], b) for i in range(rows)], axis=1)
            acc[r, :] = acc[r, :] + jnp.dot(hot, chip_p[...], preferred_element_type=F32)

    def combine(m, last):
        n_in = 1 if last and odd else 2
        ids = [tokrow[pl.ds(2 * m + k, 1), :] for k in range(n_in)]
        back_wait(m)
        back = rland[at(2 * m * cap, n_in * cap), :]

        def block(b):
            r = at(b * blk, blk)
            hot = jnp.concatenate([owners(i, b) for i in ids], axis=1)
            return r, acc[r, :] + jnp.dot(hot, back, preferred_element_type=F32)

        if last:
            for b in range(n_blk):
                r, total = block(b)
                out[r, :] = total.astype(BF16)
        else:
            @pl.loop(0, n_blk)
            def _(b):
                r, total = block(b)
                acc[r, :] = total

    @pl.loop(early, nc - 1)
    def _(m):
        forward_back(m + 1)
        combine(m, False)

    combine(nc - 1, True)

    @pl.loop(0, no)
    def _(m):
        def go():
            d_copy(m).wait_send()
            f_copy(m).wait_send()

        if_in(2 * m + core, n_out, go)

    @pl.loop(0, nc)
    def _(m):
        def go():
            r_copy(m).wait_send()
            g_copy(m).wait_send()

        if_in(2 * m + core, n_list, go)

    @pl.loop(0, n_exp)
    def _(e):
        p_copy(e).wait_send()


def solution(mesh):
    n_dp, n_ep = mesh.shape["dp"], mesh.shape["ep"]
    row_spec = P(("dp", "ep"), None)
    expert_spec = P("ep", None, None)
    dma = pltpu.SemaphoreType.DMA
    any_spec = pl.BlockSpec(memory_space=pl.ANY)
    vmem_spec = pl.BlockSpec(memory_space=pltpu.VMEM)

    def local_layer(tok, idx, gate, w_in, w_out):
        n_tok, d_model = tok.shape
        n_exp, cap = idx.shape
        d_ff = w_in.shape[2]
        slots = n_exp * cap
        sizes = tuple((slots + i * cap, slots + j * cap) for i, j in LENGTHS)
        n_dev = n_dp * n_ep

        chip_tok, xown, meta, bucket = pl.pallas_call(
            functools.partial(plan_kernel, n_dp, n_ep, sizes),
            out_shape=(jax.ShapeDtypeStruct((2 * n_tok, d_model), BF16),
                       jax.ShapeDtypeStruct((slots, d_model), BF16),
                       jax.ShapeDtypeStruct((2, 4 * n_exp, cap), I32),
                       jax.ShapeDtypeStruct((1,), I32)),
            in_specs=[any_spec] * 2,
            out_specs=(vmem_spec, vmem_spec, vmem_spec, any_spec),
            scratch_shapes=[
                pltpu.VMEM((n_dev, n_exp, cap), I32),
                pltpu.SMEM((1,), I32),
                dma((3,)), dma((n_dev - 1,)), dma((n_dev - 1,)), dma, dma,
            ],
            compiler_params=pltpu.CompilerParams(
                collective_id=0, has_side_effects=True, vmem_limit_bytes=58 * 1024 * 1024),
        )(tok, idx)

        def branch(i):
            k_out, k_rows = sizes[i]
            no = (k_out // cap + 1) // 2
            nc = (k_rows // cap + 1) // 2

            def run(chip_tok, xown, meta, gate, w_in, w_out):
                return pl.pallas_call(
                    functools.partial(layer_kernel, k_out, k_rows),
                    out_shape=jax.ShapeDtypeStruct((n_tok, d_model), BF16),
                    in_specs=[vmem_spec] * 4 + [any_spec] * 2,
                    out_specs=vmem_spec,
                    scratch_shapes=[
                        pltpu.VMEM(((no + 1) // 2 * 2 * cap, d_model), BF16),
                        pltpu.VMEM((2 * no * cap, d_model), BF16),
                        pltpu.VMEM((2 * no * cap, d_model), BF16),
                        pltpu.VMEM((slots, d_model), BF16),
                        pltpu.VMEM((2 * slots, d_model), BF16),
                        pltpu.VMEM((slots, d_model), BF16),
                        pltpu.VMEM((nc * cap, d_model), BF16),
                        pltpu.VMEM((2 * nc * cap, d_model), BF16),
                        pltpu.VMEM((2 * n_exp, cap), I32),
                        pltpu.VMEM((2 * n_exp, cap), I32),
                        pltpu.VMEM((4 * n_exp, cap), I32),
                        pltpu.VMEM((n_tok, d_model), F32),
                        pltpu.VMEM((cap, d_model), F32),
                        pltpu.VMEM((W_SLOTS, d_model, d_ff), BF16),
                        pltpu.VMEM((W_SLOTS, d_ff, d_model), BF16),
                        dma((2, W_SLOTS)),
                        dma((no,)), dma((no,)), dma((no,)), dma((no,)),
                        dma((n_exp,)), dma((n_exp,)),
                        dma((nc,)), dma((nc,)), dma((nc,)), dma((nc,)),
                    ],
                    compiler_params=pltpu.CompilerParams(
                        collective_id=1 + i, has_side_effects=True, vmem_limit_bytes=54 * 1024 * 1024),
                )(chip_tok, xown, meta, gate, w_in, w_out)

            return run

        return lax.switch(bucket[0], [branch(i) for i in range(len(sizes))], chip_tok, xown, meta, gate, w_in, w_out)

    return jax.shard_map(local_layer, mesh=mesh, in_specs=(row_spec, row_spec, row_spec, expert_spec, expert_spec),
                         out_specs=row_spec, check_vma=False)
```

```python
import functools

import jax
import jax.numpy as jnp
from jax import lax
from jax.experimental import pallas as pl
from jax.experimental.pallas import tpu as pltpu
from jax.sharding import PartitionSpec as P

F32, BF16, I32 = jnp.float32, jnp.bfloat16, jnp.int32
W_SLOTS = 3
LANES = 128
FAR = 1 << 20
LENGTHS = ((2, 4), (3, 6), (5, 8), (8, 8))


def remote(src, dst, ss, rs, **dev):
    return pltpu.make_async_remote_copy(src_ref=src, dst_ref=dst, send_sem=ss, recv_sem=rs,
                                        device_id=dev, device_id_type=pl.DeviceIdType.MESH)


def signal(sem, **dev):
    pl.semaphore_signal(sem, inc=1, device_id=dev, device_id_type=pl.DeviceIdType.MESH)


def spread(col, width, lane):
    return jnp.concatenate(
        [jnp.where(col == lane + LANES * j, 1.0, 0.0).astype(BF16) for j in range(width // LANES)], axis=1)


def column(row, cap):
    return jnp.broadcast_to(row, (LANES, cap)).T


def table(pos, his, los):
    n = len(pos)
    sub_b = lax.broadcasted_iota(I32, (n, LANES), 0)
    sub_l = lax.broadcasted_iota(I32, (LANES, LANES), 0)
    blocks, his_b, los_b, lanes = [], [], [], []
    for p, hi, lo in zip(pos, his, los):
        b = jnp.where(jnp.broadcast_to(p >> 7, sub_b.shape) == sub_b, 1.0, 0.0)
        blocks.append(b.astype(BF16))
        his_b.append((b * hi.astype(F32)).astype(BF16))
        los_b.append((b * lo.astype(F32)).astype(BF16))
        lanes.append(jnp.where(jnp.broadcast_to(p & (LANES - 1), sub_l.shape) == sub_l, 1.0, 0.0).astype(BF16))
    left = jnp.concatenate([jnp.concatenate(x, axis=1) for x in (blocks, his_b, los_b)], axis=0)
    out = lax.dot_general(left, jnp.concatenate(lanes, axis=1), (((1,), (1,)), ((), ())), preferred_element_type=F32)
    ids = (out[n:2 * n] * LANES + out[2 * n:3 * n]).astype(I32)
    return jnp.where(out[0:n] > 0.5, ids, -FAR)


def below(shape, key):
    r, c = (key(lax.broadcasted_iota(I32, shape, a)) for a in (0, 1))
    return jnp.where(c < r, 1.0, 0.0).astype(BF16)


def plan_kernel(n_dp, n_ep, sizes, tok, idx, chip_tok, xown, meta, bucket, idx_g, pick_s, loc_sem, idx_ss, idx_rs, tok_ss, tok_rs):
    n_tok = tok.shape[0]
    n_exp, cap = idx.shape
    dp, ep = lax.axis_index("dp"), lax.axis_index("ep")
    me = dp * n_ep + ep
    n_dev = n_dp * n_ep
    core = lax.rem(ep, 2)
    own_rows = chip_tok.at[pl.ds(pl.multiple_of(core * n_tok, n_tok), n_tok)]
    own_idx = pltpu.make_async_copy(idx, idx_g.at[me], loc_sem.at[0])
    own_tok = pltpu.make_async_copy(tok, own_rows, loc_sem.at[1])
    own_idx.start()
    own_tok.start()
    barrier = pltpu.get_barrier_semaphore()
    offsets = [(a, b) for a in range(n_dp - 1, -1, -1) for b in range(n_ep - 1, -1, -1) if a or b]
    others = [(lax.rem(dp + a, n_dp), lax.rem(ep + b, n_ep)) for a, b in offsets]
    n_far = (n_dp - 1) * n_ep
    for d, e in others:
        signal(barrier, dp=d, ep=e)
    own_idx.wait()
    pl.semaphore_wait(barrier, n_dev - 1)
    for k, (d, e) in enumerate(others):
        remote(idx_g.at[me], idx_g.at[me], idx_ss, idx_rs.at[0 if k < n_far else 1], dp=d, ep=e).start()

    def blocks(n, k):
        r = idx_g.at[0:n]
        return remote(r, r, idx_ss, idx_rs.at[k], dp=dp, ep=ep + 1 - 2 * core)

    own_tok.wait()
    tok_out = remote(own_rows, own_rows, tok_ss, tok_rs, dp=dp, ep=ep + 1 - 2 * core)
    tok_out.start()
    lane = lax.broadcasted_iota(I32, (cap, LANES), 1)

    @pl.loop(0, n_exp // 2)
    def _(g):
        hot = jnp.concatenate(
            [spread(column(idx_g[me, pl.ds(2 * g + k, 1), :] - ep * n_tok, cap), n_tok, lane) for k in range(2)], axis=0)
        xown[pl.ds(pl.multiple_of(2 * g * cap, 2 * cap), 2 * cap), :] = jnp.dot(
            hot, own_rows[...], preferred_element_type=F32).astype(BF16)

    rows = 2 * n_exp
    half = 2 * n_tok
    t_lanes = LANES // 2
    t_rows = half // t_lanes

    upper_t = jnp.where(lax.broadcasted_iota(I32, (t_lanes, t_lanes), 0) < lax.broadcasted_iota(I32, (t_lanes, t_lanes), 1),
                        1.0, 0.0).astype(BF16)
    ones_t = jnp.ones((t_lanes, t_lanes), BF16)
    lower = below((n_exp * t_rows, n_exp * t_rows), lambda x: x)
    sub_hi = lax.broadcasted_iota(I32, (t_rows, cap), 0)
    sub_lo = lax.broadcasted_iota(I32, (t_lanes, cap), 0)

    def presence(d, h, e):
        his, los = [], []
        for c in range(2):
            at_chip = idx_g[d * n_ep + 2 * h + c, e:e + 1, :] - (1 - h) * half
            his.append(jnp.where(jnp.broadcast_to(at_chip >> 6, sub_hi.shape) == sub_hi, 1.0, 0.0).astype(BF16))
            los.append(jnp.where(jnp.broadcast_to(at_chip & (t_lanes - 1), sub_lo.shape) == sub_lo, 1.0, 0.0).astype(BF16))
        count = lax.dot_general(jnp.concatenate(his, axis=1), jnp.concatenate(los, axis=1),
                                (((1,), (1,)), ((), ())), preferred_element_type=F32)
        return jnp.minimum(count, 1.0)

    def crosses(d, h):
        ids = jnp.concatenate([idx_g[d * n_ep + 2 * h], idx_g[d * n_ep + 2 * h + 1]], axis=0)
        return ids, (ids >= half) if h == 0 else (ids < half)

    with jax.named_scope("A_near"):
        blocks(n_ep - 1, 1).wait_recv()

    distinct = most = None
    lists = []
    for h in range(2):
        seen = jnp.zeros((t_rows, t_lanes), F32)
        fresh = []
        for e in range(n_exp):
            here = presence(dp, h, e)
            fresh.append(here * (1.0 - seen))
            seen = jnp.maximum(seen, here)
        lists.append((seen, fresh))
        n = jnp.sum(seen)
        distinct = n if distinct is None else jnp.maximum(distinct, n)
        ids, need = crosses(dp, h)
        meta[0, h * rows:(h + 1) * rows, :] = ids
        n = jnp.sum(jnp.where(need, 1.0, 0.0))
        most = n if most is None else jnp.maximum(most, n)

    with jax.named_scope("A_far"):
        blocks(n_far, 0).wait_recv()

    for a in range(1, n_dp):
        d = lax.rem(dp + a, n_dp)
        for h in range(2):
            most = jnp.maximum(most, jnp.sum(jnp.where(crosses(d, h)[1], 1.0, 0.0)))
            seen = presence(d, h, 0)
            for e in range(1, n_exp):
                seen = jnp.maximum(seen, presence(d, h, e))
            distinct = jnp.maximum(distinct, jnp.sum(seen))
    pick = jnp.int32(0)
    for k_out, k_back in sizes[:-1]:
        pick = pick + jnp.where((distinct > k_out) | (most > k_back), 1, 0).astype(I32)
    pick_s[0] = pick
    pick_out = pltpu.make_async_copy(pick_s, bucket, loc_sem.at[2])
    pick_out.start()

    for h, (seen, fresh) in enumerate(lists):
        new = jnp.concatenate(fresh, axis=0)
        new_b = new.astype(BF16)
        row_sum = jnp.dot(new_b, ones_t, preferred_element_type=F32).astype(BF16)
        pos = (jnp.dot(new_b, upper_t, preferred_element_type=F32) + jnp.dot(lower, row_sum, preferred_element_type=F32)) * new
        place = jnp.zeros((t_rows, t_lanes), F32)
        for e in range(n_exp):
            place = place + pos[e * t_rows:(e + 1) * t_rows, :]
        place = jnp.where(seen > 0.5, place.astype(I32), FAR)
        meta[1, h * rows:(h + 1) * rows, :] = jnp.concatenate([place[0:t_rows // 2], place[t_rows // 2:]], axis=1)

    blocks(n_dev - 1, 0).wait_send()
    with jax.named_scope("A_tok"):
        tok_out.wait()
    pick_out.wait()


def layer_kernel(k_out, k_rows, chip_tok, xown, meta_v, gate_v, w_in, w_out, out,
                 xsend, land, local, xbuf, chip_p, pland, rsend, rland, listtok, tokrow, back_at, hot_last, acc, sum_o, wi, wo,
                 w_sem, d_ss, d_rs, f_ss, f_rs, p_ss, p_rs, r_ss, r_rs, g_ss, g_rs):
    n_tok, d_model = out.shape
    n_exp, d_ff = w_in.shape[0], w_in.shape[2]
    cap = gate_v.shape[1]
    slots = n_exp * cap
    rows = 2 * n_exp
    n_list = k_rows // cap
    assert n_list % 2 == 0
    nc = n_list // 2
    n_out = k_out // cap
    no = (n_out + 1) // 2
    ep = lax.axis_index("ep")
    chip, core = ep // 2, ep % 2
    mate = chip * 2 + (1 - core)
    opp = (1 - chip) * 2 + core

    def at(start, size):
        return pl.ds(start if isinstance(start, int) else pl.multiple_of(start, cap), size)

    def w_copies(e):
        slot = lax.rem(e, W_SLOTS)
        return (pltpu.make_async_copy(w_in.at[e], wi.at[slot], w_sem.at[0, slot]),
                pltpu.make_async_copy(w_out.at[e], wo.at[slot], w_sem.at[1, slot]))

    barrier = pltpu.get_barrier_semaphore()
    signal(barrier, ep=mate)
    signal(barrier, ep=opp)
    for e in range(W_SLOTS):
        for c in w_copies(e):
            c.start()

    def d_copy(m):
        return remote(xsend.at[at(m * cap, cap)], land.at[at((2 * m + core) * cap, cap)], d_ss, d_rs.at[m], ep=opp)

    def f_copy(m):
        r = at((2 * m + core) * cap, cap)
        return remote(land.at[r], land.at[r], f_ss, f_rs.at[m], ep=mate)

    def p_copy(e):
        return remote(chip_p.at[at(core * slots + e * cap, cap)], pland.at[at(e * cap, cap)], p_ss, p_rs.at[e], ep=mate)

    def r_copy(m):
        return remote(rsend.at[at(m * cap, cap)], rland.at[at((2 * m + core) * cap, cap)], r_ss, r_rs.at[m], ep=opp)

    def g_copy(m):
        r = at((2 * m + core) * cap, cap)
        return remote(rland.at[r], rland.at[r], g_ss, g_rs.at[m], ep=mate)

    def if_in(block, total, f):
        if total % 2:
            pl.when(block < total)(f)
        else:
            f()

    lane = lax.broadcasted_iota(I32, (cap, LANES), 1)
    sub = lax.broadcasted_iota(I32, (cap, LANES), 0)
    t_half = LANES // 2

    def tokens_of(lanes, i):
        return jnp.where(lanes < t_half, lanes, lanes + (n_tok - t_half)) + t_half * i

    their = (1 - chip) * rows
    mine = chip * rows

    def gather_block(m):
        t = jnp.zeros((cap, LANES), I32)
        for i in range(rows):
            pos = meta_v[1, pl.ds(their + i, 1), :]
            t = t + jnp.where(jnp.broadcast_to(pos, (cap, LANES)) == sub + (2 * m + core) * cap, tokens_of(lane, i), 0)
        at_chip = jnp.sum(t.astype(F32), axis=1, keepdims=True).astype(I32)
        return spread(jnp.broadcast_to(at_chip, (cap, LANES)), 2 * n_tok, lane)

    @pl.loop(0, (no + 1) // 2)
    def _(g):
        with jax.named_scope("send_group"):
            hot = jnp.concatenate([gather_block(2 * g + k) for k in range(2)], axis=0)
            xsend[at(2 * g * cap, 2 * cap), :] = jnp.dot(hot, chip_tok[...], preferred_element_type=F32).astype(BF16)

        @pl.when(g == 0)
        def _():
            pl.semaphore_wait(barrier, 2)

        for k in range(2):
            pl.when(2 * (2 * g + k) + core < n_out)(lambda k=k: d_copy(2 * g + k).start())

    mate_rows = at((1 - core) * n_tok, n_tok)

    @pl.loop(0, n_exp // 2)
    def _(g):
        with jax.named_scope("own_gather"):
            hot = jnp.concatenate(
                [spread(column(meta_v[0, pl.ds(mine + core * n_exp + 2 * g + k, 1), :] - mate * n_tok, cap), n_tok, lane)
                 for k in range(2)], axis=0)
            r = at(2 * g * cap, 2 * cap)
            xbuf[r, :] = xown[r, :] + jnp.dot(hot, chip_tok[mate_rows, :], preferred_element_type=F32).astype(BF16)

    @pl.loop(0, no)
    def _(b):
        local[at(b * 2 * cap, 2 * cap), :] = jnp.zeros((2 * cap, d_model), BF16)

    @pl.loop(0, n_exp)
    def _(b):
        chip_p[at(b * 2 * cap, 2 * cap), :] = jnp.zeros((2 * cap, d_model), BF16)

    def forward(m):
        def go():
            with jax.named_scope("forward"):
                d_copy(m).wait_recv()
                f_copy(m).start()

        if_in(2 * m + core, n_out, go)

    lane_row = lax.broadcasted_iota(I32, (1, LANES), 1)
    listtok[...] = table([meta_v[1, pl.ds(mine + i, 1), :] for i in range(rows)],
                         [tokens_of(lane_row, i) >> 7 for i in range(rows)],
                         [tokens_of(lane_row, i) & (LANES - 1) for i in range(rows)])
    before = below((rows, rows), lambda x: lax.rem(x, n_exp) * 2 + x // n_exp) - jnp.ones((rows, rows), BF16)
    upper = below((cap, cap), lambda x: -x)
    ones = jnp.ones((cap, cap), BF16)
    for h in range(2):
        ids = meta_v[0, h * rows:(h + 1) * rows, :]
        need = (ids >= 2 * n_tok) if h == 0 else (ids < 2 * n_tok)
        flag = jnp.where(need, 1.0, 0.0).astype(BF16)
        slot_sum = jnp.dot(flag, ones, preferred_element_type=F32).astype(BF16)
        place = jnp.dot(flag, upper, preferred_element_type=F32) + jnp.dot(before, slot_sum, preferred_element_type=F32)
        back_at[h * rows:(h + 1) * rows, :] = jnp.where(need, place.astype(I32) + k_rows, FAR)

    forward(0)

    back_pos = [back_at[pl.ds(their + i, 1), :] for i in range(rows)]
    back_ids = [meta_v[0, pl.ds(their + i, 1), :] for i in range(rows)]
    tokrow[...] = table(back_pos, [i >> 7 for i in back_ids], [i & (LANES - 1) for i in back_ids])
    f_tile = 512
    n_f = d_ff // f_tile

    def m_of(e):
        return e - (n_exp - nc)

    def pack_return(e):
        with jax.named_scope("pwait"):
            p_copy(e).wait_recv()
        chip_p[at((1 - core) * slots + e * cap, cap), :] = pland[at(e * cap, cap), :]
        m = m_of(e)

        @pl.when(m >= 0)
        def _():
            parts = []
            for i in range(rows):
                pos = back_at[pl.ds(mine + i, 1), :]
                parts.append(jnp.where(jnp.broadcast_to(pos, (cap, LANES)) == sub + (2 * m + core) * cap, 1.0, 0.0).astype(BF16))
            hot = jnp.concatenate(parts, axis=1)
            rsend[at(m * cap, cap), :] = jnp.dot(hot, chip_p[...], preferred_element_type=F32).astype(BF16)
            r_copy(m).start()

    @pl.loop(0, n_exp)
    def _(e):
        slot = lax.rem(e, W_SLOTS)

        mine_e = at(e * cap, cap)

        def take_block():
            def go():
                with jax.named_scope("fwait"):
                    f_copy(e).wait_recv()

            if_in(2 * e + 1 - core, n_out, go)
            for k in range(2):
                @pl.when(2 * e + k < n_out)
                def _():
                    r = at((2 * e + k) * cap, cap)
                    local[r, :] = land[r, :]

        def fill():
            pl.when(e < no)(take_block)
            wanted = column(meta_v[0, pl.ds(mine + core * n_exp + e, 1), :], cap) - (1 - chip) * (2 * n_tok)
            hot = jnp.concatenate(
                [jnp.where(wanted == jnp.broadcast_to(listtok[j:j + 1, :], (cap, LANES)), 1.0, 0.0).astype(BF16)
                 for j in range(n_out)], axis=1)
            xbuf[mine_e, :] = xbuf[mine_e, :] + jnp.dot(hot, local[0:k_out, :], preferred_element_type=F32).astype(BF16)
            with jax.named_scope("wwait"):
                for c in w_copies(e):
                    c.wait()
            sum_o[...] = jnp.zeros((cap, d_model), F32)

        soon = (m_of(e - 1) == 0) | (m_of(e - 1) == 1)

        @pl.loop(0, 2)
        def _(half):
            @pl.when((e > 0) & ((half == 0) == soon))
            def _():
                pack_return(e - 1)

            pl.when(half == 0)(fill)

            @pl.when((half == 1) & (e + 1 < no) & (m_of(e) != 0))
            def _():
                forward(e + 1)

            x = xbuf[mine_e, :]
            o = None
            for f in range(n_f // 2):
                fs = at(half * (d_ff // 2) + f * f_tile, f_tile)
                pre = jnp.dot(x, wi[slot, :, fs], preferred_element_type=F32)
                h = jax.nn.gelu(pre, approximate=True).astype(BF16)
                part = jnp.dot(h, wo[slot, fs, :], preferred_element_type=F32)
                o = part if o is None else o + part
            sum_o[...] = sum_o[...] + o

        gcol = column(gate_v[pl.ds(e, 1), :], cap)
        chip_p[at(core * slots + e * cap, cap), :] = (
            jnp.concatenate([gcol] * (d_model // LANES), axis=1) * sum_o[...]).astype(BF16)
        p_copy(e).start()

        @pl.when((e + 1 < no) & (m_of(e) == 0))
        def _():
            forward(e + 1)

        @pl.when(e + W_SLOTS < n_exp)
        def _():
            for c in w_copies(e + W_SLOTS):
                c.start()

    n_blk = n_tok // (2 * cap)
    blk = 2 * cap
    sub_b = lax.broadcasted_iota(I32, (blk, LANES), 0) + ep * n_tok
    early = min(nc - 3, 10 - nc)

    def forward_back(m):
        with jax.named_scope("rwait"):
            r_copy(m).wait_recv()
            g_copy(m).start()

    def back_wait(m):
        with jax.named_scope("gwait"):
            g_copy(m).wait_recv()

    pl.loop(0, early)(forward_back)
    with jax.named_scope("pack_last"):
        pack_return(n_exp - 1)
    pl.loop(0, early)(back_wait)

    def owners(row, b):
        return jnp.where(jnp.broadcast_to(row, (blk, LANES)) == sub_b + b * blk, 1.0, 0.0).astype(BF16)

    @pl.loop(0, n_blk)
    def _(b):
        with jax.named_scope("early_back"):
            hot = jnp.concatenate([owners(tokrow[pl.ds(i, 1), :], b) for i in range(2 * early)], axis=1)
            own = chip_tok[at(core * n_tok + b * blk, blk), :].astype(F32)
            acc[at(b * blk, blk), :] = own + jnp.dot(hot, rland[0:early * 2 * cap, :], preferred_element_type=F32)

    @pl.loop(0, n_blk)
    def _(b):
        @pl.when(b == n_blk // 2)
        def _():
            forward_back(early)

        with jax.named_scope("own_scatter"):
            r = at(b * blk, blk)
            hot = jnp.concatenate([owners(meta_v[0, pl.ds(mine + i, 1), :], b) for i in range(rows)], axis=1)
            acc[r, :] = acc[r, :] + jnp.dot(hot, chip_p[...], preferred_element_type=F32)

    def combine(m):
        ids = [tokrow[pl.ds(2 * m + k, 1), :] for k in range(2)]
        back_wait(m)
        back = rland[at(2 * m * cap, 2 * cap), :]

        @pl.loop(0, n_blk)
        def _(b):
            r = at(b * blk, blk)
            hot = jnp.concatenate([owners(i, b) for i in ids], axis=1)
            acc[r, :] = acc[r, :] + jnp.dot(hot, back, preferred_element_type=F32)

    last = nc - 1

    @pl.loop(0, n_blk)
    def _(b):
        hot_last[at(b * blk, blk), :] = jnp.concatenate(
            [owners(tokrow[2 * last + k:2 * last + k + 1, :], b) for k in range(2)], axis=1)

    def sent(sem, buf, blocks):
        r = buf.at[0:blocks * cap]
        remote(r, r, sem, sem, ep=mate).wait_send()

    def sent_out(blocks):
        sent(d_ss, xsend, blocks)
        sent(f_ss, land, blocks)

    if n_out % 2:
        pl.when(core == 0)(lambda: sent_out(no))
        pl.when(core == 1)(lambda: sent_out(no - 1))
    else:
        sent_out(no)
    sent(p_ss, chip_p, n_exp)

    @pl.loop(early, nc - 2)
    def _(m):
        forward_back(m + 1)
        combine(m)

    combine(nc - 2)
    forward_back(last)
    sent(r_ss, rsend, nc)
    back_wait(last)
    with jax.named_scope("last_add"):
        back = rland[2 * last * cap:2 * nc * cap, :]
        for b in range(n_blk):
            r = at(b * blk, blk)
            out[r, :] = (acc[r, :] + jnp.dot(hot_last[r, :], back, preferred_element_type=F32)).astype(BF16)

    sent(g_ss, rland, nc)


def solution(mesh):
    n_dp, n_ep = mesh.shape["dp"], mesh.shape["ep"]
    row_spec = P(("dp", "ep"), None)
    expert_spec = P("ep", None, None)
    dma = pltpu.SemaphoreType.DMA
    any_spec = pl.BlockSpec(memory_space=pl.ANY)
    vmem_spec = pl.BlockSpec(memory_space=pltpu.VMEM)

    def local_layer(tok, idx, gate, w_in, w_out):
        n_tok, d_model = tok.shape
        n_exp, cap = idx.shape
        d_ff = w_in.shape[2]
        slots = n_exp * cap
        sizes = tuple((slots + i * cap, slots + j * cap) for i, j in LENGTHS)
        n_dev = n_dp * n_ep

        chip_tok, xown, meta, bucket = pl.pallas_call(
            functools.partial(plan_kernel, n_dp, n_ep, sizes),
            out_shape=(jax.ShapeDtypeStruct((2 * n_tok, d_model), BF16),
                       jax.ShapeDtypeStruct((slots, d_model), BF16),
                       jax.ShapeDtypeStruct((2, 4 * n_exp, cap), I32),
                       jax.ShapeDtypeStruct((1,), I32)),
            in_specs=[any_spec] * 2,
            out_specs=(vmem_spec, vmem_spec, vmem_spec, any_spec),
            scratch_shapes=[
                pltpu.VMEM((n_dev, n_exp, cap), I32),
                pltpu.SMEM((1,), I32),
                dma((3,)), dma, dma((2,)), dma, dma,
            ],
            compiler_params=pltpu.CompilerParams(
                collective_id=0, has_side_effects=True, vmem_limit_bytes=58 * 1024 * 1024),
        )(tok, idx)

        def branch(i):
            k_out, k_rows = sizes[i]
            no = (k_out // cap + 1) // 2
            nc = k_rows // (2 * cap)

            def run(chip_tok, xown, meta, gate, w_in, w_out):
                return pl.pallas_call(
                    functools.partial(layer_kernel, k_out, k_rows),
                    out_shape=jax.ShapeDtypeStruct((n_tok, d_model), BF16),
                    in_specs=[vmem_spec] * 4 + [any_spec] * 2,
                    out_specs=vmem_spec,
                    scratch_shapes=[
                        pltpu.VMEM(((no + 1) // 2 * 2 * cap, d_model), BF16),
                        pltpu.VMEM((2 * no * cap, d_model), BF16),
                        pltpu.VMEM((2 * no * cap, d_model), BF16),
                        pltpu.VMEM((slots, d_model), BF16),
                        pltpu.VMEM((2 * slots, d_model), BF16),
                        pltpu.VMEM((slots, d_model), BF16),
                        pltpu.VMEM((nc * cap, d_model), BF16),
                        pltpu.VMEM((2 * nc * cap, d_model), BF16),
                        pltpu.VMEM((2 * n_exp, cap), I32),
                        pltpu.VMEM((2 * n_exp, cap), I32),
                        pltpu.VMEM((4 * n_exp, cap), I32),
                        pltpu.VMEM((n_tok, 2 * cap), BF16),
                        pltpu.VMEM((n_tok, d_model), F32),
                        pltpu.VMEM((cap, d_model), F32),
                        pltpu.VMEM((W_SLOTS, d_model, d_ff), BF16),
                        pltpu.VMEM((W_SLOTS, d_ff, d_model), BF16),
                        dma((2, W_SLOTS)),
                        dma, dma((no,)), dma, dma((no,)), dma, dma((n_exp,)), dma, dma((nc,)), dma, dma((nc,)),
                    ],
                    compiler_params=pltpu.CompilerParams(
                        collective_id=1 + i, has_side_effects=True, vmem_limit_bytes=54 * 1024 * 1024),
                )(chip_tok, xown, meta, gate, w_in, w_out)

            return run

        return lax.switch(bucket[0], [branch(i) for i in range(len(sizes))], chip_tok, xown, meta, gate, w_in, w_out)

    return jax.shard_map(local_layer, mesh=mesh, in_specs=(row_spec, row_spec, row_spec, expert_spec, expert_spec),
                         out_specs=row_spec, check_vma=False)
```

```python
import functools

import jax
import jax.numpy as jnp
from jax import lax
from jax.experimental import pallas as pl
from jax.experimental.pallas import tpu as pltpu
from jax.sharding import PartitionSpec as P

F32, BF16, I32 = jnp.float32, jnp.bfloat16, jnp.int32
W_SLOTS = 3
LANES = 128
FAR = 1 << 20
LENGTHS = ((2, 4), (3, 6), (5, 8), (8, 8))


def remote(src, dst, ss, rs, **dev):
    return pltpu.make_async_remote_copy(src_ref=src, dst_ref=dst, send_sem=ss, recv_sem=rs,
                                        device_id=dev, device_id_type=pl.DeviceIdType.MESH)


def signal(sem, **dev):
    pl.semaphore_signal(sem, inc=1, device_id=dev, device_id_type=pl.DeviceIdType.MESH)


def spread(col, width, lane):
    return jnp.concatenate(
        [jnp.where(col == lane + LANES * j, 1.0, 0.0).astype(BF16) for j in range(width // LANES)], axis=1)


def column(row, cap):
    return jnp.broadcast_to(row, (LANES, cap)).T


def table(pos, his, los):
    n = len(pos)
    sub_b = lax.broadcasted_iota(I32, (n, LANES), 0)
    sub_l = lax.broadcasted_iota(I32, (LANES, LANES), 0)
    blocks, his_b, los_b, lanes = [], [], [], []
    for p, hi, lo in zip(pos, his, los):
        b = jnp.where(jnp.broadcast_to(p >> 7, sub_b.shape) == sub_b, 1.0, 0.0)
        blocks.append(b.astype(BF16))
        his_b.append((b * hi.astype(F32)).astype(BF16))
        los_b.append((b * lo.astype(F32)).astype(BF16))
        lanes.append(jnp.where(jnp.broadcast_to(p & (LANES - 1), sub_l.shape) == sub_l, 1.0, 0.0).astype(BF16))
    left = jnp.concatenate([jnp.concatenate(x, axis=1) for x in (blocks, his_b, los_b)], axis=0)
    out = lax.dot_general(left, jnp.concatenate(lanes, axis=1), (((1,), (1,)), ((), ())), preferred_element_type=F32)
    ids = (out[n:2 * n] * LANES + out[2 * n:3 * n]).astype(I32)
    return jnp.where(out[0:n] > 0.5, ids, -FAR)


def below(shape, key):
    r, c = (key(lax.broadcasted_iota(I32, shape, a)) for a in (0, 1))
    return jnp.where(c < r, 1.0, 0.0).astype(BF16)


def plan_kernel(n_dp, n_ep, sizes, tok, idx, chip_tok, xown, meta, bucket, idx_g, pick_s, loc_sem, idx_ss, idx_rs, tok_ss, tok_rs):
    n_tok = tok.shape[0]
    n_exp, cap = idx.shape
    dp, ep = lax.axis_index("dp"), lax.axis_index("ep")
    me = dp * n_ep + ep
    n_dev = n_dp * n_ep
    core = lax.rem(ep, 2)
    own_rows = chip_tok.at[pl.ds(pl.multiple_of(core * n_tok, n_tok), n_tok)]
    own_idx = pltpu.make_async_copy(idx, idx_g.at[me], loc_sem.at[0])
    own_tok = pltpu.make_async_copy(tok, own_rows, loc_sem.at[1])
    own_idx.start()
    own_tok.start()
    barrier = pltpu.get_barrier_semaphore()
    offsets = [(a, b) for a in range(n_dp - 1, -1, -1) for b in range(n_ep - 1, -1, -1) if a or b]
    others = [(lax.rem(dp + a, n_dp), lax.rem(ep + b, n_ep)) for a, b in offsets]
    n_far = (n_dp - 1) * n_ep
    for d, e in others:
        signal(barrier, dp=d, ep=e)
    own_idx.wait()
    pl.semaphore_wait(barrier, n_dev - 1)
    for k, (d, e) in enumerate(others):
        remote(idx_g.at[me], idx_g.at[me], idx_ss, idx_rs.at[0 if k < n_far else 1], dp=d, ep=e).start()

    def blocks(n, k):
        r = idx_g.at[0:n]
        return remote(r, r, idx_ss, idx_rs.at[k], dp=dp, ep=ep + 1 - 2 * core)

    own_tok.wait()
    tok_out = remote(own_rows, own_rows, tok_ss, tok_rs, dp=dp, ep=ep + 1 - 2 * core)
    tok_out.start()
    lane = lax.broadcasted_iota(I32, (cap, LANES), 1)

    @pl.loop(0, n_exp // 2)
    def _(g):
        hot = jnp.concatenate(
            [spread(column(idx_g[me, pl.ds(2 * g + k, 1), :] - ep * n_tok, cap), n_tok, lane) for k in range(2)], axis=0)
        xown[pl.ds(pl.multiple_of(2 * g * cap, 2 * cap), 2 * cap), :] = jnp.dot(
            hot, own_rows[...], preferred_element_type=F32).astype(BF16)

    rows = 2 * n_exp
    half = 2 * n_tok
    t_lanes = LANES // 2
    t_rows = half // t_lanes

    upper_t = jnp.where(lax.broadcasted_iota(I32, (t_lanes, t_lanes), 0) < lax.broadcasted_iota(I32, (t_lanes, t_lanes), 1),
                        1.0, 0.0).astype(BF16)
    ones_t = jnp.ones((t_lanes, t_lanes), BF16)
    lower = below((n_exp * t_rows, n_exp * t_rows), lambda x: x)
    sub_hi = lax.broadcasted_iota(I32, (t_rows, cap), 0)
    sub_lo = lax.broadcasted_iota(I32, (t_lanes, cap), 0)

    def presence(d, h, e):
        his, los = [], []
        for c in range(2):
            at_chip = idx_g[d * n_ep + 2 * h + c, e:e + 1, :] - (1 - h) * half
            his.append(jnp.where(jnp.broadcast_to(at_chip >> 6, sub_hi.shape) == sub_hi, 1.0, 0.0).astype(BF16))
            los.append(jnp.where(jnp.broadcast_to(at_chip & (t_lanes - 1), sub_lo.shape) == sub_lo, 1.0, 0.0).astype(BF16))
        count = lax.dot_general(jnp.concatenate(his, axis=1), jnp.concatenate(los, axis=1),
                                (((1,), (1,)), ((), ())), preferred_element_type=F32)
        return jnp.minimum(count, 1.0)

    def crosses(d, h):
        ids = jnp.concatenate([idx_g[d * n_ep + 2 * h], idx_g[d * n_ep + 2 * h + 1]], axis=0)
        return ids, (ids >= half) if h == 0 else (ids < half)

    with jax.named_scope("A_near"):
        blocks(n_ep - 1, 1).wait_recv()

    distinct = most = None
    lists = []
    for h in range(2):
        seen = jnp.zeros((t_rows, t_lanes), F32)
        fresh = []
        for e in range(n_exp):
            here = presence(dp, h, e)
            fresh.append(here * (1.0 - seen))
            seen = jnp.maximum(seen, here)
        lists.append((seen, fresh))
        n = jnp.sum(seen)
        distinct = n if distinct is None else jnp.maximum(distinct, n)
        ids, need = crosses(dp, h)
        meta[0, h * rows:(h + 1) * rows, :] = ids
        n = jnp.sum(jnp.where(need, 1.0, 0.0))
        most = n if most is None else jnp.maximum(most, n)

    with jax.named_scope("A_far"):
        blocks(n_far, 0).wait_recv()

    for a in range(1, n_dp):
        d = lax.rem(dp + a, n_dp)
        for h in range(2):
            most = jnp.maximum(most, jnp.sum(jnp.where(crosses(d, h)[1], 1.0, 0.0)))
            seen = presence(d, h, 0)
            for e in range(1, n_exp):
                seen = jnp.maximum(seen, presence(d, h, e))
            distinct = jnp.maximum(distinct, jnp.sum(seen))
    pick = jnp.int32(0)
    for k_out, k_back in sizes[:-1]:
        pick = pick + jnp.where((distinct > k_out) | (most > k_back), 1, 0).astype(I32)
    pick_s[0] = pick
    pick_out = pltpu.make_async_copy(pick_s, bucket, loc_sem.at[2])
    pick_out.start()

    for h, (seen, fresh) in enumerate(lists):
        new = jnp.concatenate(fresh, axis=0)
        new_b = new.astype(BF16)
        row_sum = jnp.dot(new_b, ones_t, preferred_element_type=F32).astype(BF16)
        pos = (jnp.dot(new_b, upper_t, preferred_element_type=F32) + jnp.dot(lower, row_sum, preferred_element_type=F32)) * new
        place = jnp.zeros((t_rows, t_lanes), F32)
        for e in range(n_exp):
            place = place + pos[e * t_rows:(e + 1) * t_rows, :]
        place = jnp.where(seen > 0.5, place.astype(I32), FAR)
        meta[1, h * rows:(h + 1) * rows, :] = jnp.concatenate([place[0:t_rows // 2], place[t_rows // 2:]], axis=1)

    blocks(n_dev - 1, 0).wait_send()
    with jax.named_scope("A_tok"):
        tok_out.wait()
    pick_out.wait()


def layer_kernel(k_out, k_rows, chip_tok, xown, meta_v, gate_v, w_in, w_out, out,
                 xsend, land, local, xbuf, chip_p, pland, rsend, rland, listtok, tokrow, back_at, hot_last, acc, sum_o, wi, wo,
                 w_sem, d_ss, d_rs, f_ss, f_rs, p_ss, p_rs, r_ss, r_rs, g_ss, g_rs):
    n_tok, d_model = out.shape
    n_exp, d_ff = w_in.shape[0], w_in.shape[2]
    cap = gate_v.shape[1]
    slots = n_exp * cap
    rows = 2 * n_exp
    n_list = k_rows // cap
    assert n_list % 2 == 0
    nc = n_list // 2
    n_out = k_out // cap
    no = (n_out + 1) // 2
    ep = lax.axis_index("ep")
    chip, core = ep // 2, ep % 2
    mate = chip * 2 + (1 - core)
    opp = (1 - chip) * 2 + core

    def at(start, size):
        return pl.ds(start if isinstance(start, int) else pl.multiple_of(start, cap), size)

    def w_copies(e):
        slot = lax.rem(e, W_SLOTS)
        return (pltpu.make_async_copy(w_in.at[e], wi.at[slot], w_sem.at[0, slot]),
                pltpu.make_async_copy(w_out.at[e], wo.at[slot], w_sem.at[1, slot]))

    barrier = pltpu.get_barrier_semaphore()
    signal(barrier, ep=mate)
    signal(barrier, ep=opp)
    for e in range(W_SLOTS):
        for c in w_copies(e):
            c.start()

    def d_copy(m):
        return remote(xsend.at[at(m * cap, cap)], land.at[at((2 * m + core) * cap, cap)], d_ss, d_rs.at[m], ep=opp)

    def f_copy(m):
        r = at((2 * m + core) * cap, cap)
        return remote(land.at[r], land.at[r], f_ss, f_rs.at[m], ep=mate)

    def p_copy(e):
        return remote(chip_p.at[at(core * slots + e * cap, cap)], pland.at[at(e * cap, cap)], p_ss, p_rs.at[e], ep=mate)

    def r_copy(m):
        return remote(rsend.at[at(m * cap, cap)], rland.at[at((2 * m + core) * cap, cap)], r_ss, r_rs.at[m], ep=opp)

    def g_copy(m):
        r = at((2 * m + core) * cap, cap)
        return remote(rland.at[r], rland.at[r], g_ss, g_rs.at[m], ep=mate)

    def if_in(block, total, f):
        if total % 2:
            pl.when(block < total)(f)
        else:
            f()

    lane = lax.broadcasted_iota(I32, (cap, LANES), 1)
    sub = lax.broadcasted_iota(I32, (cap, LANES), 0)
    t_half = LANES // 2

    def tokens_of(lanes, i):
        return jnp.where(lanes < t_half, lanes, lanes + (n_tok - t_half)) + t_half * i

    their = (1 - chip) * rows
    mine = chip * rows

    def gather_block(m):
        t = jnp.zeros((cap, LANES), I32)
        for i in range(rows):
            pos = meta_v[1, pl.ds(their + i, 1), :]
            t = t + jnp.where(jnp.broadcast_to(pos, (cap, LANES)) == sub + (2 * m + core) * cap, tokens_of(lane, i), 0)
        at_chip = jnp.sum(t.astype(F32), axis=1, keepdims=True).astype(I32)
        return spread(jnp.broadcast_to(at_chip, (cap, LANES)), 2 * n_tok, lane)

    def gather_send(m0, count):
        with jax.named_scope("send_group"):
            hot = jnp.concatenate([gather_block(m0 + k) for k in range(count)], axis=0)
            xsend[at(m0 * cap, count * cap), :] = jnp.dot(hot, chip_tok[...], preferred_element_type=F32).astype(BF16)

        @pl.when(m0 == 0)
        def _():
            pl.semaphore_wait(barrier, 2)

        for k in range(count):
            pl.when(2 * (m0 + k) + core < n_out)(lambda k=k: d_copy(m0 + k).start())

    gather_send(0, 1)

    @pl.loop(0, no // 2)
    def _(g):
        gather_send(2 * g + 1, 2)

    mate_rows = at((1 - core) * n_tok, n_tok)

    @pl.loop(0, n_exp // 2)
    def _(g):
        with jax.named_scope("own_gather"):
            hot = jnp.concatenate(
                [spread(column(meta_v[0, pl.ds(mine + core * n_exp + 2 * g + k, 1), :] - mate * n_tok, cap), n_tok, lane)
                 for k in range(2)], axis=0)
            r = at(2 * g * cap, 2 * cap)
            xbuf[r, :] = xown[r, :] + jnp.dot(hot, chip_tok[mate_rows, :], preferred_element_type=F32).astype(BF16)

    @pl.loop(0, no)
    def _(b):
        local[at(b * 2 * cap, 2 * cap), :] = jnp.zeros((2 * cap, d_model), BF16)

    @pl.loop(0, n_exp)
    def _(b):
        chip_p[at(b * 2 * cap, 2 * cap), :] = jnp.zeros((2 * cap, d_model), BF16)

    def forward(m):
        def go():
            with jax.named_scope("forward"):
                d_copy(m).wait_recv()
                f_copy(m).start()

        if_in(2 * m + core, n_out, go)

    lane_row = lax.broadcasted_iota(I32, (1, LANES), 1)
    listtok[...] = table([meta_v[1, pl.ds(mine + i, 1), :] for i in range(rows)],
                         [tokens_of(lane_row, i) >> 7 for i in range(rows)],
                         [tokens_of(lane_row, i) & (LANES - 1) for i in range(rows)])
    before = below((rows, rows), lambda x: lax.rem(x, n_exp) * 2 + x // n_exp) - jnp.ones((rows, rows), BF16)
    upper = below((cap, cap), lambda x: -x)
    ones = jnp.ones((cap, cap), BF16)
    for h in range(2):
        ids = meta_v[0, h * rows:(h + 1) * rows, :]
        need = (ids >= 2 * n_tok) if h == 0 else (ids < 2 * n_tok)
        flag = jnp.where(need, 1.0, 0.0).astype(BF16)
        slot_sum = jnp.dot(flag, ones, preferred_element_type=F32).astype(BF16)
        place = jnp.dot(flag, upper, preferred_element_type=F32) + jnp.dot(before, slot_sum, preferred_element_type=F32)
        back_at[h * rows:(h + 1) * rows, :] = jnp.where(need, place.astype(I32) + k_rows, FAR)

    forward(0)

    back_pos = [back_at[pl.ds(their + i, 1), :] for i in range(rows)]
    back_ids = [meta_v[0, pl.ds(their + i, 1), :] for i in range(rows)]
    tokrow[...] = table(back_pos, [i >> 7 for i in back_ids], [i & (LANES - 1) for i in back_ids])
    f_tile = 512
    n_f = d_ff // f_tile

    def m_of(e):
        return e - (n_exp - nc)

    def pack_return(e):
        with jax.named_scope("pwait"):
            p_copy(e).wait_recv()
        chip_p[at((1 - core) * slots + e * cap, cap), :] = pland[at(e * cap, cap), :]
        m = m_of(e)

        @pl.when(m >= 0)
        def _():
            parts = []
            for i in range(rows):
                pos = back_at[pl.ds(mine + i, 1), :]
                parts.append(jnp.where(jnp.broadcast_to(pos, (cap, LANES)) == sub + (2 * m + core) * cap, 1.0, 0.0).astype(BF16))
            hot = jnp.concatenate(parts, axis=1)
            rsend[at(m * cap, cap), :] = jnp.dot(hot, chip_p[...], preferred_element_type=F32).astype(BF16)
            r_copy(m).start()

    @pl.loop(0, n_exp)
    def _(e):
        slot = lax.rem(e, W_SLOTS)

        mine_e = at(e * cap, cap)

        def take_block():
            def go():
                with jax.named_scope("fwait"):
                    f_copy(e).wait_recv()

            if_in(2 * e + 1 - core, n_out, go)
            for k in range(2):
                @pl.when(2 * e + k < n_out)
                def _():
                    r = at((2 * e + k) * cap, cap)
                    local[r, :] = land[r, :]

        def fill():
            pl.when(e < no)(take_block)
            wanted = column(meta_v[0, pl.ds(mine + core * n_exp + e, 1), :], cap) - (1 - chip) * (2 * n_tok)
            hot = jnp.concatenate(
                [jnp.where(wanted == jnp.broadcast_to(listtok[j:j + 1, :], (cap, LANES)), 1.0, 0.0).astype(BF16)
                 for j in range(n_out)], axis=1)
            xbuf[mine_e, :] = xbuf[mine_e, :] + jnp.dot(hot, local[0:k_out, :], preferred_element_type=F32).astype(BF16)
            with jax.named_scope("wwait"):
                for c in w_copies(e):
                    c.wait()
            sum_o[...] = jnp.zeros((cap, d_model), F32)

        soon = (m_of(e - 1) == 0) | (m_of(e - 1) == 1)

        @pl.loop(0, 2)
        def _(half):
            @pl.when((e > 0) & ((half == 0) == soon))
            def _():
                pack_return(e - 1)

            pl.when(half == 0)(fill)

            @pl.when((half == 1) & (e + 1 < no) & (m_of(e) != 0) & (m_of(e) != 1))
            def _():
                forward(e + 1)

            x = xbuf[mine_e, :]
            o = None
            for f in range(n_f // 2):
                fs = at(half * (d_ff // 2) + f * f_tile, f_tile)
                pre = jnp.dot(x, wi[slot, :, fs], preferred_element_type=F32)
                h = jax.nn.gelu(pre, approximate=True).astype(BF16)
                part = jnp.dot(h, wo[slot, fs, :], preferred_element_type=F32)
                o = part if o is None else o + part
            sum_o[...] = sum_o[...] + o

        gcol = column(gate_v[pl.ds(e, 1), :], cap)
        chip_p[at(core * slots + e * cap, cap), :] = (
            jnp.concatenate([gcol] * (d_model // LANES), axis=1) * sum_o[...]).astype(BF16)
        p_copy(e).start()

        @pl.when((e + 1 < no) & ((m_of(e) == 0) | (m_of(e) == 1)))
        def _():
            forward(e + 1)

        @pl.when(e + W_SLOTS < n_exp)
        def _():
            for c in w_copies(e + W_SLOTS):
                c.start()

    n_blk = n_tok // (2 * cap)
    blk = 2 * cap
    sub_b = lax.broadcasted_iota(I32, (blk, LANES), 0) + ep * n_tok
    early = min(nc - 3, 10 - nc)

    def forward_back(m):
        with jax.named_scope("rwait"):
            r_copy(m).wait_recv()
            g_copy(m).start()

    def back_wait(m):
        with jax.named_scope("gwait"):
            g_copy(m).wait_recv()

    pl.loop(0, early)(forward_back)
    with jax.named_scope("pack_last"):
        pack_return(n_exp - 1)
    pl.loop(0, early)(back_wait)

    def owners(row, b):
        return jnp.where(jnp.broadcast_to(row, (blk, LANES)) == sub_b + b * blk, 1.0, 0.0).astype(BF16)

    @pl.loop(0, n_blk)
    def _(b):
        with jax.named_scope("early_back"):
            hot = jnp.concatenate([owners(tokrow[pl.ds(i, 1), :], b) for i in range(2 * early)], axis=1)
            own = chip_tok[at(core * n_tok + b * blk, blk), :].astype(F32)
            acc[at(b * blk, blk), :] = own + jnp.dot(hot, rland[0:early * 2 * cap, :], preferred_element_type=F32)

    @pl.loop(0, n_blk)
    def _(b):
        @pl.when(b == n_blk // 2)
        def _():
            forward_back(early)

        with jax.named_scope("own_scatter"):
            r = at(b * blk, blk)
            hot = jnp.concatenate([owners(meta_v[0, pl.ds(mine + i, 1), :], b) for i in range(rows)], axis=1)
            acc[r, :] = acc[r, :] + jnp.dot(hot, chip_p[...], preferred_element_type=F32)

    def combine(m):
        ids = [tokrow[pl.ds(2 * m + k, 1), :] for k in range(2)]
        back_wait(m)
        back = rland[at(2 * m * cap, 2 * cap), :]

        @pl.loop(0, n_blk)
        def _(b):
            r = at(b * blk, blk)
            hot = jnp.concatenate([owners(i, b) for i in ids], axis=1)
            acc[r, :] = acc[r, :] + jnp.dot(hot, back, preferred_element_type=F32)

    last = nc - 1

    @pl.loop(0, n_blk)
    def _(b):
        hot_last[at(b * blk, blk), :] = jnp.concatenate(
            [owners(tokrow[2 * last + k:2 * last + k + 1, :], b) for k in range(2)], axis=1)

    def sent(sem, buf, blocks):
        r = buf.at[0:blocks * cap]
        remote(r, r, sem, sem, ep=mate).wait_send()

    def sent_out(blocks):
        sent(d_ss, xsend, blocks)
        sent(f_ss, land, blocks)

    if n_out % 2:
        pl.when(core == 0)(lambda: sent_out(no))
        pl.when(core == 1)(lambda: sent_out(no - 1))
    else:
        sent_out(no)
    sent(p_ss, chip_p, n_exp)

    @pl.loop(early, nc - 2)
    def _(m):
        forward_back(m + 1)
        combine(m)

    combine(nc - 2)
    forward_back(last)
    sent(r_ss, rsend, nc)
    back_wait(last)
    with jax.named_scope("last_add"):
        back = rland[2 * last * cap:2 * nc * cap, :]
        for b in range(n_blk):
            r = at(b * blk, blk)
            out[r, :] = (acc[r, :] + jnp.dot(hot_last[r, :], back, preferred_element_type=F32)).astype(BF16)

    sent(g_ss, rland, nc)


def solution(mesh):
    n_dp, n_ep = mesh.shape["dp"], mesh.shape["ep"]
    row_spec = P(("dp", "ep"), None)
    expert_spec = P("ep", None, None)
    dma = pltpu.SemaphoreType.DMA
    any_spec = pl.BlockSpec(memory_space=pl.ANY)
    vmem_spec = pl.BlockSpec(memory_space=pltpu.VMEM)

    def local_layer(tok, idx, gate, w_in, w_out):
        n_tok, d_model = tok.shape
        n_exp, cap = idx.shape
        d_ff = w_in.shape[2]
        slots = n_exp * cap
        sizes = tuple((slots + i * cap, slots + j * cap) for i, j in LENGTHS)
        n_dev = n_dp * n_ep

        chip_tok, xown, meta, bucket = pl.pallas_call(
            functools.partial(plan_kernel, n_dp, n_ep, sizes),
            out_shape=(jax.ShapeDtypeStruct((2 * n_tok, d_model), BF16),
                       jax.ShapeDtypeStruct((slots, d_model), BF16),
                       jax.ShapeDtypeStruct((2, 4 * n_exp, cap), I32),
                       jax.ShapeDtypeStruct((1,), I32)),
            in_specs=[any_spec] * 2,
            out_specs=(vmem_spec, vmem_spec, vmem_spec, any_spec),
            scratch_shapes=[
                pltpu.VMEM((n_dev, n_exp, cap), I32),
                pltpu.SMEM((1,), I32),
                dma((3,)), dma, dma((2,)), dma, dma,
            ],
            compiler_params=pltpu.CompilerParams(
                collective_id=0, has_side_effects=True, vmem_limit_bytes=58 * 1024 * 1024),
        )(tok, idx)

        def branch(i):
            k_out, k_rows = sizes[i]
            no = (k_out // cap + 1) // 2
            nc = k_rows // (2 * cap)

            def run(chip_tok, xown, meta, gate, w_in, w_out):
                return pl.pallas_call(
                    functools.partial(layer_kernel, k_out, k_rows),
                    out_shape=jax.ShapeDtypeStruct((n_tok, d_model), BF16),
                    in_specs=[vmem_spec] * 4 + [any_spec] * 2,
                    out_specs=vmem_spec,
                    scratch_shapes=[
                        pltpu.VMEM(((no // 2 * 2 + 1) * cap, d_model), BF16),
                        pltpu.VMEM((2 * no * cap, d_model), BF16),
                        pltpu.VMEM((2 * no * cap, d_model), BF16),
                        pltpu.VMEM((slots, d_model), BF16),
                        pltpu.VMEM((2 * slots, d_model), BF16),
                        pltpu.VMEM((slots, d_model), BF16),
                        pltpu.VMEM((nc * cap, d_model), BF16),
                        pltpu.VMEM((2 * nc * cap, d_model), BF16),
                        pltpu.VMEM((2 * n_exp, cap), I32),
                        pltpu.VMEM((2 * n_exp, cap), I32),
                        pltpu.VMEM((4 * n_exp, cap), I32),
                        pltpu.VMEM((n_tok, 2 * cap), BF16),
                        pltpu.VMEM((n_tok, d_model), F32),
                        pltpu.VMEM((cap, d_model), F32),
                        pltpu.VMEM((W_SLOTS, d_model, d_ff), BF16),
                        pltpu.VMEM((W_SLOTS, d_ff, d_model), BF16),
                        dma((2, W_SLOTS)),
                        dma, dma((no,)), dma, dma((no,)), dma, dma((n_exp,)), dma, dma((nc,)), dma, dma((nc,)),
                    ],
                    compiler_params=pltpu.CompilerParams(
                        collective_id=1 + i, has_side_effects=True, vmem_limit_bytes=54 * 1024 * 1024),
                )(chip_tok, xown, meta, gate, w_in, w_out)

            return run

        return lax.switch(bucket[0], [branch(i) for i in range(len(sizes))], chip_tok, xown, meta, gate, w_in, w_out)

    return jax.shard_map(local_layer, mesh=mesh, in_specs=(row_spec, row_spec, row_spec, expert_spec, expert_spec),
                         out_specs=row_spec, check_vma=False)
```

```python
import functools

import jax
import jax.numpy as jnp
from jax import lax
from jax.experimental import pallas as pl
from jax.experimental.pallas import tpu as pltpu
from jax.sharding import PartitionSpec as P

F32, BF16, I32 = jnp.float32, jnp.bfloat16, jnp.int32
W_SLOTS = 3
LANES = 128
FAR = 1 << 20
LENGTHS = ((1, 2), (2, 4), (3, 6), (5, 8), (8, 8))


def remote(src, dst, ss, rs, **dev):
    return pltpu.make_async_remote_copy(src_ref=src, dst_ref=dst, send_sem=ss, recv_sem=rs,
                                        device_id=dev, device_id_type=pl.DeviceIdType.MESH)


def signal(sem, **dev):
    pl.semaphore_signal(sem, inc=1, device_id=dev, device_id_type=pl.DeviceIdType.MESH)


def spread(col, width, lane):
    return jnp.concatenate(
        [jnp.where(col == lane + LANES * j, 1.0, 0.0).astype(BF16) for j in range(width // LANES)], axis=1)


def column(row, cap):
    return jnp.broadcast_to(row, (LANES, cap)).T


def table(pos, his, los):
    n = len(pos)
    sub_b = lax.broadcasted_iota(I32, (n, LANES), 0)
    sub_l = lax.broadcasted_iota(I32, (LANES, LANES), 0)
    blocks, his_b, los_b, lanes = [], [], [], []
    for p, hi, lo in zip(pos, his, los):
        b = jnp.where(jnp.broadcast_to(p >> 7, sub_b.shape) == sub_b, 1.0, 0.0)
        blocks.append(b.astype(BF16))
        his_b.append((b * hi.astype(F32)).astype(BF16))
        los_b.append((b * lo.astype(F32)).astype(BF16))
        lanes.append(jnp.where(jnp.broadcast_to(p & (LANES - 1), sub_l.shape) == sub_l, 1.0, 0.0).astype(BF16))
    left = jnp.concatenate([jnp.concatenate(x, axis=1) for x in (blocks, his_b, los_b)], axis=0)
    out = lax.dot_general(left, jnp.concatenate(lanes, axis=1), (((1,), (1,)), ((), ())), preferred_element_type=F32)
    ids = (out[n:2 * n] * LANES + out[2 * n:3 * n]).astype(I32)
    return jnp.where(out[0:n] > 0.5, ids, -FAR)


def below(shape, key):
    r, c = (key(lax.broadcasted_iota(I32, shape, a)) for a in (0, 1))
    return jnp.where(c < r, 1.0, 0.0).astype(BF16)


def plan_kernel(n_dp, n_ep, sizes, tok, idx, chip_tok, xown, meta, bucket, idx_g, pick_s, loc_sem, idx_ss, idx_rs, tok_ss, tok_rs):
    n_tok = tok.shape[0]
    n_exp, cap = idx.shape
    dp, ep = lax.axis_index("dp"), lax.axis_index("ep")
    me = dp * n_ep + ep
    n_dev = n_dp * n_ep
    core = lax.rem(ep, 2)
    own_rows = chip_tok.at[pl.ds(pl.multiple_of(core * n_tok, n_tok), n_tok)]
    own_idx = pltpu.make_async_copy(idx, idx_g.at[me], loc_sem.at[0])
    own_tok = pltpu.make_async_copy(tok, own_rows, loc_sem.at[1])
    own_idx.start()
    own_tok.start()
    barrier = pltpu.get_barrier_semaphore()
    offsets = [(a, b) for a in range(n_dp - 1, -1, -1) for b in range(n_ep - 1, -1, -1) if a or b]
    others = [(lax.rem(dp + a, n_dp), lax.rem(ep + b, n_ep)) for a, b in offsets]
    n_far = (n_dp - 1) * n_ep
    for d, e in others:
        signal(barrier, dp=d, ep=e)
    own_idx.wait()
    pl.semaphore_wait(barrier, n_dev - 1)
    for k, (d, e) in enumerate(others):
        remote(idx_g.at[me], idx_g.at[me], idx_ss, idx_rs.at[0 if k < n_far else 1], dp=d, ep=e).start()

    def blocks(n, k):
        r = idx_g.at[0:n]
        return remote(r, r, idx_ss, idx_rs.at[k], dp=dp, ep=ep + 1 - 2 * core)

    own_tok.wait()
    tok_out = remote(own_rows, own_rows, tok_ss, tok_rs, dp=dp, ep=ep + 1 - 2 * core)
    tok_out.start()
    lane = lax.broadcasted_iota(I32, (cap, LANES), 1)

    @pl.loop(0, n_exp // 2)
    def _(g):
        hot = jnp.concatenate(
            [spread(column(idx_g[me, pl.ds(2 * g + k, 1), :] - ep * n_tok, cap), n_tok, lane) for k in range(2)], axis=0)
        xown[pl.ds(pl.multiple_of(2 * g * cap, 2 * cap), 2 * cap), :] = jnp.dot(
            hot, own_rows[...], preferred_element_type=F32).astype(BF16)

    rows = 2 * n_exp
    half = 2 * n_tok
    t_lanes = LANES // 2
    t_rows = half // t_lanes

    upper_t = jnp.where(lax.broadcasted_iota(I32, (t_lanes, t_lanes), 0) < lax.broadcasted_iota(I32, (t_lanes, t_lanes), 1),
                        1.0, 0.0).astype(BF16)
    ones_t = jnp.ones((t_lanes, t_lanes), BF16)
    lower = below((n_exp * t_rows, n_exp * t_rows), lambda x: x)
    sub_hi = lax.broadcasted_iota(I32, (t_rows, cap), 0)
    sub_lo = lax.broadcasted_iota(I32, (t_lanes, cap), 0)

    def presence(d, h, e):
        his, los = [], []
        for c in range(2):
            at_chip = idx_g[d * n_ep + 2 * h + c, e:e + 1, :] - (1 - h) * half
            his.append(jnp.where(jnp.broadcast_to(at_chip >> 6, sub_hi.shape) == sub_hi, 1.0, 0.0).astype(BF16))
            los.append(jnp.where(jnp.broadcast_to(at_chip & (t_lanes - 1), sub_lo.shape) == sub_lo, 1.0, 0.0).astype(BF16))
        count = lax.dot_general(jnp.concatenate(his, axis=1), jnp.concatenate(los, axis=1),
                                (((1,), (1,)), ((), ())), preferred_element_type=F32)
        return jnp.minimum(count, 1.0)

    def crosses(d, h):
        ids = jnp.concatenate([idx_g[d * n_ep + 2 * h], idx_g[d * n_ep + 2 * h + 1]], axis=0)
        return ids, (ids >= half) if h == 0 else (ids < half)

    with jax.named_scope("A_near"):
        blocks(n_ep - 1, 1).wait_recv()

    distinct = most = None
    lists = []
    for h in range(2):
        seen = jnp.zeros((t_rows, t_lanes), F32)
        fresh = []
        for e in range(n_exp):
            here = presence(dp, h, e)
            fresh.append(here * (1.0 - seen))
            seen = jnp.maximum(seen, here)
        lists.append((seen, fresh))
        n = jnp.sum(seen)
        distinct = n if distinct is None else jnp.maximum(distinct, n)
        ids, need = crosses(dp, h)
        meta[0, h * rows:(h + 1) * rows, :] = ids
        n = jnp.sum(jnp.where(need, 1.0, 0.0))
        most = n if most is None else jnp.maximum(most, n)

    with jax.named_scope("A_far"):
        blocks(n_far, 0).wait_recv()

    for a in range(1, n_dp):
        d = lax.rem(dp + a, n_dp)
        for h in range(2):
            most = jnp.maximum(most, jnp.sum(jnp.where(crosses(d, h)[1], 1.0, 0.0)))
            seen = presence(d, h, 0)
            for e in range(1, n_exp):
                seen = jnp.maximum(seen, presence(d, h, e))
            distinct = jnp.maximum(distinct, jnp.sum(seen))
    pick = jnp.int32(0)
    for k_out, k_back in sizes[:-1]:
        pick = pick + jnp.where((distinct > k_out) | (most > k_back), 1, 0).astype(I32)
    pick_s[0] = pick
    pick_out = pltpu.make_async_copy(pick_s, bucket, loc_sem.at[2])
    pick_out.start()

    for h, (seen, fresh) in enumerate(lists):
        new = jnp.concatenate(fresh, axis=0)
        new_b = new.astype(BF16)
        row_sum = jnp.dot(new_b, ones_t, preferred_element_type=F32).astype(BF16)
        pos = (jnp.dot(new_b, upper_t, preferred_element_type=F32) + jnp.dot(lower, row_sum, preferred_element_type=F32)) * new
        place = jnp.zeros((t_rows, t_lanes), F32)
        for e in range(n_exp):
            place = place + pos[e * t_rows:(e + 1) * t_rows, :]
        place = jnp.where(seen > 0.5, place.astype(I32), FAR)
        meta[1, h * rows:(h + 1) * rows, :] = jnp.concatenate([place[0:t_rows // 2], place[t_rows // 2:]], axis=1)

    blocks(n_dev - 1, 0).wait_send()
    with jax.named_scope("A_tok"):
        tok_out.wait()
    pick_out.wait()


def layer_kernel(k_out, k_rows, chip_tok, xown, meta_v, gate_v, w_in, w_out, out,
                 xsend, land, local, xbuf, chip_p, pland, rsend, rland, listtok, tokrow, back_at, hot_last, acc, sum_o, wi, wo,
                 w_sem, d_ss, d_rs, f_ss, f_rs, p_ss, p_rs, r_ss, r_rs, g_ss, g_rs):
    n_tok, d_model = out.shape
    n_exp, d_ff = w_in.shape[0], w_in.shape[2]
    cap = gate_v.shape[1]
    slots = n_exp * cap
    rows = 2 * n_exp
    n_list = k_rows // cap
    assert n_list % 2 == 0
    nc = n_list // 2
    n_out = k_out // cap
    no = (n_out + 1) // 2
    ep = lax.axis_index("ep")
    chip, core = ep // 2, ep % 2
    mate = chip * 2 + (1 - core)
    opp = (1 - chip) * 2 + core

    def at(start, size):
        return pl.ds(start if isinstance(start, int) else pl.multiple_of(start, cap), size)

    def w_copies(e):
        slot = lax.rem(e, W_SLOTS)
        return (pltpu.make_async_copy(w_in.at[e], wi.at[slot], w_sem.at[0, slot]),
                pltpu.make_async_copy(w_out.at[e], wo.at[slot], w_sem.at[1, slot]))

    barrier = pltpu.get_barrier_semaphore()
    signal(barrier, ep=mate)
    signal(barrier, ep=opp)
    for e in range(W_SLOTS):
        for c in w_copies(e):
            c.start()

    def d_copy(m):
        return remote(xsend.at[at(m * cap, cap)], land.at[at((2 * m + core) * cap, cap)], d_ss, d_rs.at[m], ep=opp)

    def f_copy(m):
        r = at((2 * m + core) * cap, cap)
        return remote(land.at[r], land.at[r], f_ss, f_rs.at[m], ep=mate)

    def p_copy(e):
        return remote(chip_p.at[at(core * slots + e * cap, cap)], pland.at[at(e * cap, cap)], p_ss, p_rs.at[e], ep=mate)

    def r_copy(m):
        return remote(rsend.at[at(m * cap, cap)], rland.at[at((2 * m + core) * cap, cap)], r_ss, r_rs.at[m], ep=opp)

    def g_copy(m):
        r = at((2 * m + core) * cap, cap)
        return remote(rland.at[r], rland.at[r], g_ss, g_rs.at[m], ep=mate)

    def if_in(block, total, f):
        if total % 2:
            pl.when(block < total)(f)
        else:
            f()

    lane = lax.broadcasted_iota(I32, (cap, LANES), 1)
    sub = lax.broadcasted_iota(I32, (cap, LANES), 0)
    t_half = LANES // 2

    def tokens_of(lanes, i):
        return jnp.where(lanes < t_half, lanes, lanes + (n_tok - t_half)) + t_half * i

    their = (1 - chip) * rows
    mine = chip * rows

    def gather_block(m):
        t = jnp.zeros((cap, LANES), I32)
        for i in range(rows):
            pos = meta_v[1, pl.ds(their + i, 1), :]
            t = t + jnp.where(jnp.broadcast_to(pos, (cap, LANES)) == sub + (2 * m + core) * cap, tokens_of(lane, i), 0)
        at_chip = jnp.sum(t.astype(F32), axis=1, keepdims=True).astype(I32)
        return spread(jnp.broadcast_to(at_chip, (cap, LANES)), 2 * n_tok, lane)

    @pl.loop(0, no)
    def _(m):
        with jax.named_scope("send_group"):
            xsend[at(m * cap, cap), :] = jnp.dot(gather_block(m), chip_tok[...], preferred_element_type=F32).astype(BF16)

        @pl.when(m == 0)
        def _():
            pl.semaphore_wait(barrier, 2)

        pl.when(2 * m + core < n_out)(lambda: d_copy(m).start())

    mate_rows = at((1 - core) * n_tok, n_tok)

    @pl.loop(0, n_exp // 2)
    def _(g):
        with jax.named_scope("own_gather"):
            hot = jnp.concatenate(
                [spread(column(meta_v[0, pl.ds(mine + core * n_exp + 2 * g + k, 1), :] - mate * n_tok, cap), n_tok, lane)
                 for k in range(2)], axis=0)
            r = at(2 * g * cap, 2 * cap)
            xbuf[r, :] = xown[r, :] + jnp.dot(hot, chip_tok[mate_rows, :], preferred_element_type=F32).astype(BF16)

    @pl.loop(0, no)
    def _(b):
        local[at(b * 2 * cap, 2 * cap), :] = jnp.zeros((2 * cap, d_model), BF16)

    @pl.loop(0, n_exp)
    def _(b):
        chip_p[at(b * 2 * cap, 2 * cap), :] = jnp.zeros((2 * cap, d_model), BF16)

    def forward(m):
        def go():
            with jax.named_scope("forward"):
                d_copy(m).wait_recv()
                f_copy(m).start()

        if_in(2 * m + core, n_out, go)

    lane_row = lax.broadcasted_iota(I32, (1, LANES), 1)
    listtok[...] = table([meta_v[1, pl.ds(mine + i, 1), :] for i in range(rows)],
                         [tokens_of(lane_row, i) >> 7 for i in range(rows)],
                         [tokens_of(lane_row, i) & (LANES - 1) for i in range(rows)])
    before = below((rows, rows), lambda x: lax.rem(x, n_exp) * 2 + x // n_exp) - jnp.ones((rows, rows), BF16)
    upper = below((cap, cap), lambda x: -x)
    ones = jnp.ones((cap, cap), BF16)
    for h in range(2):
        ids = meta_v[0, h * rows:(h + 1) * rows, :]
        need = (ids >= 2 * n_tok) if h == 0 else (ids < 2 * n_tok)
        flag = jnp.where(need, 1.0, 0.0).astype(BF16)
        slot_sum = jnp.dot(flag, ones, preferred_element_type=F32).astype(BF16)
        place = jnp.dot(flag, upper, preferred_element_type=F32) + jnp.dot(before, slot_sum, preferred_element_type=F32)
        back_at[h * rows:(h + 1) * rows, :] = jnp.where(need, place.astype(I32) + k_rows, FAR)

    forward(0)

    back_pos = [back_at[pl.ds(their + i, 1), :] for i in range(rows)]
    back_ids = [meta_v[0, pl.ds(their + i, 1), :] for i in range(rows)]
    tokrow[...] = table(back_pos, [i >> 7 for i in back_ids], [i & (LANES - 1) for i in back_ids])
    f_tile = 512
    n_f = d_ff // f_tile

    def m_of(e):
        return e - (n_exp - nc)

    def pack_return(e):
        with jax.named_scope("pwait"):
            p_copy(e).wait_recv()
        chip_p[at((1 - core) * slots + e * cap, cap), :] = pland[at(e * cap, cap), :]
        m = m_of(e)

        @pl.when(m >= 0)
        def _():
            parts = []
            for i in range(rows):
                pos = back_at[pl.ds(mine + i, 1), :]
                parts.append(jnp.where(jnp.broadcast_to(pos, (cap, LANES)) == sub + (2 * m + core) * cap, 1.0, 0.0).astype(BF16))
            hot = jnp.concatenate(parts, axis=1)
            rsend[at(m * cap, cap), :] = jnp.dot(hot, chip_p[...], preferred_element_type=F32).astype(BF16)
            r_copy(m).start()

    @pl.loop(0, n_exp)
    def _(e):
        slot = lax.rem(e, W_SLOTS)

        mine_e = at(e * cap, cap)

        def take_block():
            def go():
                with jax.named_scope("fwait"):
                    f_copy(e).wait_recv()

            if_in(2 * e + 1 - core, n_out, go)
            for k in range(2):
                @pl.when(2 * e + k < n_out)
                def _():
                    r = at((2 * e + k) * cap, cap)
                    local[r, :] = land[r, :]

        def fill():
            pl.when(e < no)(take_block)
            wanted = column(meta_v[0, pl.ds(mine + core * n_exp + e, 1), :], cap) - (1 - chip) * (2 * n_tok)
            hot = jnp.concatenate(
                [jnp.where(wanted == jnp.broadcast_to(listtok[j:j + 1, :], (cap, LANES)), 1.0, 0.0).astype(BF16)
                 for j in range(n_out)], axis=1)
            xbuf[mine_e, :] = xbuf[mine_e, :] + jnp.dot(hot, local[0:k_out, :], preferred_element_type=F32).astype(BF16)
            with jax.named_scope("wwait"):
                for c in w_copies(e):
                    c.wait()
            sum_o[...] = jnp.zeros((cap, d_model), F32)

        soon = (m_of(e - 1) == 0) | (m_of(e - 1) == 1)

        @pl.loop(0, 2)
        def _(half):
            @pl.when((e > 0) & ((half == 0) == soon))
            def _():
                pack_return(e - 1)

            pl.when(half == 0)(fill)

            @pl.when((half == 1) & (e + 1 < no) & (m_of(e) != 0) & (m_of(e) != 1))
            def _():
                forward(e + 1)

            x = xbuf[mine_e, :]
            o = None
            for f in range(n_f // 2):
                fs = at(half * (d_ff // 2) + f * f_tile, f_tile)
                pre = jnp.dot(x, wi[slot, :, fs], preferred_element_type=F32)
                h = jax.nn.gelu(pre, approximate=True).astype(BF16)
                part = jnp.dot(h, wo[slot, fs, :], preferred_element_type=F32)
                o = part if o is None else o + part
            sum_o[...] = sum_o[...] + o

        gcol = column(gate_v[pl.ds(e, 1), :], cap)
        chip_p[at(core * slots + e * cap, cap), :] = (
            jnp.concatenate([gcol] * (d_model // LANES), axis=1) * sum_o[...]).astype(BF16)
        p_copy(e).start()

        @pl.when((e + 1 < no) & ((m_of(e) == 0) | (m_of(e) == 1)))
        def _():
            forward(e + 1)

        @pl.when(e + W_SLOTS < n_exp)
        def _():
            for c in w_copies(e + W_SLOTS):
                c.start()

    n_blk = n_tok // (2 * cap)
    blk = 2 * cap
    sub_b = lax.broadcasted_iota(I32, (blk, LANES), 0) + ep * n_tok
    early = min(nc - 3, 10 - nc)

    def forward_back(m):
        with jax.named_scope("rwait"):
            r_copy(m).wait_recv()
            g_copy(m).start()

    def back_wait(m):
        with jax.named_scope("gwait"):
            g_copy(m).wait_recv()

    pl.loop(0, early)(forward_back)
    with jax.named_scope("pack_last"):
        pack_return(n_exp - 1)
    pl.loop(0, early)(back_wait)

    def owners(row, b):
        return jnp.where(jnp.broadcast_to(row, (blk, LANES)) == sub_b + b * blk, 1.0, 0.0).astype(BF16)

    @pl.loop(0, n_blk)
    def _(b):
        with jax.named_scope("early_back"):
            hot = jnp.concatenate([owners(tokrow[pl.ds(i, 1), :], b) for i in range(2 * early)], axis=1)
            own = chip_tok[at(core * n_tok + b * blk, blk), :].astype(F32)
            acc[at(b * blk, blk), :] = own + jnp.dot(hot, rland[0:early * 2 * cap, :], preferred_element_type=F32)

    @pl.loop(0, n_blk)
    def _(b):
        @pl.when(b == n_blk // 2)
        def _():
            forward_back(early)

        with jax.named_scope("own_scatter"):
            r = at(b * blk, blk)
            hot = jnp.concatenate([owners(meta_v[0, pl.ds(mine + i, 1), :], b) for i in range(rows)], axis=1)
            acc[r, :] = acc[r, :] + jnp.dot(hot, chip_p[...], preferred_element_type=F32)

    def combine(m):
        ids = [tokrow[pl.ds(2 * m + k, 1), :] for k in range(2)]
        back_wait(m)
        back = rland[at(2 * m * cap, 2 * cap), :]

        @pl.loop(0, n_blk)
        def _(b):
            r = at(b * blk, blk)
            hot = jnp.concatenate([owners(i, b) for i in ids], axis=1)
            acc[r, :] = acc[r, :] + jnp.dot(hot, back, preferred_element_type=F32)

    last = nc - 1

    @pl.loop(0, n_blk)
    def _(b):
        hot_last[at(b * blk, blk), :] = jnp.concatenate(
            [owners(tokrow[2 * last + k:2 * last + k + 1, :], b) for k in range(2)], axis=1)

    def sent(sem, buf, blocks):
        r = buf.at[0:blocks * cap]
        remote(r, r, sem, sem, ep=mate).wait_send()

    def sent_out(blocks):
        sent(d_ss, xsend, blocks)
        sent(f_ss, land, blocks)

    if n_out % 2:
        pl.when(core == 0)(lambda: sent_out(no))
        pl.when(core == 1)(lambda: sent_out(no - 1))
    else:
        sent_out(no)
    sent(p_ss, chip_p, n_exp)

    @pl.loop(early, nc - 2)
    def _(m):
        forward_back(m + 1)
        combine(m)

    combine(nc - 2)
    forward_back(last)
    sent(r_ss, rsend, nc)
    back_wait(last)
    with jax.named_scope("last_add"):
        back = rland[2 * last * cap:2 * nc * cap, :]
        for b in range(n_blk):
            r = at(b * blk, blk)
            out[r, :] = (acc[r, :] + jnp.dot(hot_last[r, :], back, preferred_element_type=F32)).astype(BF16)

    sent(g_ss, rland, nc)


def solution(mesh):
    n_dp, n_ep = mesh.shape["dp"], mesh.shape["ep"]
    row_spec = P(("dp", "ep"), None)
    expert_spec = P("ep", None, None)
    dma = pltpu.SemaphoreType.DMA
    any_spec = pl.BlockSpec(memory_space=pl.ANY)
    vmem_spec = pl.BlockSpec(memory_space=pltpu.VMEM)

    def local_layer(tok, idx, gate, w_in, w_out):
        n_tok, d_model = tok.shape
        n_exp, cap = idx.shape
        d_ff = w_in.shape[2]
        slots = n_exp * cap
        sizes = tuple((slots + i * cap, slots + j * cap) for i, j in LENGTHS)
        n_dev = n_dp * n_ep

        chip_tok, xown, meta, bucket = pl.pallas_call(
            functools.partial(plan_kernel, n_dp, n_ep, sizes),
            out_shape=(jax.ShapeDtypeStruct((2 * n_tok, d_model), BF16),
                       jax.ShapeDtypeStruct((slots, d_model), BF16),
                       jax.ShapeDtypeStruct((2, 4 * n_exp, cap), I32),
                       jax.ShapeDtypeStruct((1,), I32)),
            in_specs=[any_spec] * 2,
            out_specs=(vmem_spec, vmem_spec, vmem_spec, any_spec),
            scratch_shapes=[
                pltpu.VMEM((n_dev, n_exp, cap), I32),
                pltpu.SMEM((1,), I32),
                dma((3,)), dma, dma((2,)), dma, dma,
            ],
            compiler_params=pltpu.CompilerParams(
                collective_id=0, has_side_effects=True, vmem_limit_bytes=58 * 1024 * 1024),
        )(tok, idx)

        def branch(i):
            k_out, k_rows = sizes[i]
            no = (k_out // cap + 1) // 2
            nc = k_rows // (2 * cap)

            def run(chip_tok, xown, meta, gate, w_in, w_out):
                return pl.pallas_call(
                    functools.partial(layer_kernel, k_out, k_rows),
                    out_shape=jax.ShapeDtypeStruct((n_tok, d_model), BF16),
                    in_specs=[vmem_spec] * 4 + [any_spec] * 2,
                    out_specs=vmem_spec,
                    scratch_shapes=[
                        pltpu.VMEM((no * cap, d_model), BF16),
                        pltpu.VMEM((2 * no * cap, d_model), BF16),
                        pltpu.VMEM((2 * no * cap, d_model), BF16),
                        pltpu.VMEM((slots, d_model), BF16),
                        pltpu.VMEM((2 * slots, d_model), BF16),
                        pltpu.VMEM((slots, d_model), BF16),
                        pltpu.VMEM((nc * cap, d_model), BF16),
                        pltpu.VMEM((2 * nc * cap, d_model), BF16),
                        pltpu.VMEM((2 * n_exp, cap), I32),
                        pltpu.VMEM((2 * n_exp, cap), I32),
                        pltpu.VMEM((4 * n_exp, cap), I32),
                        pltpu.VMEM((n_tok, 2 * cap), BF16),
                        pltpu.VMEM((n_tok, d_model), F32),
                        pltpu.VMEM((cap, d_model), F32),
                        pltpu.VMEM((W_SLOTS, d_model, d_ff), BF16),
                        pltpu.VMEM((W_SLOTS, d_ff, d_model), BF16),
                        dma((2, W_SLOTS)),
                        dma, dma((no,)), dma, dma((no,)), dma, dma((n_exp,)), dma, dma((nc,)), dma, dma((nc,)),
                    ],
                    compiler_params=pltpu.CompilerParams(
                        collective_id=1 + i, has_side_effects=True, vmem_limit_bytes=54 * 1024 * 1024),
                )(chip_tok, xown, meta, gate, w_in, w_out)

            return run

        return lax.switch(bucket[0], [branch(i) for i in range(len(sizes))], chip_tok, xown, meta, gate, w_in, w_out)

    return jax.shard_map(local_layer, mesh=mesh, in_specs=(row_spec, row_spec, row_spec, expert_spec, expert_spec),
                         out_specs=row_spec, check_vma=False)
```

```python
import functools

import jax
import jax.numpy as jnp
from jax import lax
from jax.experimental import pallas as pl
from jax.experimental.pallas import tpu as pltpu
from jax.sharding import PartitionSpec as P

F32, BF16, I32 = jnp.float32, jnp.bfloat16, jnp.int32
W_SLOTS = 3
LANES = 128
FAR = 1 << 20
LENGTHS = ((1, 2), (2, 4), (3, 6), (5, 8), (8, 8))


def remote(src, dst, ss, rs, **dev):
    return pltpu.make_async_remote_copy(src_ref=src, dst_ref=dst, send_sem=ss, recv_sem=rs,
                                        device_id=dev, device_id_type=pl.DeviceIdType.MESH)


def signal(sem, **dev):
    pl.semaphore_signal(sem, inc=1, device_id=dev, device_id_type=pl.DeviceIdType.MESH)


def spread(col, width, lane):
    return jnp.concatenate(
        [jnp.where(col == lane + LANES * j, 1.0, 0.0).astype(BF16) for j in range(width // LANES)], axis=1)


def column(row, cap):
    return jnp.broadcast_to(row, (LANES, cap)).T


def table(pos, his, los):
    n = len(pos)
    sub_b = lax.broadcasted_iota(I32, (n, LANES), 0)
    sub_l = lax.broadcasted_iota(I32, (LANES, LANES), 0)
    blocks, his_b, los_b, lanes = [], [], [], []
    for p, hi, lo in zip(pos, his, los):
        b = jnp.where(jnp.broadcast_to(p >> 7, sub_b.shape) == sub_b, 1.0, 0.0)
        blocks.append(b.astype(BF16))
        his_b.append((b * hi.astype(F32)).astype(BF16))
        los_b.append((b * lo.astype(F32)).astype(BF16))
        lanes.append(jnp.where(jnp.broadcast_to(p & (LANES - 1), sub_l.shape) == sub_l, 1.0, 0.0).astype(BF16))
    left = jnp.concatenate([jnp.concatenate(x, axis=1) for x in (blocks, his_b, los_b)], axis=0)
    out = lax.dot_general(left, jnp.concatenate(lanes, axis=1), (((1,), (1,)), ((), ())), preferred_element_type=F32)
    ids = (out[n:2 * n] * LANES + out[2 * n:3 * n]).astype(I32)
    return jnp.where(out[0:n] > 0.5, ids, -FAR)


def below(shape, key):
    r, c = (key(lax.broadcasted_iota(I32, shape, a)) for a in (0, 1))
    return jnp.where(c < r, 1.0, 0.0).astype(BF16)


def plan_kernel(n_dp, n_ep, sizes, tok, idx, chip_tok, xown, meta, bucket, idx_g, pick_s, loc_sem, idx_ss, idx_rs, tok_ss, tok_rs):
    n_tok = tok.shape[0]
    n_exp, cap = idx.shape
    dp, ep = lax.axis_index("dp"), lax.axis_index("ep")
    me = dp * n_ep + ep
    n_dev = n_dp * n_ep
    core = lax.rem(ep, 2)
    own_rows = chip_tok.at[pl.ds(pl.multiple_of(core * n_tok, n_tok), n_tok)]
    own_idx = pltpu.make_async_copy(idx, idx_g.at[me], loc_sem.at[0])
    own_tok = pltpu.make_async_copy(tok, own_rows, loc_sem.at[1])
    own_idx.start()
    own_tok.start()
    barrier = pltpu.get_barrier_semaphore()
    offsets = [(a, b) for a in range(n_dp - 1, -1, -1) for b in range(n_ep - 1, -1, -1) if a or b]
    others = [(lax.rem(dp + a, n_dp), lax.rem(ep + b, n_ep)) for a, b in offsets]
    n_far = (n_dp - 1) * n_ep
    for d, e in others:
        signal(barrier, dp=d, ep=e)
    own_idx.wait()
    pl.semaphore_wait(barrier, n_dev - 1)
    for k, (d, e) in enumerate(others):
        remote(idx_g.at[me], idx_g.at[me], idx_ss, idx_rs.at[0 if k < n_far else 1], dp=d, ep=e).start()

    def blocks(n, k):
        r = idx_g.at[0:n]
        return remote(r, r, idx_ss, idx_rs.at[k], dp=dp, ep=ep + 1 - 2 * core)

    own_tok.wait()
    tok_out = remote(own_rows, own_rows, tok_ss, tok_rs, dp=dp, ep=ep + 1 - 2 * core)
    tok_out.start()
    lane = lax.broadcasted_iota(I32, (cap, LANES), 1)

    @pl.loop(0, n_exp // 2)
    def _(g):
        hot = jnp.concatenate(
            [spread(column(idx_g[me, pl.ds(2 * g + k, 1), :] - ep * n_tok, cap), n_tok, lane) for k in range(2)], axis=0)
        xown[pl.ds(pl.multiple_of(2 * g * cap, 2 * cap), 2 * cap), :] = jnp.dot(
            hot, own_rows[...], preferred_element_type=F32).astype(BF16)

    rows = 2 * n_exp
    half = 2 * n_tok
    t_lanes = LANES // 2
    t_rows = half // t_lanes

    upper_t = jnp.where(lax.broadcasted_iota(I32, (t_lanes, t_lanes), 0) < lax.broadcasted_iota(I32, (t_lanes, t_lanes), 1),
                        1.0, 0.0).astype(BF16)
    ones_t = jnp.ones((t_lanes, t_lanes), BF16)
    lower = below((n_exp * t_rows, n_exp * t_rows), lambda x: x)
    sub_hi = lax.broadcasted_iota(I32, (t_rows, cap), 0)
    sub_lo = lax.broadcasted_iota(I32, (t_lanes, cap), 0)

    def presence(d, h, e):
        his, los = [], []
        for c in range(2):
            at_chip = idx_g[d * n_ep + 2 * h + c, e:e + 1, :] - (1 - h) * half
            his.append(jnp.where(jnp.broadcast_to(at_chip >> 6, sub_hi.shape) == sub_hi, 1.0, 0.0).astype(BF16))
            los.append(jnp.where(jnp.broadcast_to(at_chip & (t_lanes - 1), sub_lo.shape) == sub_lo, 1.0, 0.0).astype(BF16))
        count = lax.dot_general(jnp.concatenate(his, axis=1), jnp.concatenate(los, axis=1),
                                (((1,), (1,)), ((), ())), preferred_element_type=F32)
        return jnp.minimum(count, 1.0)

    def crosses(d, h):
        ids = jnp.concatenate([idx_g[d * n_ep + 2 * h], idx_g[d * n_ep + 2 * h + 1]], axis=0)
        return ids, (ids >= half) if h == 0 else (ids < half)

    with jax.named_scope("A_near"):
        blocks(n_ep - 1, 1).wait_recv()

    distinct = most = None
    lists = []
    for h in range(2):
        seen = jnp.zeros((t_rows, t_lanes), F32)
        fresh = []
        for e in range(n_exp):
            here = presence(dp, h, e)
            fresh.append(here * (1.0 - seen))
            seen = jnp.maximum(seen, here)
        lists.append((seen, fresh))
        n = jnp.sum(seen)
        distinct = n if distinct is None else jnp.maximum(distinct, n)
        ids, need = crosses(dp, h)
        meta[0, h * rows:(h + 1) * rows, :] = ids
        n = jnp.sum(jnp.where(need, 1.0, 0.0))
        most = n if most is None else jnp.maximum(most, n)

    with jax.named_scope("A_far"):
        blocks(n_far, 0).wait_recv()

    for a in range(1, n_dp):
        d = lax.rem(dp + a, n_dp)
        for h in range(2):
            most = jnp.maximum(most, jnp.sum(jnp.where(crosses(d, h)[1], 1.0, 0.0)))
            seen = presence(d, h, 0)
            for e in range(1, n_exp):
                seen = jnp.maximum(seen, presence(d, h, e))
            distinct = jnp.maximum(distinct, jnp.sum(seen))
    pick = jnp.int32(0)
    for k_out, k_back in sizes[:-1]:
        pick = pick + jnp.where((distinct > k_out) | (most > k_back), 1, 0).astype(I32)
    pick_s[0] = pick
    pick_out = pltpu.make_async_copy(pick_s, bucket, loc_sem.at[2])
    pick_out.start()

    for h, (seen, fresh) in enumerate(lists):
        new = jnp.concatenate(fresh, axis=0)
        new_b = new.astype(BF16)
        row_sum = jnp.dot(new_b, ones_t, preferred_element_type=F32).astype(BF16)
        pos = (jnp.dot(new_b, upper_t, preferred_element_type=F32) + jnp.dot(lower, row_sum, preferred_element_type=F32)) * new
        place = jnp.zeros((t_rows, t_lanes), F32)
        for e in range(n_exp):
            place = place + pos[e * t_rows:(e + 1) * t_rows, :]
        place = jnp.where(seen > 0.5, place.astype(I32), FAR)
        meta[1, h * rows:(h + 1) * rows, :] = jnp.concatenate([place[0:t_rows // 2], place[t_rows // 2:]], axis=1)

    blocks(n_dev - 1, 0).wait_send()
    with jax.named_scope("A_tok"):
        tok_out.wait()
    pick_out.wait()


def layer_kernel(k_out, k_rows, chip_tok, xown, meta_v, gate_v, w_in, w_out, out,
                 xsend, land, local, xbuf, chip_p, pland, rsend, rland, listtok, tokrow, back_at, hot_last, acc, sum_o, wi, wo,
                 w_sem, d_ss, d_rs, f_ss, f_rs, p_ss, p_rs, r_ss, r_rs, g_ss, g_rs):
    n_tok, d_model = out.shape
    n_exp, d_ff = w_in.shape[0], w_in.shape[2]
    cap = gate_v.shape[1]
    slots = n_exp * cap
    rows = 2 * n_exp
    n_list = k_rows // cap
    assert n_list % 2 == 0
    nc = n_list // 2
    n_out = k_out // cap
    no = (n_out + 1) // 2
    ep = lax.axis_index("ep")
    chip, core = ep // 2, ep % 2
    mate = chip * 2 + (1 - core)
    opp = (1 - chip) * 2 + core

    def at(start, size):
        return pl.ds(start if isinstance(start, int) else pl.multiple_of(start, cap), size)

    def w_copies(e):
        slot = lax.rem(e, W_SLOTS)
        return (pltpu.make_async_copy(w_in.at[e], wi.at[slot], w_sem.at[0, slot]),
                pltpu.make_async_copy(w_out.at[e], wo.at[slot], w_sem.at[1, slot]))

    barrier = pltpu.get_barrier_semaphore()
    signal(barrier, ep=mate)
    signal(barrier, ep=opp)
    for e in range(W_SLOTS):
        for c in w_copies(e):
            c.start()

    def d_copy(m):
        return remote(xsend.at[at(m * cap, cap)], land.at[at((2 * m + core) * cap, cap)], d_ss, d_rs.at[m], ep=opp)

    def f_copy(m):
        r = at((2 * m + core) * cap, cap)
        return remote(land.at[r], land.at[r], f_ss, f_rs.at[m], ep=mate)

    def p_copy(e):
        return remote(chip_p.at[at(core * slots + e * cap, cap)], pland.at[at(e * cap, cap)], p_ss, p_rs.at[e], ep=mate)

    def r_copy(m):
        return remote(rsend.at[at(m * cap, cap)], rland.at[at((2 * m + core) * cap, cap)], r_ss, r_rs.at[m], ep=opp)

    def g_copy(m):
        r = at((2 * m + core) * cap, cap)
        return remote(rland.at[r], rland.at[r], g_ss, g_rs.at[m], ep=mate)

    def if_in(block, total, f):
        if total % 2:
            pl.when(block < total)(f)
        else:
            f()

    lane = lax.broadcasted_iota(I32, (cap, LANES), 1)
    sub = lax.broadcasted_iota(I32, (cap, LANES), 0)
    t_half = LANES // 2

    def tokens_of(lanes, i):
        return jnp.where(lanes < t_half, lanes, lanes + (n_tok - t_half)) + t_half * i

    their = (1 - chip) * rows
    mine = chip * rows

    def gather_block(m):
        t = jnp.zeros((cap, LANES), I32)
        for i in range(rows):
            pos = meta_v[1, pl.ds(their + i, 1), :]
            t = t + jnp.where(jnp.broadcast_to(pos, (cap, LANES)) == sub + (2 * m + core) * cap, tokens_of(lane, i), 0)
        at_chip = jnp.sum(t.astype(F32), axis=1, keepdims=True).astype(I32)
        return spread(jnp.broadcast_to(at_chip, (cap, LANES)), 2 * n_tok, lane)

    @pl.loop(0, no)
    def _(m):
        with jax.named_scope("send_group"):
            xsend[at(m * cap, cap), :] = jnp.dot(gather_block(m), chip_tok[...], preferred_element_type=F32).astype(BF16)

        @pl.when(m == 0)
        def _():
            pl.semaphore_wait(barrier, 2)

        pl.when(2 * m + core < n_out)(lambda: d_copy(m).start())

    mate_rows = at((1 - core) * n_tok, n_tok)

    @pl.loop(0, n_exp // 2)
    def _(g):
        with jax.named_scope("own_gather"):
            hot = jnp.concatenate(
                [spread(column(meta_v[0, pl.ds(mine + core * n_exp + 2 * g + k, 1), :] - mate * n_tok, cap), n_tok, lane)
                 for k in range(2)], axis=0)
            r = at(2 * g * cap, 2 * cap)
            xbuf[r, :] = xown[r, :] + jnp.dot(hot, chip_tok[mate_rows, :], preferred_element_type=F32).astype(BF16)

    @pl.loop(0, no)
    def _(b):
        local[at(b * 2 * cap, 2 * cap), :] = jnp.zeros((2 * cap, d_model), BF16)

    @pl.loop(0, n_exp)
    def _(b):
        chip_p[at(b * 2 * cap, 2 * cap), :] = jnp.zeros((2 * cap, d_model), BF16)

    def forward(m):
        def go():
            with jax.named_scope("forward"):
                d_copy(m).wait_recv()
                f_copy(m).start()

        if_in(2 * m + core, n_out, go)

    lane_row = lax.broadcasted_iota(I32, (1, LANES), 1)
    listtok[...] = table([meta_v[1, pl.ds(mine + i, 1), :] for i in range(rows)],
                         [tokens_of(lane_row, i) >> 7 for i in range(rows)],
                         [tokens_of(lane_row, i) & (LANES - 1) for i in range(rows)])
    before = below((rows, rows), lambda x: lax.rem(x, n_exp) * 2 + x // n_exp) - jnp.ones((rows, rows), BF16)
    upper = below((cap, cap), lambda x: -x)
    ones = jnp.ones((cap, cap), BF16)
    for h in range(2):
        ids = meta_v[0, h * rows:(h + 1) * rows, :]
        need = (ids >= 2 * n_tok) if h == 0 else (ids < 2 * n_tok)
        flag = jnp.where(need, 1.0, 0.0).astype(BF16)
        slot_sum = jnp.dot(flag, ones, preferred_element_type=F32).astype(BF16)
        place = jnp.dot(flag, upper, preferred_element_type=F32) + jnp.dot(before, slot_sum, preferred_element_type=F32)
        back_at[h * rows:(h + 1) * rows, :] = jnp.where(need, place.astype(I32) + k_rows, FAR)

    forward(0)

    back_pos = [back_at[pl.ds(their + i, 1), :] for i in range(rows)]
    back_ids = [meta_v[0, pl.ds(their + i, 1), :] for i in range(rows)]
    tokrow[...] = table(back_pos, [i >> 7 for i in back_ids], [i & (LANES - 1) for i in back_ids])
    f_tile = 1536
    n_f = d_ff // f_tile

    def m_of(e):
        return e - (n_exp - nc)

    def pack_return(e):
        with jax.named_scope("pwait"):
            p_copy(e).wait_recv()
        chip_p[at((1 - core) * slots + e * cap, cap), :] = pland[at(e * cap, cap), :]
        m = m_of(e)

        @pl.when(m >= 0)
        def _():
            parts = []
            for i in range(rows):
                pos = back_at[pl.ds(mine + i, 1), :]
                parts.append(jnp.where(jnp.broadcast_to(pos, (cap, LANES)) == sub + (2 * m + core) * cap, 1.0, 0.0).astype(BF16))
            hot = jnp.concatenate(parts, axis=1)
            rsend[at(m * cap, cap), :] = jnp.dot(hot, chip_p[...], preferred_element_type=F32).astype(BF16)
            r_copy(m).start()

    @pl.loop(0, n_exp)
    def _(e):
        slot = lax.rem(e, W_SLOTS)

        mine_e = at(e * cap, cap)

        def take_block():
            def go():
                with jax.named_scope("fwait"):
                    f_copy(e).wait_recv()

            if_in(2 * e + 1 - core, n_out, go)
            for k in range(2):
                @pl.when(2 * e + k < n_out)
                def _():
                    r = at((2 * e + k) * cap, cap)
                    local[r, :] = land[r, :]

        def fill():
            pl.when(e < no)(take_block)
            wanted = column(meta_v[0, pl.ds(mine + core * n_exp + e, 1), :], cap) - (1 - chip) * (2 * n_tok)
            hot = jnp.concatenate(
                [jnp.where(wanted == jnp.broadcast_to(listtok[j:j + 1, :], (cap, LANES)), 1.0, 0.0).astype(BF16)
                 for j in range(n_out)], axis=1)
            xbuf[mine_e, :] = xbuf[mine_e, :] + jnp.dot(hot, local[0:k_out, :], preferred_element_type=F32).astype(BF16)
            with jax.named_scope("wwait"):
                for c in w_copies(e):
                    c.wait()
            sum_o[...] = jnp.zeros((cap, d_model), F32)

        soon = (m_of(e - 1) == 0) | (m_of(e - 1) == 1)

        @pl.loop(0, 2)
        def _(half):
            @pl.when((e > 0) & ((half == 0) == soon))
            def _():
                pack_return(e - 1)

            pl.when(half == 0)(fill)

            @pl.when((half == 1) & (e + 1 < no) & (m_of(e) != 0) & (m_of(e) != 1))
            def _():
                forward(e + 1)

            x = xbuf[mine_e, :]
            o = None
            for f in range(n_f // 2):
                fs = at(half * (d_ff // 2) + f * f_tile, f_tile)
                pre = jnp.dot(x, wi[slot, :, fs], preferred_element_type=F32)
                h = jax.nn.gelu(pre, approximate=True).astype(BF16)
                part = jnp.dot(h, wo[slot, fs, :], preferred_element_type=F32)
                o = part if o is None else o + part
            sum_o[...] = sum_o[...] + o

        gcol = column(gate_v[pl.ds(e, 1), :], cap)
        chip_p[at(core * slots + e * cap, cap), :] = (
            jnp.concatenate([gcol] * (d_model // LANES), axis=1) * sum_o[...]).astype(BF16)
        p_copy(e).start()

        @pl.when((e + 1 < no) & ((m_of(e) == 0) | (m_of(e) == 1)))
        def _():
            forward(e + 1)

        @pl.when(e + W_SLOTS < n_exp)
        def _():
            for c in w_copies(e + W_SLOTS):
                c.start()

    n_blk = n_tok // (2 * cap)
    blk = 2 * cap
    sub_b = lax.broadcasted_iota(I32, (blk, LANES), 0) + ep * n_tok
    early = min(nc - 3, 10 - nc)

    def forward_back(m):
        with jax.named_scope("rwait"):
            r_copy(m).wait_recv()
            g_copy(m).start()

    def back_wait(m):
        with jax.named_scope("gwait"):
            g_copy(m).wait_recv()

    pl.loop(0, early)(forward_back)
    with jax.named_scope("pack_last"):
        pack_return(n_exp - 1)
    pl.loop(0, early)(back_wait)

    def owners(row, b):
        return jnp.where(jnp.broadcast_to(row, (blk, LANES)) == sub_b + b * blk, 1.0, 0.0).astype(BF16)

    @pl.loop(0, n_blk)
    def _(b):
        with jax.named_scope("early_back"):
            hot = jnp.concatenate([owners(tokrow[pl.ds(i, 1), :], b) for i in range(2 * early)], axis=1)
            own = chip_tok[at(core * n_tok + b * blk, blk), :].astype(F32)
            acc[at(b * blk, blk), :] = own + jnp.dot(hot, rland[0:early * 2 * cap, :], preferred_element_type=F32)

    @pl.loop(0, n_blk)
    def _(b):
        @pl.when(b == n_blk // 2)
        def _():
            forward_back(early)

        with jax.named_scope("own_scatter"):
            r = at(b * blk, blk)
            hot = jnp.concatenate([owners(meta_v[0, pl.ds(mine + i, 1), :], b) for i in range(rows)], axis=1)
            acc[r, :] = acc[r, :] + jnp.dot(hot, chip_p[...], preferred_element_type=F32)

    def combine(m):
        ids = [tokrow[pl.ds(2 * m + k, 1), :] for k in range(2)]
        back_wait(m)
        back = rland[at(2 * m * cap, 2 * cap), :]

        @pl.loop(0, n_blk)
        def _(b):
            r = at(b * blk, blk)
            hot = jnp.concatenate([owners(i, b) for i in ids], axis=1)
            acc[r, :] = acc[r, :] + jnp.dot(hot, back, preferred_element_type=F32)

    last = nc - 1

    @pl.loop(0, n_blk)
    def _(b):
        hot_last[at(b * blk, blk), :] = jnp.concatenate(
            [owners(tokrow[2 * last + k:2 * last + k + 1, :], b) for k in range(2)], axis=1)

    def sent(sem, buf, blocks):
        r = buf.at[0:blocks * cap]
        remote(r, r, sem, sem, ep=mate).wait_send()

    def sent_out(blocks):
        sent(d_ss, xsend, blocks)
        sent(f_ss, land, blocks)

    if n_out % 2:
        pl.when(core == 0)(lambda: sent_out(no))
        pl.when(core == 1)(lambda: sent_out(no - 1))
    else:
        sent_out(no)
    sent(p_ss, chip_p, n_exp)

    @pl.loop(early, nc - 2)
    def _(m):
        forward_back(m + 1)
        combine(m)

    combine(nc - 2)
    forward_back(last)
    sent(r_ss, rsend, nc)
    back_wait(last)
    with jax.named_scope("last_add"):
        back = rland[2 * last * cap:2 * nc * cap, :]
        for b in range(n_blk):
            r = at(b * blk, blk)
            out[r, :] = (acc[r, :] + jnp.dot(hot_last[r, :], back, preferred_element_type=F32)).astype(BF16)

    sent(g_ss, rland, nc)


def solution(mesh):
    n_dp, n_ep = mesh.shape["dp"], mesh.shape["ep"]
    row_spec = P(("dp", "ep"), None)
    expert_spec = P("ep", None, None)
    dma = pltpu.SemaphoreType.DMA
    any_spec = pl.BlockSpec(memory_space=pl.ANY)
    vmem_spec = pl.BlockSpec(memory_space=pltpu.VMEM)

    def local_layer(tok, idx, gate, w_in, w_out):
        n_tok, d_model = tok.shape
        n_exp, cap = idx.shape
        d_ff = w_in.shape[2]
        slots = n_exp * cap
        sizes = tuple((slots + i * cap, slots + j * cap) for i, j in LENGTHS)
        n_dev = n_dp * n_ep

        chip_tok, xown, meta, bucket = pl.pallas_call(
            functools.partial(plan_kernel, n_dp, n_ep, sizes),
            out_shape=(jax.ShapeDtypeStruct((2 * n_tok, d_model), BF16),
                       jax.ShapeDtypeStruct((slots, d_model), BF16),
                       jax.ShapeDtypeStruct((2, 4 * n_exp, cap), I32),
                       jax.ShapeDtypeStruct((1,), I32)),
            in_specs=[any_spec] * 2,
            out_specs=(vmem_spec, vmem_spec, vmem_spec, any_spec),
            scratch_shapes=[
                pltpu.VMEM((n_dev, n_exp, cap), I32),
                pltpu.SMEM((1,), I32),
                dma((3,)), dma, dma((2,)), dma, dma,
            ],
            compiler_params=pltpu.CompilerParams(
                collective_id=0, has_side_effects=True, vmem_limit_bytes=58 * 1024 * 1024),
        )(tok, idx)

        def branch(i):
            k_out, k_rows = sizes[i]
            no = (k_out // cap + 1) // 2
            nc = k_rows // (2 * cap)

            def run(chip_tok, xown, meta, gate, w_in, w_out):
                return pl.pallas_call(
                    functools.partial(layer_kernel, k_out, k_rows),
                    out_shape=jax.ShapeDtypeStruct((n_tok, d_model), BF16),
                    in_specs=[vmem_spec] * 4 + [any_spec] * 2,
                    out_specs=vmem_spec,
                    scratch_shapes=[
                        pltpu.VMEM((no * cap, d_model), BF16),
                        pltpu.VMEM((2 * no * cap, d_model), BF16),
                        pltpu.VMEM((2 * no * cap, d_model), BF16),
                        pltpu.VMEM((slots, d_model), BF16),
                        pltpu.VMEM((2 * slots, d_model), BF16),
                        pltpu.VMEM((slots, d_model), BF16),
                        pltpu.VMEM((nc * cap, d_model), BF16),
                        pltpu.VMEM((2 * nc * cap, d_model), BF16),
                        pltpu.VMEM((2 * n_exp, cap), I32),
                        pltpu.VMEM((2 * n_exp, cap), I32),
                        pltpu.VMEM((4 * n_exp, cap), I32),
                        pltpu.VMEM((n_tok, 2 * cap), BF16),
                        pltpu.VMEM((n_tok, d_model), F32),
                        pltpu.VMEM((cap, d_model), F32),
                        pltpu.VMEM((W_SLOTS, d_model, d_ff), BF16),
                        pltpu.VMEM((W_SLOTS, d_ff, d_model), BF16),
                        dma((2, W_SLOTS)),
                        dma, dma((no,)), dma, dma((no,)), dma, dma((n_exp,)), dma, dma((nc,)), dma, dma((nc,)),
                    ],
                    compiler_params=pltpu.CompilerParams(
                        collective_id=1 + i, has_side_effects=True, vmem_limit_bytes=54 * 1024 * 1024),
                )(chip_tok, xown, meta, gate, w_in, w_out)

            return run

        return lax.switch(bucket[0], [branch(i) for i in range(len(sizes))], chip_tok, xown, meta, gate, w_in, w_out)

    return jax.shard_map(local_layer, mesh=mesh, in_specs=(row_spec, row_spec, row_spec, expert_spec, expert_spec),
                         out_specs=row_spec, check_vma=False)
```

```python
import functools

import jax
import jax.numpy as jnp
from jax import lax
from jax.experimental import pallas as pl
from jax.experimental.pallas import tpu as pltpu
from jax.sharding import PartitionSpec as P

F32, BF16, I32 = jnp.float32, jnp.bfloat16, jnp.int32
W_SLOTS = 3
LANES = 128
FAR = 1 << 20
LENGTHS = ((1, 2), (2, 4), (3, 6), (5, 8), (8, 8))


def remote(src, dst, ss, rs, **dev):
    return pltpu.make_async_remote_copy(src_ref=src, dst_ref=dst, send_sem=ss, recv_sem=rs,
                                        device_id=dev, device_id_type=pl.DeviceIdType.MESH)


def signal(sem, **dev):
    pl.semaphore_signal(sem, inc=1, device_id=dev, device_id_type=pl.DeviceIdType.MESH)


def spread(col, width, lane):
    return jnp.concatenate(
        [jnp.where(col == lane + LANES * j, 1.0, 0.0).astype(BF16) for j in range(width // LANES)], axis=1)


def column(row, cap):
    return jnp.broadcast_to(row, (LANES, cap)).T


def table(pos, his, los):
    n = len(pos)
    sub_b = lax.broadcasted_iota(I32, (n, LANES), 0)
    sub_l = lax.broadcasted_iota(I32, (LANES, LANES), 0)
    blocks, his_b, los_b, lanes = [], [], [], []
    for p, hi, lo in zip(pos, his, los):
        b = jnp.where(jnp.broadcast_to(p >> 7, sub_b.shape) == sub_b, 1.0, 0.0)
        blocks.append(b.astype(BF16))
        his_b.append((b * hi.astype(F32)).astype(BF16))
        los_b.append((b * lo.astype(F32)).astype(BF16))
        lanes.append(jnp.where(jnp.broadcast_to(p & (LANES - 1), sub_l.shape) == sub_l, 1.0, 0.0).astype(BF16))
    left = jnp.concatenate([jnp.concatenate(x, axis=1) for x in (blocks, his_b, los_b)], axis=0)
    out = lax.dot_general(left, jnp.concatenate(lanes, axis=1), (((1,), (1,)), ((), ())), preferred_element_type=F32)
    ids = (out[n:2 * n] * LANES + out[2 * n:3 * n]).astype(I32)
    return jnp.where(out[0:n] > 0.5, ids, -FAR)


def below(shape, key):
    r, c = (key(lax.broadcasted_iota(I32, shape, a)) for a in (0, 1))
    return jnp.where(c < r, 1.0, 0.0).astype(BF16)


def plan_kernel(n_dp, n_ep, sizes, tok, idx, chip_tok, xown, meta, bucket, idx_g, pick_s, loc_sem, idx_ss, idx_rs, tok_ss, tok_rs):
    n_tok = tok.shape[0]
    n_exp, cap = idx.shape
    dp, ep = lax.axis_index("dp"), lax.axis_index("ep")
    me = dp * n_ep + ep
    n_dev = n_dp * n_ep
    core = lax.rem(ep, 2)
    own_rows = chip_tok.at[pl.ds(pl.multiple_of(core * n_tok, n_tok), n_tok)]
    own_idx = pltpu.make_async_copy(idx, idx_g.at[me], loc_sem.at[0])
    own_tok = pltpu.make_async_copy(tok, own_rows, loc_sem.at[1])
    own_idx.start()
    own_tok.start()
    barrier = pltpu.get_barrier_semaphore()
    offsets = [(a, b) for a in range(n_dp - 1, -1, -1) for b in range(n_ep - 1, -1, -1) if a or b]
    others = [(lax.rem(dp + a, n_dp), lax.rem(ep + b, n_ep)) for a, b in offsets]
    n_far = (n_dp - 1) * n_ep
    for d, e in others:
        signal(barrier, dp=d, ep=e)
    own_idx.wait()
    pl.semaphore_wait(barrier, n_dev - 1)
    for k, (d, e) in enumerate(others):
        remote(idx_g.at[me], idx_g.at[me], idx_ss, idx_rs.at[0 if k < n_far else 1], dp=d, ep=e).start()

    def blocks(n, k):
        r = idx_g.at[0:n]
        return remote(r, r, idx_ss, idx_rs.at[k], dp=dp, ep=ep + 1 - 2 * core)

    own_tok.wait()
    tok_out = remote(own_rows, own_rows, tok_ss, tok_rs, dp=dp, ep=ep + 1 - 2 * core)
    tok_out.start()
    lane = lax.broadcasted_iota(I32, (cap, LANES), 1)

    @pl.loop(0, n_exp // 2)
    def _(g):
        hot = jnp.concatenate(
            [spread(column(idx_g[me, pl.ds(2 * g + k, 1), :] - ep * n_tok, cap), n_tok, lane) for k in range(2)], axis=0)
        xown[pl.ds(pl.multiple_of(2 * g * cap, 2 * cap), 2 * cap), :] = jnp.dot(
            hot, own_rows[...], preferred_element_type=F32).astype(BF16)

    rows = 2 * n_exp
    half = 2 * n_tok
    t_lanes = LANES // 2
    t_rows = half // t_lanes

    upper_t = jnp.where(lax.broadcasted_iota(I32, (t_lanes, t_lanes), 0) < lax.broadcasted_iota(I32, (t_lanes, t_lanes), 1),
                        1.0, 0.0).astype(BF16)
    ones_t = jnp.ones((t_lanes, t_lanes), BF16)
    lower = below((n_exp * t_rows, n_exp * t_rows), lambda x: x)
    sub_hi = lax.broadcasted_iota(I32, (t_rows, cap), 0)
    sub_lo = lax.broadcasted_iota(I32, (t_lanes, cap), 0)

    def presence(d, h, e):
        his, los = [], []
        for c in range(2):
            at_chip = idx_g[d * n_ep + 2 * h + c, e:e + 1, :] - (1 - h) * half
            his.append(jnp.where(jnp.broadcast_to(at_chip >> 6, sub_hi.shape) == sub_hi, 1.0, 0.0).astype(BF16))
            los.append(jnp.where(jnp.broadcast_to(at_chip & (t_lanes - 1), sub_lo.shape) == sub_lo, 1.0, 0.0).astype(BF16))
        count = lax.dot_general(jnp.concatenate(his, axis=1), jnp.concatenate(los, axis=1),
                                (((1,), (1,)), ((), ())), preferred_element_type=F32)
        return jnp.minimum(count, 1.0)

    def crosses(d, h):
        ids = jnp.concatenate([idx_g[d * n_ep + 2 * h], idx_g[d * n_ep + 2 * h + 1]], axis=0)
        return ids, (ids >= half) if h == 0 else (ids < half)

    with jax.named_scope("A_near"):
        blocks(n_ep - 1, 1).wait_recv()

    distinct = most = None
    lists = []
    for h in range(2):
        seen = jnp.zeros((t_rows, t_lanes), F32)
        fresh = []
        for e in range(n_exp):
            here = presence(dp, h, e)
            fresh.append(here * (1.0 - seen))
            seen = jnp.maximum(seen, here)
        lists.append((seen, fresh))
        n = jnp.sum(seen)
        distinct = n if distinct is None else jnp.maximum(distinct, n)
        ids, need = crosses(dp, h)
        meta[0, h * rows:(h + 1) * rows, :] = ids
        n = jnp.sum(jnp.where(need, 1.0, 0.0))
        most = n if most is None else jnp.maximum(most, n)

    with jax.named_scope("A_far"):
        blocks(n_far, 0).wait_recv()

    for a in range(1, n_dp):
        d = lax.rem(dp + a, n_dp)
        for h in range(2):
            most = jnp.maximum(most, jnp.sum(jnp.where(crosses(d, h)[1], 1.0, 0.0)))
            seen = presence(d, h, 0)
            for e in range(1, n_exp):
                seen = jnp.maximum(seen, presence(d, h, e))
            distinct = jnp.maximum(distinct, jnp.sum(seen))
    pick = jnp.int32(0)
    for k_out, k_back in sizes[:-1]:
        pick = pick + jnp.where((distinct > k_out) | (most > k_back), 1, 0).astype(I32)
    pick_s[0] = pick
    pick_out = pltpu.make_async_copy(pick_s, bucket, loc_sem.at[2])
    pick_out.start()

    for h, (seen, fresh) in enumerate(lists):
        new = jnp.concatenate(fresh, axis=0)
        new_b = new.astype(BF16)
        row_sum = jnp.dot(new_b, ones_t, preferred_element_type=F32).astype(BF16)
        pos = (jnp.dot(new_b, upper_t, preferred_element_type=F32) + jnp.dot(lower, row_sum, preferred_element_type=F32)) * new
        place = jnp.zeros((t_rows, t_lanes), F32)
        for e in range(n_exp):
            place = place + pos[e * t_rows:(e + 1) * t_rows, :]
        place = jnp.where(seen > 0.5, place.astype(I32), FAR)
        meta[1, h * rows:(h + 1) * rows, :] = jnp.concatenate([place[0:t_rows // 2], place[t_rows // 2:]], axis=1)

    blocks(n_dev - 1, 0).wait_send()
    with jax.named_scope("A_tok"):
        tok_out.wait()
    pick_out.wait()


def layer_kernel(k_out, k_rows, chip_tok, xown, meta_v, gate_v, w_in, w_out, out,
                 xsend, land, local, xbuf, chip_p, pland, rsend, rland, listtok, tokrow, back_at, hot_last, acc, sum_o, wi, wo,
                 w_sem, d_ss, d_rs, f_ss, f_rs, p_ss, p_rs, r_ss, r_rs, g_ss, g_rs):
    n_tok, d_model = out.shape
    n_exp, d_ff = w_in.shape[0], w_in.shape[2]
    cap = gate_v.shape[1]
    slots = n_exp * cap
    rows = 2 * n_exp
    n_list = k_rows // cap
    assert n_list % 2 == 0
    nc = n_list // 2
    n_out = k_out // cap
    no = (n_out + 1) // 2
    ep = lax.axis_index("ep")
    chip, core = ep // 2, ep % 2
    mate = chip * 2 + (1 - core)
    opp = (1 - chip) * 2 + core

    def at(start, size):
        return pl.ds(start if isinstance(start, int) else pl.multiple_of(start, cap), size)

    def w_copies(e):
        slot = lax.rem(e, W_SLOTS)
        return (pltpu.make_async_copy(w_in.at[e], wi.at[slot], w_sem.at[0, slot]),
                pltpu.make_async_copy(w_out.at[e], wo.at[slot], w_sem.at[1, slot]))

    barrier = pltpu.get_barrier_semaphore()
    signal(barrier, ep=mate)
    signal(barrier, ep=opp)
    for e in range(W_SLOTS):
        for c in w_copies(e):
            c.start()

    def d_copy(m):
        return remote(xsend.at[at(m * cap, cap)], land.at[at((2 * m + core) * cap, cap)], d_ss, d_rs.at[m], ep=opp)

    def f_copy(m):
        r = at((2 * m + core) * cap, cap)
        return remote(land.at[r], land.at[r], f_ss, f_rs.at[m], ep=mate)

    def p_copy(e):
        return remote(chip_p.at[at(core * slots + e * cap, cap)], pland.at[at(e * cap, cap)], p_ss, p_rs.at[e], ep=mate)

    def r_copy(m):
        return remote(rsend.at[at(m * cap, cap)], rland.at[at((2 * m + core) * cap, cap)], r_ss, r_rs.at[m], ep=opp)

    def g_copy(m):
        r = at((2 * m + core) * cap, cap)
        return remote(rland.at[r], rland.at[r], g_ss, g_rs.at[m], ep=mate)

    def if_in(block, total, f):
        if total % 2:
            pl.when(block < total)(f)
        else:
            f()

    lane = lax.broadcasted_iota(I32, (cap, LANES), 1)
    sub = lax.broadcasted_iota(I32, (cap, LANES), 0)
    t_half = LANES // 2

    def tokens_of(lanes, i):
        return jnp.where(lanes < t_half, lanes, lanes + (n_tok - t_half)) + t_half * i

    their = (1 - chip) * rows
    mine = chip * rows

    def gather_block(m):
        t = jnp.zeros((cap, LANES), I32)
        for i in range(rows):
            pos = meta_v[1, pl.ds(their + i, 1), :]
            t = t + jnp.where(jnp.broadcast_to(pos, (cap, LANES)) == sub + (2 * m + core) * cap, tokens_of(lane, i), 0)
        at_chip = jnp.sum(t.astype(F32), axis=1, keepdims=True).astype(I32)
        return spread(jnp.broadcast_to(at_chip, (cap, LANES)), 2 * n_tok, lane)

    @pl.loop(0, no)
    def _(m):
        with jax.named_scope("send_group"):
            xsend[at(m * cap, cap), :] = jnp.dot(gather_block(m), chip_tok[...], preferred_element_type=F32).astype(BF16)

        @pl.when(m == 0)
        def _():
            pl.semaphore_wait(barrier, 2)

        pl.when(2 * m + core < n_out)(lambda: d_copy(m).start())

    mate_rows = at((1 - core) * n_tok, n_tok)

    @pl.loop(0, n_exp // 2)
    def _(g):
        with jax.named_scope("own_gather"):
            hot = jnp.concatenate(
                [spread(column(meta_v[0, pl.ds(mine + core * n_exp + 2 * g + k, 1), :] - mate * n_tok, cap), n_tok, lane)
                 for k in range(2)], axis=0)
            r = at(2 * g * cap, 2 * cap)
            xbuf[r, :] = xown[r, :] + jnp.dot(hot, chip_tok[mate_rows, :], preferred_element_type=F32).astype(BF16)

    @pl.loop(0, no)
    def _(b):
        local[at(b * 2 * cap, 2 * cap), :] = jnp.zeros((2 * cap, d_model), BF16)

    @pl.loop(0, n_exp)
    def _(b):
        chip_p[at(b * 2 * cap, 2 * cap), :] = jnp.zeros((2 * cap, d_model), BF16)

    def forward(m):
        def go():
            with jax.named_scope("forward"):
                d_copy(m).wait_recv()
                f_copy(m).start()

        if_in(2 * m + core, n_out, go)

    lane_row = lax.broadcasted_iota(I32, (1, LANES), 1)
    listtok[...] = table([meta_v[1, pl.ds(mine + i, 1), :] for i in range(rows)],
                         [tokens_of(lane_row, i) >> 7 for i in range(rows)],
                         [tokens_of(lane_row, i) & (LANES - 1) for i in range(rows)])
    before = below((rows, rows), lambda x: lax.rem(x, n_exp) * 2 + x // n_exp) - jnp.ones((rows, rows), BF16)
    upper = below((cap, cap), lambda x: -x)
    ones = jnp.ones((cap, cap), BF16)
    for h in range(2):
        ids = meta_v[0, h * rows:(h + 1) * rows, :]
        need = (ids >= 2 * n_tok) if h == 0 else (ids < 2 * n_tok)
        flag = jnp.where(need, 1.0, 0.0).astype(BF16)
        slot_sum = jnp.dot(flag, ones, preferred_element_type=F32).astype(BF16)
        place = jnp.dot(flag, upper, preferred_element_type=F32) + jnp.dot(before, slot_sum, preferred_element_type=F32)
        back_at[h * rows:(h + 1) * rows, :] = jnp.where(need, place.astype(I32) + k_rows, FAR)

    forward(0)

    back_pos = [back_at[pl.ds(their + i, 1), :] for i in range(rows)]
    back_ids = [meta_v[0, pl.ds(their + i, 1), :] for i in range(rows)]
    tokrow[...] = table(back_pos, [i >> 7 for i in back_ids], [i & (LANES - 1) for i in back_ids])
    f_tile = 1536
    n_f = d_ff // f_tile

    def m_of(e):
        return e - (n_exp - nc)

    def pack_return(e):
        with jax.named_scope("pwait"):
            p_copy(e).wait_recv()
        chip_p[at((1 - core) * slots + e * cap, cap), :] = pland[at(e * cap, cap), :]
        m = m_of(e)

        @pl.when(m >= 0)
        def _():
            parts = []
            for i in range(rows):
                pos = back_at[pl.ds(mine + i, 1), :]
                parts.append(jnp.where(jnp.broadcast_to(pos, (cap, LANES)) == sub + (2 * m + core) * cap, 1.0, 0.0).astype(BF16))
            hot = jnp.concatenate(parts, axis=1)
            rsend[at(m * cap, cap), :] = jnp.dot(hot, chip_p[...], preferred_element_type=F32).astype(BF16)
            r_copy(m).start()

    @pl.loop(0, n_exp)
    def _(e):
        slot = lax.rem(e, W_SLOTS)

        mine_e = at(e * cap, cap)

        def take_block():
            def go():
                with jax.named_scope("fwait"):
                    f_copy(e).wait_recv()

            if_in(2 * e + 1 - core, n_out, go)
            for k in range(2):
                @pl.when(2 * e + k < n_out)
                def _():
                    r = at((2 * e + k) * cap, cap)
                    local[r, :] = land[r, :]

        def fill():
            pl.when(e < no)(take_block)
            wanted = column(meta_v[0, pl.ds(mine + core * n_exp + e, 1), :], cap) - (1 - chip) * (2 * n_tok)
            hot = jnp.concatenate(
                [jnp.where(wanted == jnp.broadcast_to(listtok[j:j + 1, :], (cap, LANES)), 1.0, 0.0).astype(BF16)
                 for j in range(n_out)], axis=1)
            xbuf[mine_e, :] = xbuf[mine_e, :] + jnp.dot(hot, local[0:k_out, :], preferred_element_type=F32).astype(BF16)
            with jax.named_scope("wwait"):
                for c in w_copies(e):
                    c.wait()
            sum_o[...] = jnp.zeros((cap, d_model), F32)

        soon = (m_of(e - 1) == 0) | (m_of(e - 1) == 1)

        @pl.loop(0, 2)
        def _(half):
            @pl.when((e > 0) & ((half == 0) == soon))
            def _():
                pack_return(e - 1)

            pl.when(half == 0)(fill)

            @pl.when((half == 1) & (e + 1 < no) & (m_of(e) != 0) & (m_of(e) != 1))
            def _():
                forward(e + 1)

            x = xbuf[mine_e, :]
            o = None
            for f in range(n_f // 2):
                fs = at(half * (d_ff // 2) + f * f_tile, f_tile)
                pre = jnp.dot(x, wi[slot, :, fs], preferred_element_type=F32)
                h = jax.nn.gelu(pre, approximate=True).astype(BF16)
                part = jnp.dot(h, wo[slot, fs, :], preferred_element_type=F32)
                o = part if o is None else o + part
            sum_o[...] = sum_o[...] + o

        gcol = column(gate_v[pl.ds(e, 1), :], cap)
        chip_p[at(core * slots + e * cap, cap), :] = (
            jnp.concatenate([gcol] * (d_model // LANES), axis=1) * sum_o[...]).astype(BF16)
        p_copy(e).start()

        @pl.when((e + 1 < no) & ((m_of(e) == 0) | (m_of(e) == 1)))
        def _():
            forward(e + 1)

        @pl.when(e + W_SLOTS < n_exp)
        def _():
            for c in w_copies(e + W_SLOTS):
                c.start()

    n_blk = n_tok // (2 * cap)
    blk = 2 * cap
    sub_b = lax.broadcasted_iota(I32, (blk, LANES), 0) + ep * n_tok
    early = min(nc - 3, 10 - nc)

    def forward_back(m):
        with jax.named_scope("rwait"):
            r_copy(m).wait_recv()
            g_copy(m).start()

    def back_wait(m):
        with jax.named_scope("gwait"):
            g_copy(m).wait_recv()

    pl.loop(0, early)(forward_back)
    with jax.named_scope("pack_last"):
        pack_return(n_exp - 1)
    pl.loop(0, early)(back_wait)

    def owners(row, b):
        return jnp.where(jnp.broadcast_to(row, (blk, LANES)) == sub_b + b * blk, 1.0, 0.0).astype(BF16)

    @pl.loop(0, n_blk)
    def _(b):
        with jax.named_scope("early_back"):
            hot = jnp.concatenate([owners(tokrow[pl.ds(i, 1), :], b) for i in range(2 * early)], axis=1)
            own = chip_tok[at(core * n_tok + b * blk, blk), :].astype(F32)
            acc[at(b * blk, blk), :] = own + jnp.dot(hot, rland[0:early * 2 * cap, :], preferred_element_type=F32)

    @pl.loop(0, n_blk)
    def _(b):
        @pl.when(b == n_blk // 2)
        def _():
            forward_back(early)

        with jax.named_scope("own_scatter"):
            r = at(b * blk, blk)
            hot = jnp.concatenate([owners(meta_v[0, pl.ds(mine + i, 1), :], b) for i in range(rows)], axis=1)
            acc[r, :] = acc[r, :] + jnp.dot(hot, chip_p[...], preferred_element_type=F32)

    def combine(m):
        ids = [tokrow[pl.ds(2 * m + k, 1), :] for k in range(2)]
        back_wait(m)
        back = rland[at(2 * m * cap, 2 * cap), :]

        @pl.loop(0, n_blk)
        def _(b):
            r = at(b * blk, blk)
            hot = jnp.concatenate([owners(i, b) for i in ids], axis=1)
            acc[r, :] = acc[r, :] + jnp.dot(hot, back, preferred_element_type=F32)

    last = nc - 1

    @pl.loop(0, n_blk)
    def _(b):
        hot_last[at(b * blk, blk), :] = jnp.concatenate(
            [owners(tokrow[2 * last + k:2 * last + k + 1, :], b) for k in range(2)], axis=1)

    def sent(sem, buf, blocks):
        r = buf.at[0:blocks * cap]
        remote(r, r, sem, sem, ep=mate).wait_send()

    def sent_out(blocks):
        sent(d_ss, xsend, blocks)
        sent(f_ss, land, blocks)

    if n_out % 2:
        pl.when(core == 0)(lambda: sent_out(no))
        pl.when(core == 1)(lambda: sent_out(no - 1))
    else:
        sent_out(no)
    sent(p_ss, chip_p, n_exp)

    @pl.loop(early, nc - 2)
    def _(m):
        forward_back(m + 1)
        combine(m)

    combine(nc - 2)
    forward_back(last)
    sent(r_ss, rsend, nc)
    back_wait(last)
    with jax.named_scope("last_add"):
        back = rland[2 * last * cap:2 * nc * cap, :]
        out[...] = (acc[...] + jnp.dot(hot_last[...], back, preferred_element_type=F32)).astype(BF16)

    sent(g_ss, rland, nc)


def solution(mesh):
    n_dp, n_ep = mesh.shape["dp"], mesh.shape["ep"]
    row_spec = P(("dp", "ep"), None)
    expert_spec = P("ep", None, None)
    dma = pltpu.SemaphoreType.DMA
    any_spec = pl.BlockSpec(memory_space=pl.ANY)
    vmem_spec = pl.BlockSpec(memory_space=pltpu.VMEM)

    def local_layer(tok, idx, gate, w_in, w_out):
        n_tok, d_model = tok.shape
        n_exp, cap = idx.shape
        d_ff = w_in.shape[2]
        slots = n_exp * cap
        sizes = tuple((slots + i * cap, slots + j * cap) for i, j in LENGTHS)
        n_dev = n_dp * n_ep

        chip_tok, xown, meta, bucket = pl.pallas_call(
            functools.partial(plan_kernel, n_dp, n_ep, sizes),
            out_shape=(jax.ShapeDtypeStruct((2 * n_tok, d_model), BF16),
                       jax.ShapeDtypeStruct((slots, d_model), BF16),
                       jax.ShapeDtypeStruct((2, 4 * n_exp, cap), I32),
                       jax.ShapeDtypeStruct((1,), I32)),
            in_specs=[any_spec] * 2,
            out_specs=(vmem_spec, vmem_spec, vmem_spec, any_spec),
            scratch_shapes=[
                pltpu.VMEM((n_dev, n_exp, cap), I32),
                pltpu.SMEM((1,), I32),
                dma((3,)), dma, dma((2,)), dma, dma,
            ],
            compiler_params=pltpu.CompilerParams(
                collective_id=0, has_side_effects=True, vmem_limit_bytes=58 * 1024 * 1024),
        )(tok, idx)

        def branch(i):
            k_out, k_rows = sizes[i]
            no = (k_out // cap + 1) // 2
            nc = k_rows // (2 * cap)

            def run(chip_tok, xown, meta, gate, w_in, w_out):
                return pl.pallas_call(
                    functools.partial(layer_kernel, k_out, k_rows),
                    out_shape=jax.ShapeDtypeStruct((n_tok, d_model), BF16),
                    in_specs=[vmem_spec] * 4 + [any_spec] * 2,
                    out_specs=vmem_spec,
                    scratch_shapes=[
                        pltpu.VMEM((no * cap, d_model), BF16),
                        pltpu.VMEM((2 * no * cap, d_model), BF16),
                        pltpu.VMEM((2 * no * cap, d_model), BF16),
                        pltpu.VMEM((slots, d_model), BF16),
                        pltpu.VMEM((2 * slots, d_model), BF16),
                        pltpu.VMEM((slots, d_model), BF16),
                        pltpu.VMEM((nc * cap, d_model), BF16),
                        pltpu.VMEM((2 * nc * cap, d_model), BF16),
                        pltpu.VMEM((2 * n_exp, cap), I32),
                        pltpu.VMEM((2 * n_exp, cap), I32),
                        pltpu.VMEM((4 * n_exp, cap), I32),
                        pltpu.VMEM((n_tok, 2 * cap), BF16),
                        pltpu.VMEM((n_tok, d_model), F32),
                        pltpu.VMEM((cap, d_model), F32),
                        pltpu.VMEM((W_SLOTS, d_model, d_ff), BF16),
                        pltpu.VMEM((W_SLOTS, d_ff, d_model), BF16),
                        dma((2, W_SLOTS)),
                        dma, dma((no,)), dma, dma((no,)), dma, dma((n_exp,)), dma, dma((nc,)), dma, dma((nc,)),
                    ],
                    compiler_params=pltpu.CompilerParams(
                        collective_id=1 + i, has_side_effects=True, vmem_limit_bytes=54 * 1024 * 1024),
                )(chip_tok, xown, meta, gate, w_in, w_out)

            return run

        return lax.switch(bucket[0], [branch(i) for i in range(len(sizes))], chip_tok, xown, meta, gate, w_in, w_out)

    return jax.shard_map(local_layer, mesh=mesh, in_specs=(row_spec, row_spec, row_spec, expert_spec, expert_spec),
                         out_specs=row_spec, check_vma=False)
```
